8 devices in a mesh: ep: 8 (over z, y, x, core).
Axes of the slice: x: 2, y: 2, z: 1, core: 2. Of those that a mesh axis runs over, the one named last changes fastest.
Arguments:
- x_tokens: bfloat16 [65536, 768], P('ep')
- w_router: float32 [768, 16], replicated
- expert_idx: int32 [65536], P('ep')
- w_in: bfloat16 [16, 768, 3072], P('ep')
- w_out: bfloat16 [16, 3072, 768], P('ep')
- grad_y: bfloat16 [65536, 768], P('ep')
Outputs:
- output 1: bfloat16 [65536, 768], P('ep')
- output 2: float32 [16, 768, 3072], P('ep')
- output 3: float32 [16, 3072, 768], P('ep')
- output 4: float32 [768, 16], replicated
- output 5: float32 [], replicated
- output 6: float32 [], replicated
All inputs are finite; a program needn't handle non-finite values.
Results may differ from the reference program's by a relative error of at most 0.0122261.
Values are sent between devices in bfloat16 or wider.
A program may use at most 1 GiB of HBM per device.

```python
import jax
import jax.numpy as jnp
from jax import lax

D = 768
FF = 3072
EXPERTS = 16
TOKENS = 8192
GROUPS = 8

CAPACITY = (5 * TOKENS + 4 * EXPERTS - 1) // (4 * EXPERTS)
TOTAL_TOK = GROUPS * TOKENS
N_SLOTS = EXPERTS * CAPACITY
AUX_WEIGHT = 0.01
Z_WEIGHT = 0.001
LOGIT_SCALE = 1.5


def draw_routes(route_key):
    key_perm, key_hot, key_tok = jax.random.split(route_key, 3)
    expert_perm = jax.random.permutation(key_perm, EXPERTS)
    hot_expert = jax.random.randint(key_hot, (GROUPS,), 0, EXPERTS)
    n_hot = TOKENS // 4
    n_rest = TOKENS - n_hot - EXPERTS

    def one_group(group_id):
        key_a, key_b, key_c = jax.random.split(jax.random.fold_in(key_tok, group_id), 3)
        first_pick = jax.random.randint(key_a, (n_rest,), 0, EXPERTS)
        second_pick = jax.random.randint(key_b, (n_rest,), 0, EXPERTS)
        skewed = expert_perm[jnp.minimum(first_pick, second_pick)].astype(jnp.int32)
        hot_rows = jnp.full((n_hot,), hot_expert[group_id], jnp.int32)
        listed = jnp.concatenate([hot_rows, jnp.arange(EXPERTS, dtype=jnp.int32), skewed])
        return listed[jax.random.permutation(key_c, TOKENS)]

    return jax.vmap(one_group)(jnp.arange(GROUPS)).reshape(TOTAL_TOK).astype(jnp.int32)


def setup_inputs(seed: int = 0) -> dict:
    base_key = jax.random.key(seed)
    key_x, key_router, key_in, key_out, key_gy, key_route = jax.random.split(base_key, 6)
    x_tokens = jax.random.normal(key_x, (TOTAL_TOK, D), jnp.float32).astype(jnp.bfloat16)
    w_router = jax.random.normal(key_router, (D, EXPERTS), jnp.float32) * (LOGIT_SCALE * D ** -0.5)
    w_in = (jax.random.normal(key_in, (EXPERTS, D, FF), jnp.float32) * D ** -0.5).astype(jnp.bfloat16)
    w_out = (jax.random.normal(key_out, (EXPERTS, FF, D), jnp.float32) * FF ** -0.5).astype(jnp.bfloat16)
    grad_y = jax.random.normal(key_gy, (TOTAL_TOK, D), jnp.float32).astype(jnp.bfloat16)
    expert_idx = draw_routes(key_route)
    return {'x_tokens': x_tokens, 'w_router': w_router, 'expert_idx': expert_idx, 'w_in': w_in, 'w_out': w_out, 'grad_y': grad_y}


def router_group(x_group, w_router, idx_group):
    logits = jnp.dot(x_group.astype(jnp.float32), w_router)
    router_prob = jax.nn.softmax(logits, axis=-1)
    log_norm = jax.nn.logsumexp(logits, axis=-1)
    onehot = (idx_group[:, None] == jnp.arange(EXPERTS)[None, :]).astype(jnp.int32)
    position = jnp.sum(jnp.cumsum(onehot, axis=0) * onehot, axis=1) - 1
    tok_slot = jnp.where(position < CAPACITY, idx_group * CAPACITY + position, N_SLOTS)
    onehot_f = onehot.astype(jnp.float32)
    gate_val = jnp.sum(router_prob * onehot_f, axis=-1)
    return router_prob, log_norm, onehot_f, gate_val, tok_slot


def reference(x_tokens, w_router, expert_idx, w_in, w_out, grad_y):
    x_groups = x_tokens.reshape(GROUPS, TOKENS, D)
    idx_groups = expert_idx.reshape(GROUPS, TOKENS)
    gy_groups = grad_y.reshape(GROUPS, TOKENS, D)

    def first_pass(operands):
        x_group, idx_group, gy_group = operands
        router_prob, log_norm, onehot_f, gate_val, tok_slot = router_group(x_group, w_router, idx_group)
        scaled = (gate_val[:, None] * gy_group.astype(jnp.float32)).astype(jnp.bfloat16)
        empty_buf = jnp.zeros((N_SLOTS + 1, D), jnp.bfloat16)
        sent_rows = empty_buf.at[tok_slot].set(x_group)[:N_SLOTS]
        sent_grad = empty_buf.at[tok_slot].set(scaled)[:N_SLOTS]
        route_stats = jnp.concatenate([jnp.sum(onehot_f, axis=0), jnp.sum(router_prob, axis=0), jnp.sum(log_norm * log_norm)[None]])
        return sent_rows, sent_grad, route_stats

    sent_rows, sent_grad, route_stats = lax.map(first_pass, (x_groups, idx_groups, gy_groups))
    rows_all = sent_rows.reshape(GROUPS, EXPERTS, CAPACITY, D).transpose(1, 0, 2, 3).reshape(EXPERTS, GROUPS * CAPACITY, D)
    grads_all = sent_grad.reshape(GROUPS, EXPERTS, CAPACITY, D).transpose(1, 0, 2, 3).reshape(EXPERTS, GROUPS * CAPACITY, D)

    def expert_pass(operands):
        recv_rows, recv_grad, w_first, w_second = operands
        pre_act = jnp.dot(recv_rows, w_first, preferred_element_type=jnp.float32)
        hidden = jnp.maximum(pre_act, 0.0).astype(jnp.bfloat16)
        expert_out = jnp.dot(hidden, w_second, preferred_element_type=jnp.float32).astype(jnp.bfloat16)
        d_hidden = jnp.dot(recv_grad, w_second.T, preferred_element_type=jnp.float32)
        d_pre = jnp.where(hidden > 0, d_hidden, 0.0).astype(jnp.bfloat16)
        grad_out_e = jnp.dot(hidden.T, recv_grad, preferred_element_type=jnp.float32)
        grad_in_e = jnp.dot(recv_rows.T, d_pre, preferred_element_type=jnp.float32)
        d_rows = jnp.dot(d_pre, w_first.T, preferred_element_type=jnp.float32).astype(jnp.bfloat16)
        return expert_out, d_rows, grad_in_e, grad_out_e

    expert_out, d_rows, grad_w_in, grad_w_out = lax.map(expert_pass, (rows_all, grads_all, w_in, w_out))
    out_groups = expert_out.reshape(EXPERTS, GROUPS, CAPACITY, D).transpose(1, 0, 2, 3).reshape(GROUPS, N_SLOTS, D)
    back_groups = d_rows.reshape(EXPERTS, GROUPS, CAPACITY, D).transpose(1, 0, 2, 3).reshape(GROUPS, N_SLOTS, D)

    totals = jnp.sum(route_stats, axis=0)
    load_frac = totals[:EXPERTS] / TOTAL_TOK
    mean_prob = totals[EXPERTS:2 * EXPERTS] / TOTAL_TOK
    aux_loss = AUX_WEIGHT * EXPERTS * jnp.sum(load_frac * mean_prob)
    z_loss = Z_WEIGHT * totals[2 * EXPERTS] / TOTAL_TOK
    aux_vec = AUX_WEIGHT * EXPERTS * load_frac / TOTAL_TOK
    z_coef = 2.0 * Z_WEIGHT / TOTAL_TOK
    pad_row = jnp.zeros((1, D), jnp.bfloat16)

    def second_pass(operands):
        x_group, idx_group, gy_group, out_group, back_group = operands
        router_prob, log_norm, onehot_f, gate_val, tok_slot = router_group(x_group, w_router, idx_group)
        out_tok = jnp.concatenate([out_group, pad_row])[tok_slot]
        back_tok = jnp.concatenate([back_group, pad_row])[tok_slot]
        d_gate = jnp.sum(out_tok.astype(jnp.float32) * gy_group.astype(jnp.float32), axis=-1)
        spread = jnp.sum(router_prob * aux_vec[None, :], axis=-1, keepdims=True)
        d_logits = ((gate_val * d_gate)[:, None] * (onehot_f - router_prob)
                    + router_prob * (aux_vec[None, :] - spread)
                    + (z_coef * log_norm)[:, None] * router_prob)
        grad_x = (back_tok.astype(jnp.float32) + jnp.dot(d_logits, w_router.T)).astype(jnp.bfloat16)
        part_router = jnp.dot(x_group.astype(jnp.float32).T, d_logits)
        return grad_x, part_router

    grad_x, parts_router = lax.map(second_pass, (x_groups, idx_groups, gy_groups, out_groups, back_groups))
    return grad_x.reshape(TOTAL_TOK, D), grad_w_in, grad_w_out, jnp.sum(parts_router, axis=0), aux_loss, z_loss
```

```python
import jax
import jax.numpy as jnp
from jax import lax
from jax.experimental import pallas as pl
from jax.experimental.pallas import tpu as pltpu
from jax.sharding import PartitionSpec as P

AUX_WEIGHT = 0.01
Z_WEIGHT = 0.001
MESH = pl.DeviceIdType.MESH
F32 = jnp.float32
BF16 = jnp.bfloat16
LANES = 128


def route_slots(idx_group, num_experts, capacity):
    tokens = idx_group.shape[0]
    n_slots = num_experts * capacity
    onehot = (idx_group[:, None] == jnp.arange(num_experts, dtype=jnp.int32)[None, :]).astype(jnp.int32)
    position = jnp.sum(jnp.cumsum(onehot, axis=0) * onehot, axis=1) - 1
    tok_slot = jnp.where(position < capacity, idx_group * capacity + position, n_slots)
    slot_tok = jnp.full((n_slots,), tokens, jnp.int32).at[tok_slot].set(jnp.arange(tokens, dtype=jnp.int32), mode='drop')
    return onehot.astype(jnp.float32), tok_slot, slot_tok


def gather_rows(source, row_index):
    return jnp.take(source, row_index, axis=0, mode='fill', fill_value=0)


def router_grad(router_prob, onehot, gate_val, d_gate, log_norm, aux_vec, z_coef):
    spread = jnp.sum(router_prob * aux_vec, axis=-1, keepdims=True)
    return ((gate_val * d_gate)[..., None] * (onehot - router_prob)
            + router_prob * (aux_vec - spread)
            + (z_coef * log_norm)[..., None] * router_prob)


def split3(w):
    hi = lax.reduce_precision(w, 8, 7)
    mid = lax.reduce_precision(w - hi, 8, 7)
    return hi.astype(BF16), mid.astype(BF16), (w - hi - mid).astype(BF16)


def nt(a, b):
    return lax.dot_general(a, b, (((1,), (1,)), ((), ())), preferred_element_type=F32)


def nn(a, b):
    return jnp.dot(a, b, preferred_element_type=F32)


def expert_kernel(n_dev, n_local, num_experts, blk, xs, dys, wr, w_in, w_out,
                  xr, dyr, dsend, dback, gback, gwin, gwout_t,
                  xv, dyv, gv, x_t, g_t, win_v, wout_v, acc_in, acc_out, o_acc, r_acc, r_out, g_all,
                  x_send, x_recv, dy_send, dy_recv, r_send, r_recv, s_send, s_recv, ld_sem, st_sem, w_sem, flush_sem, own_sem):
    me = lax.axis_index('ep')
    n_blk = w_in.shape[2] // blk
    n_chunk = n_local * n_dev

    def peer_of(k):
        out = 0
        bit = 1
        while bit < n_dev:
            out = out + bit * (((me // bit) + (k // bit)) % 2)
            bit *= 2
        return out

    barrier = pltpu.get_barrier_semaphore()
    for k in range(1, n_dev):
        pl.semaphore_signal(barrier, inc=1, device_id=(peer_of(k),), device_id_type=MESH)
    pl.semaphore_wait(barrier, n_dev - 1)

    def x_copy(k, e):
        p = peer_of(k)
        return pltpu.make_async_remote_copy(xs.at[p, e], xr.at[me, e], x_send.at[e, k], x_recv.at[e, k], device_id=(p,), device_id_type=MESH)

    def dy_copy(k, e):
        p = peer_of(k)
        return pltpu.make_async_remote_copy(dys.at[p, e], dyr.at[me, e], dy_send.at[e, k], dy_recv.at[e, k], device_id=(p,), device_id_type=MESH)

    def r_copy(k, e):
        p = peer_of(k)
        return pltpu.make_async_remote_copy(dsend.at[p, e], dback.at[me, e], r_send.at[e, k], r_recv.at[e, k], device_id=(p,), device_id_type=MESH)

    def s_copy(k, e):
        p = peer_of(k)
        return pltpu.make_async_remote_copy(g_all.at[e, k], gback.at[me, e], s_send.at[e, k], s_recv.at[e, k], device_id=(p,), device_id_type=MESH)

    for e in range(n_local):
        for k in (1, 2, 4, 6, 3, 5, 7):
            x_copy(k, e).start()
            dy_copy(k, e).start()

    order = (0, 1, 2, 4, 6, 3, 5, 7)

    def offset_of(i):
        k = i * 0
        for at, val in enumerate(order):
            k = k + jnp.where(i == at, val, 0)
        return k

    def load(e, i, slot, do):
        k = offset_of(i)
        p = peer_of(k)

        @pl.when(i == 0)
        def _():
            do(pltpu.make_async_copy(xs.at[me, e], xv.at[slot], ld_sem.at[slot, 0]))
            do(pltpu.make_async_copy(dys.at[me, e], dyv.at[slot], ld_sem.at[slot, 1]))

        @pl.when(i > 0)
        def _():
            do(pltpu.make_async_copy(xr.at[p, e], xv.at[slot], ld_sem.at[slot, 0]))
            do(pltpu.make_async_copy(dyr.at[p, e], dyv.at[slot], ld_sem.at[slot, 1]))

    def arrive(e, i):
        @pl.when(i > 0)
        def _():
            k = offset_of(i)
            x_copy(k, e).wait_recv()
            dy_copy(k, e).wait_recv()

    def store(c, do):
        e, i = c // n_dev, c % n_dev
        k = offset_of(i)
        p = peer_of(k)

        @pl.when(i == 0)
        def _():
            do(pltpu.make_async_copy(r_out.at[c % 2], dback.at[me, e], st_sem.at[c % 2]))

        @pl.when(i > 0)
        def _():
            do(pltpu.make_async_copy(r_out.at[c % 2], dsend.at[p, e], st_sem.at[c % 2]))

    def own_g(e):
        return pltpu.make_async_copy(g_all.at[e, 0], gback.at[me, e], own_sem.at[e])

    def send_back(c):
        e, i = c // n_dev, c % n_dev
        k = offset_of(i)
        store(c, lambda cp: cp.wait())

        @pl.when(i == 0)
        def _():
            own_g(e).start()

        @pl.when(i > 0)
        def _():
            r_copy(k, e).start()
            s_copy(k, e).start()

    def weights(e):
        return (pltpu.make_async_copy(w_in.at[e], win_v, w_sem.at[0]), pltpu.make_async_copy(w_out.at[e], wout_v, w_sem.at[1]))

    def flush(e):
        return (pltpu.make_async_copy(acc_in, gwin.at[e], flush_sem.at[0]), pltpu.make_async_copy(acc_out, gwout_t.at[e], flush_sem.at[1]))

    for cp in weights(0):
        cp.start()
    load(0, 0, 0, lambda cp: cp.start())

    def chunk(c, _):
        e, i = c // n_dev, c % n_dev
        k = offset_of(i)
        slot = c % 2

        @pl.when(i == 0)
        def _():
            @pl.when(c > 0)
            def _():
                for cp in weights(e):
                    cp.start()
                for cp in flush(e - 1):
                    cp.wait()
            acc_in[...] = jnp.zeros_like(acc_in)
            acc_out[...] = jnp.zeros_like(acc_out)
            for cp in weights(e):
                cp.wait()

        load(e, i, slot, lambda cp: cp.wait())
        x = xv[slot]
        logits = nn(x, wr[0]) + nn(x, wr[1]) + nn(x, wr[2])
        lane = lax.broadcasted_iota(jnp.int32, logits.shape, 1)
        logits = jnp.where(lane < num_experts, logits, -1e30)
        prob = jnp.exp(logits - jnp.max(logits, axis=1, keepdims=True))
        mine = jnp.sum(jnp.where(lane == me * n_local + e, prob, 0.0), axis=1, keepdims=True)
        gate = mine / jnp.sum(prob, axis=1, keepdims=True)
        grad = (gate * dyv[slot].astype(F32)).astype(BF16)
        gv[...] = grad
        x_t[...] = x.T
        g_t[...] = grad.T
        o_acc[...] = jnp.zeros_like(o_acc)
        r_acc[...] = jnp.zeros_like(r_acc)

        def block(f, _):
            @pl.when(f == n_blk - 1)
            def _():
                @pl.when(c + 1 < n_chunk)
                def _():
                    ne, ni = (c + 1) // n_dev, (c + 1) % n_dev
                    arrive(ne, ni)
                    load(ne, ni, 1 - slot, lambda cp: cp.start())

            @pl.when(f == 1)
            def _():
                @pl.when(c > 0)
                def _():
                    send_back(c - 1)

            cols = pl.ds(pl.multiple_of(f * blk, LANES), blk)
            win = win_v[:, cols]
            wout = wout_v[cols, :]
            hidden = jnp.maximum(nn(xv[slot], win), 0.0).astype(BF16)
            d_hidden = nt(gv[...], wout)
            d_pre = jnp.where(hidden > 0, d_hidden, 0.0).astype(BF16)
            o_acc[...] += nn(hidden, wout)
            r_acc[...] += nt(d_pre, win)
            acc_out[:, cols] += nn(g_t[...], hidden)
            acc_in[:, cols] += nn(x_t[...], d_pre)
            return 0

        lax.fori_loop(0, n_blk, block, 0)
        r_out[slot] = r_acc[...].astype(BF16)
        store(c, lambda cp: cp.start())
        g_val = jnp.sum(o_acc[...].astype(BF16).astype(F32) * dyv[slot].astype(F32), axis=1, keepdims=True)
        g_row = jnp.broadcast_to(g_val, (g_val.shape[0], LANES)).T
        g_all[e, k] = g_row[0:1, :]

        @pl.when(i == n_dev - 1)
        def _():
            for cp in flush(e):
                cp.start()
        return 0

    lax.fori_loop(0, n_chunk, chunk, 0)
    send_back(n_chunk - 1)
    for cp in flush(n_local - 1):
        cp.wait()
    for e in range(n_local):
        own_g(e).wait()
        for k in range(1, n_dev):
            x_copy(k, e).wait_send()
            dy_copy(k, e).wait_send()
            r_copy(k, e).wait()
            s_copy(k, e).wait()


def expert_exchange(n_dev, xs, dys, wr, w_in, w_out):
    n_local, d_model, d_ff = w_in.shape
    cap = xs.shape[2]
    num_experts = n_dev * n_local
    blk = d_ff // 4
    hbm = pl.BlockSpec(memory_space=pl.ANY)
    vmem = pl.BlockSpec(memory_space=pltpu.VMEM)
    rows = jax.ShapeDtypeStruct(xs.shape, BF16)
    g_shape = jax.ShapeDtypeStruct((n_dev, n_local, 1, cap), F32)
    w_shape = jax.ShapeDtypeStruct((n_local, d_model, d_ff), F32)
    dma = pltpu.SemaphoreType.DMA
    pair = (n_local, n_dev)
    return pl.pallas_call(
        lambda *refs: expert_kernel(n_dev, n_local, num_experts, blk, *refs),
        out_shape=(rows, rows, rows, rows, g_shape, w_shape, w_shape),
        in_specs=[hbm, hbm, vmem, hbm, hbm],
        out_specs=[hbm] * 7,
        scratch_shapes=[
            pltpu.VMEM((2, cap, d_model), BF16), pltpu.VMEM((2, cap, d_model), BF16), pltpu.VMEM((cap, d_model), BF16),
            pltpu.VMEM((d_model, cap), BF16), pltpu.VMEM((d_model, cap), BF16),
            pltpu.VMEM((d_model, d_ff), BF16), pltpu.VMEM((d_ff, d_model), BF16),
            pltpu.VMEM((d_model, d_ff), F32), pltpu.VMEM((d_model, d_ff), F32),
            pltpu.VMEM((cap, d_model), F32), pltpu.VMEM((cap, d_model), F32),
            pltpu.VMEM((2, cap, d_model), BF16), pltpu.VMEM((n_local, n_dev, 1, cap), F32),
            dma(pair), dma(pair), dma(pair), dma(pair), dma(pair), dma(pair), dma(pair), dma(pair),
            dma((2, 2)), dma((2,)), dma((2,)), dma((2,)), dma((n_local,)),
        ],
        compiler_params=pltpu.CompilerParams(collective_id=0, has_side_effects=True, vmem_limit_bytes=63 * 2 ** 20),
        name='expert_exchange',
    )(xs, dys, wr, w_in, w_out)


def solution(mesh):
    n_dev = mesh.shape['ep']

    def expert_layer(x_tokens, w_router, expert_idx, w_in, w_out, grad_y):
        tokens, d_model = x_tokens.shape
        n_local = w_in.shape[0]
        num_experts = n_local * n_dev
        capacity = (5 * tokens + 4 * num_experts - 1) // (4 * num_experts)
        total_tok = tokens * n_dev
        onehot, tok_slot, slot_tok = route_slots(expert_idx, num_experts, capacity)
        xs = gather_rows(x_tokens, slot_tok).reshape(n_dev, n_local, capacity, d_model)
        dys = gather_rows(grad_y, slot_tok).reshape(n_dev, n_local, capacity, d_model)
        wr = jnp.pad(jnp.stack(split3(w_router)), ((0, 0), (0, 0), (0, LANES - num_experts)))

        logits = jnp.dot(x_tokens, w_router, preferred_element_type=jnp.float32)
        router_prob = jax.nn.softmax(logits, axis=-1)
        log_norm = jax.nn.logsumexp(logits, axis=-1)
        gate_val = jnp.sum(router_prob * onehot, axis=-1)
        route_stats = jnp.concatenate([jnp.sum(onehot, axis=0), jnp.sum(router_prob, axis=0), jnp.sum(log_norm * log_norm)[None]])
        route_stats = lax.psum(route_stats, 'ep')

        _, _, _, d_back, g_back, grad_w_in, gwout_t = expert_exchange(n_dev, xs, dys, wr, w_in, w_out)
        grad_w_out = jnp.swapaxes(gwout_t, 1, 2)
        d_gate = gather_rows(g_back.reshape(-1), tok_slot)
        dx_expert = gather_rows(d_back.reshape(num_experts * capacity, d_model), tok_slot)

        load_frac = route_stats[:num_experts] / total_tok
        mean_prob = route_stats[num_experts:2 * num_experts] / total_tok
        aux_loss = AUX_WEIGHT * num_experts * jnp.sum(load_frac * mean_prob)
        z_loss = Z_WEIGHT * route_stats[2 * num_experts] / total_tok
        aux_vec = AUX_WEIGHT * num_experts * load_frac / total_tok
        d_logits = router_grad(router_prob, onehot, gate_val, d_gate, log_norm, aux_vec, 2.0 * Z_WEIGHT / total_tok)
        dx_router = jnp.einsum('se,de->sd', d_logits, w_router)
        grad_x = (dx_expert.astype(jnp.float32) + dx_router).astype(jnp.bfloat16)
        grad_w_router = lax.psum(jnp.einsum('sd,se->de', x_tokens, d_logits, preferred_element_type=jnp.float32), 'ep')
        return grad_x, grad_w_in, grad_w_out, grad_w_router, aux_loss, z_loss

    return jax.shard_map(expert_layer, mesh=mesh,
                         in_specs=(P('ep', None), P(None, None), P('ep'), P('ep', None, None), P('ep', None, None), P('ep', None)),
                         out_specs=(P('ep', None), P('ep', None, None), P('ep', None, None), P(None, None), P(), P()),
                         check_vma=False)
```

```python
import jax
import jax.numpy as jnp
from jax import lax
from jax.experimental import pallas as pl
from jax.experimental.pallas import tpu as pltpu
from jax.sharding import PartitionSpec as P

AUX_WEIGHT = 0.01
Z_WEIGHT = 0.001
MESH = pl.DeviceIdType.MESH
F32 = jnp.float32
BF16 = jnp.bfloat16
LANES = 128


def route_slots(idx_group, num_experts, capacity):
    onehot = (idx_group[:, None] == jnp.arange(num_experts, dtype=jnp.int32)[None, :]).astype(jnp.int32)
    position = jnp.sum(jnp.cumsum(onehot, axis=0) * onehot, axis=1) - 1
    tok_slot = jnp.where(position < capacity, idx_group * capacity + position, num_experts * capacity)
    return tok_slot, jnp.sum(onehot, axis=0)


def split3(w):
    hi = lax.reduce_precision(w, 8, 7)
    mid = lax.reduce_precision(w - hi, 8, 7)
    return hi.astype(BF16), mid.astype(BF16), (w - hi - mid).astype(BF16)


def nt(a, b):
    return lax.dot_general(a, b, (((1,), (1,)), ((), ())), preferred_element_type=F32)


def nn(a, b):
    return jnp.dot(a, b, preferred_element_type=F32)


def expert_kernel(n_dev, n_local, num_experts, blk, xs, dys, wr, cnt, w_in, w_out,
                  xr, dyr, dsend, dback, gback, gwin, gwout_t, cnt_all,
                  xv, dyv, gv, x_t, g_t, win_v, wout_v, acc_in, acc_out, o_acc, r_acc, r_out, g_all,
                  x_send, x_recv, dy_send, dy_recv, r_send, r_recv, s_send, s_recv, c_send, c_recv, ld_sem, st_sem, w_sem, flush_sem, own_sem):
    me = lax.axis_index('ep')
    n_blk = w_in.shape[2] // blk
    n_chunk = n_local * n_dev

    def peer_of(k):
        out = 0
        bit = 1
        while bit < n_dev:
            out = out + bit * (((me // bit) + (k // bit)) % 2)
            bit *= 2
        return out

    barrier = pltpu.get_barrier_semaphore()
    for k in range(1, n_dev):
        pl.semaphore_signal(barrier, inc=1, device_id=(peer_of(k),), device_id_type=MESH)
    pl.semaphore_wait(barrier, n_dev - 1)

    def x_copy(k, e):
        p = peer_of(k)
        return pltpu.make_async_remote_copy(xs.at[p, e], xr.at[me, e], x_send.at[e, k], x_recv.at[e, k], device_id=(p,), device_id_type=MESH)

    def dy_copy(k, e):
        p = peer_of(k)
        return pltpu.make_async_remote_copy(dys.at[p, e], dyr.at[me, e], dy_send.at[e, k], dy_recv.at[e, k], device_id=(p,), device_id_type=MESH)

    def r_copy(k, e):
        p = peer_of(k)
        return pltpu.make_async_remote_copy(dsend.at[p, e], dback.at[me, e], r_send.at[e, k], r_recv.at[e, k], device_id=(p,), device_id_type=MESH)

    def s_copy(k, e):
        p = peer_of(k)
        return pltpu.make_async_remote_copy(g_all.at[e, k], gback.at[me, e], s_send.at[e, k], s_recv.at[e, k], device_id=(p,), device_id_type=MESH)

    def c_copy(k):
        p = peer_of(k)
        return pltpu.make_async_remote_copy(cnt, cnt_all.at[me], c_send.at[k], c_recv.at[k], device_id=(p,), device_id_type=MESH)

    own_cnt = pltpu.make_async_copy(cnt, cnt_all.at[me], own_sem.at[n_local])
    own_cnt.start()
    for k in range(1, n_dev):
        c_copy(k).start()
    for e in range(n_local):
        for k in (1, 2, 4, 6, 3, 5, 7):
            x_copy(k, e).start()
            dy_copy(k, e).start()

    order = (0, 1, 2, 4, 6, 3, 5, 7)

    def offset_of(i):
        k = i * 0
        for at, val in enumerate(order):
            k = k + jnp.where(i == at, val, 0)
        return k

    def load(e, i, slot, do):
        k = offset_of(i)
        p = peer_of(k)

        @pl.when(i == 0)
        def _():
            do(pltpu.make_async_copy(xs.at[me, e], xv.at[slot], ld_sem.at[slot, 0]))
            do(pltpu.make_async_copy(dys.at[me, e], dyv.at[slot], ld_sem.at[slot, 1]))

        @pl.when(i > 0)
        def _():
            do(pltpu.make_async_copy(xr.at[p, e], xv.at[slot], ld_sem.at[slot, 0]))
            do(pltpu.make_async_copy(dyr.at[p, e], dyv.at[slot], ld_sem.at[slot, 1]))

    def arrive(e, i):
        @pl.when(i > 0)
        def _():
            k = offset_of(i)
            x_copy(k, e).wait_recv()
            dy_copy(k, e).wait_recv()

    def store(c, do):
        e, i = c // n_dev, c % n_dev
        k = offset_of(i)
        p = peer_of(k)

        @pl.when(i == 0)
        def _():
            do(pltpu.make_async_copy(r_out.at[c % 2], dback.at[me, e], st_sem.at[c % 2]))

        @pl.when(i > 0)
        def _():
            do(pltpu.make_async_copy(r_out.at[c % 2], dsend.at[p, e], st_sem.at[c % 2]))

    def own_g(e):
        return pltpu.make_async_copy(g_all.at[e, 0], gback.at[me, e], own_sem.at[e])

    def send_back(c):
        e, i = c // n_dev, c % n_dev
        k = offset_of(i)
        store(c, lambda cp: cp.wait())

        @pl.when(i == 0)
        def _():
            own_g(e).start()

        @pl.when(i > 0)
        def _():
            r_copy(k, e).start()
            s_copy(k, e).start()

    def weights(e):
        return (pltpu.make_async_copy(w_in.at[e], win_v, w_sem.at[0]), pltpu.make_async_copy(w_out.at[e], wout_v, w_sem.at[1]))

    def flush(e):
        return (pltpu.make_async_copy(acc_in, gwin.at[e], flush_sem.at[0]), pltpu.make_async_copy(acc_out, gwout_t.at[e], flush_sem.at[1]))

    for cp in weights(0):
        cp.start()
    load(0, 0, 0, lambda cp: cp.start())

    def chunk(c, _):
        e, i = c // n_dev, c % n_dev
        k = offset_of(i)
        slot = c % 2

        @pl.when(i == 0)
        def _():
            @pl.when(c > 0)
            def _():
                for cp in weights(e):
                    cp.start()
                for cp in flush(e - 1):
                    cp.wait()
            acc_in[...] = jnp.zeros_like(acc_in)
            acc_out[...] = jnp.zeros_like(acc_out)
            for cp in weights(e):
                cp.wait()

        load(e, i, slot, lambda cp: cp.wait())
        x = xv[slot]
        logits = nn(x, wr[0]) + nn(x, wr[1]) + nn(x, wr[2])
        lane = lax.broadcasted_iota(jnp.int32, logits.shape, 1)
        logits = jnp.where(lane < num_experts, logits, -1e30)
        prob = jnp.exp(logits - jnp.max(logits, axis=1, keepdims=True))
        mine = jnp.sum(jnp.where(lane == me * n_local + e, prob, 0.0), axis=1, keepdims=True)
        gate = mine / jnp.sum(prob, axis=1, keepdims=True)
        grad = (gate * dyv[slot].astype(F32)).astype(BF16)
        gv[...] = grad
        x_t[...] = x.T
        g_t[...] = grad.T
        o_acc[...] = jnp.zeros_like(o_acc)
        r_acc[...] = jnp.zeros_like(r_acc)

        def block(f, _):
            @pl.when(f == n_blk - 1)
            def _():
                @pl.when(c + 1 < n_chunk)
                def _():
                    ne, ni = (c + 1) // n_dev, (c + 1) % n_dev
                    arrive(ne, ni)
                    load(ne, ni, 1 - slot, lambda cp: cp.start())

            @pl.when(f == 1)
            def _():
                @pl.when(c > 0)
                def _():
                    send_back(c - 1)

            cols = pl.ds(pl.multiple_of(f * blk, LANES), blk)
            win = win_v[:, cols]
            wout = wout_v[cols, :]
            hidden = jnp.maximum(nn(xv[slot], win), 0.0).astype(BF16)
            d_hidden = nt(gv[...], wout)
            d_pre = jnp.where(hidden > 0, d_hidden, 0.0).astype(BF16)
            o_acc[...] += nn(hidden, wout)
            r_acc[...] += nt(d_pre, win)
            acc_out[:, cols] += nn(g_t[...], hidden)
            acc_in[:, cols] += nn(x_t[...], d_pre)
            return 0

        lax.fori_loop(0, n_blk, block, 0)
        r_out[slot] = r_acc[...].astype(BF16)
        store(c, lambda cp: cp.start())
        g_val = jnp.sum(o_acc[...].astype(BF16).astype(F32) * dyv[slot].astype(F32), axis=1, keepdims=True)
        g_row = jnp.broadcast_to(g_val, (g_val.shape[0], LANES)).T
        g_all[e, k] = g_row[0:1, :]

        @pl.when(i == n_dev - 1)
        def _():
            for cp in flush(e):
                cp.start()
        return 0

    lax.fori_loop(0, n_chunk, chunk, 0)
    send_back(n_chunk - 1)
    for cp in flush(n_local - 1):
        cp.wait()
    own_cnt.wait()
    for k in range(1, n_dev):
        c_copy(k).wait()
    for e in range(n_local):
        own_g(e).wait()
        for k in range(1, n_dev):
            x_copy(k, e).wait_send()
            dy_copy(k, e).wait_send()
            r_copy(k, e).wait()
            s_copy(k, e).wait()


def expert_exchange(n_dev, xs, dys, wr, cnt, w_in, w_out):
    n_local, d_model, d_ff = w_in.shape
    cap = xs.shape[2]
    num_experts = n_dev * n_local
    blk = d_ff // 4
    hbm = pl.BlockSpec(memory_space=pl.ANY)
    vmem = pl.BlockSpec(memory_space=pltpu.VMEM)
    rows = jax.ShapeDtypeStruct(xs.shape, BF16)
    g_shape = jax.ShapeDtypeStruct((n_dev, n_local, 1, cap), F32)
    w_shape = jax.ShapeDtypeStruct((n_local, d_model, d_ff), F32)
    dma = pltpu.SemaphoreType.DMA
    pair = (n_local, n_dev)
    return pl.pallas_call(
        lambda *refs: expert_kernel(n_dev, n_local, num_experts, blk, *refs),
        out_shape=(rows, rows, rows, rows, g_shape, w_shape, w_shape, jax.ShapeDtypeStruct((n_dev,) + cnt.shape, F32)),
        in_specs=[hbm, hbm, vmem, vmem, hbm, hbm],
        out_specs=[hbm] * 8,
        scratch_shapes=[
            pltpu.VMEM((2, cap, d_model), BF16), pltpu.VMEM((2, cap, d_model), BF16), pltpu.VMEM((cap, d_model), BF16),
            pltpu.VMEM((d_model, cap), BF16), pltpu.VMEM((d_model, cap), BF16),
            pltpu.VMEM((d_model, d_ff), BF16), pltpu.VMEM((d_ff, d_model), BF16),
            pltpu.VMEM((d_model, d_ff), F32), pltpu.VMEM((d_model, d_ff), F32),
            pltpu.VMEM((cap, d_model), F32), pltpu.VMEM((cap, d_model), F32),
            pltpu.VMEM((2, cap, d_model), BF16), pltpu.VMEM((n_local, n_dev, 1, cap), F32),
            dma(pair), dma(pair), dma(pair), dma(pair), dma(pair), dma(pair), dma(pair), dma(pair), dma((n_dev,)), dma((n_dev,)),
            dma((2, 2)), dma((2,)), dma((2,)), dma((2,)), dma((n_local + 1,)),
        ],
        compiler_params=pltpu.CompilerParams(collective_id=0, has_side_effects=True, vmem_limit_bytes=63 * 2 ** 20),
        name='expert_exchange',
    )(xs, dys, wr, cnt, w_in, w_out)


PITCH = 7 * 8
ROW_TILES = 6


def row_address(slot):
    return (slot // 8) * PITCH + slot % 8


def row(addr, tiles):
    return pl.ds(addr, tiles, stride=8)


def permute_kernel(tb, addr, x_hbm, dy_hbm, xs, dys, inb, stage, table, outb, in_sem, out_sem):
    tokens = x_hbm.shape[0]
    n_out, n_local, cap, d_model = xs.shape
    groups = cap // 8
    tiled = table.reshape(table.shape[0] // PITCH, PITCH, LANES)
    stage3 = stage.reshape(tb // 8, PITCH, LANES)
    n_in = tokens // tb

    def fetch(source, b):
        return pltpu.make_async_copy(source.at[pl.ds(pl.multiple_of(b * tb, tb), tb), :], inb.at[b % 2], in_sem.at[b % 2])

    def emit(sink, c):
        return pltpu.make_async_copy(outb.at[c % 2], sink.at[c // n_local, c % n_local], out_sem.at[c % 2])

    fetch(x_hbm, 0).start()
    table[...] = jnp.zeros_like(table)
    for source, sink, follow in ((x_hbm, xs, dy_hbm), (dy_hbm, dys, None)):
        def scatter(b, _):
            @pl.when(b + 1 < n_in)
            def _():
                fetch(source, b + 1).start()
            if follow is not None:
                @pl.when(b + 1 == n_in)
                def _():
                    fetch(follow, 0).start()
            fetch(source, b).wait()
            for j in range(ROW_TILES):
                part = inb[b % 2, :, j * LANES:(j + 1) * LANES].astype(F32)
                stage3[:, j * 8:(j + 1) * 8, :] = part.reshape(tb // 8, 8, LANES)

            def move(i, _):
                for r in range(32):
                    at = addr[b * tb + i * 32 + r]
                    table[row(at, ROW_TILES), :] = stage[row(i * (4 * PITCH) + (r // 8) * PITCH + r % 8, ROW_TILES), :]
                return 0

            lax.fori_loop(0, tb // 32, move, 0)
            return 0

        lax.fori_loop(0, n_in, scatter, 0)

        def drain(c, _):
            @pl.when(c >= 2)
            def _():
                emit(sink, c - 2).wait()
            for j in range(ROW_TILES):
                part = tiled[pl.ds(c * groups, groups), j * 8:(j + 1) * 8, :].reshape(cap, LANES)
                outb[c % 2, :, j * LANES:(j + 1) * LANES] = part.astype(BF16)
            emit(sink, c).start()
            return 0

        n_chunk = n_out * n_local
        lax.fori_loop(0, n_chunk, drain, 0)
        for c in (n_chunk - 2, n_chunk - 1):
            emit(sink, c).wait()


def permute(n_dev, n_local, capacity, addr, x, dy):
    tokens, d_model = x.shape
    tb = 512
    hbm = pl.BlockSpec(memory_space=pl.ANY)
    out = jax.ShapeDtypeStruct((n_dev, n_local, capacity, d_model), BF16)
    n_groups = n_dev * n_local * capacity // 8 + 1
    return pl.pallas_call(
        lambda *refs: permute_kernel(tb, *refs),
        out_shape=(out, out),
        grid_spec=pltpu.PrefetchScalarGridSpec(
            num_scalar_prefetch=1, grid=(), in_specs=[hbm, hbm], out_specs=[hbm, hbm],
            scratch_shapes=[
                pltpu.VMEM((2, tb, d_model), BF16), pltpu.VMEM((tb // 8 * PITCH, LANES), F32), pltpu.VMEM((n_groups * PITCH, LANES), F32),
                pltpu.VMEM((2, capacity, d_model), BF16), pltpu.SemaphoreType.DMA((2,)), pltpu.SemaphoreType.DMA((2,))]),
        compiler_params=pltpu.CompilerParams(vmem_limit_bytes=60 * 2 ** 20),
        name='permute_rows',
    )(addr, x, dy)


def token_kernel(num_experts, z_coef, addr, x, idx, wr, wr_back, v_row, dback, gback, grad_x, partial, acc,
                 stage, table, inb, pieces_t, p_acc, z_acc, in_sem):
    b = pl.program_id(0)
    tb = x.shape[0]
    n_out, n_local, cap, d_model = dback.shape
    groups = cap // 8
    tiled = table.reshape(table.shape[0] // PITCH, PITCH, LANES)
    stage3 = stage.reshape(tb // 8, PITCH, LANES)
    n_chunk = n_out * n_local

    @pl.when(b == 0)
    def _():
        def fetch(c):
            return pltpu.make_async_copy(dback.at[c // n_local, c % n_local], inb.at[c % 2], in_sem.at[c % 2])

        fetch(0).start()
        acc[...] = jnp.zeros_like(acc)
        p_acc[...] = jnp.zeros_like(p_acc)
        z_acc[...] = jnp.zeros_like(z_acc)
        tiled[n_chunk * groups] = jnp.zeros((PITCH, LANES), F32)

        def fill(c, _):
            @pl.when(c + 1 < n_chunk)
            def _():
                fetch(c + 1).start()
            fetch(c).wait()
            for j in range(ROW_TILES):
                part = inb[c % 2, :, j * LANES:(j + 1) * LANES].astype(F32)
                tiled[pl.ds(c * groups, groups), j * 8:(j + 1) * 8, :] = part.reshape(groups, 8, LANES)
            g_col = jnp.broadcast_to(gback[pl.ds(c, 1), :], (LANES, cap)).T
            tiled[pl.ds(c * groups, groups), 6 * 8:7 * 8, :] = g_col.reshape(groups, 8, LANES)
            return 0

        lax.fori_loop(0, n_chunk, fill, 0)

    def move(i, _):
        for r in range(32):
            at = addr[b * tb + i * 32 + r]
            stage[row(i * (4 * PITCH) + (r // 8) * PITCH + r % 8, 7), :] = table[row(at, 7), :]
        return 0

    lax.fori_loop(0, tb // 32, move, 0)

    xv = x[...]
    logits = nn(xv, wr[0]) + nn(xv, wr[1]) + nn(xv, wr[2])
    lane = lax.broadcasted_iota(jnp.int32, logits.shape, 1)
    real = lane < num_experts
    top = jnp.max(jnp.where(real, logits, -1e30), axis=1, keepdims=True)
    expd = jnp.where(real, jnp.exp(jnp.minimum(logits - top, 0.0)), 0.0)
    total = jnp.sum(expd, axis=1, keepdims=True)
    prob = expd / total
    z = top + jnp.log(total)
    mine = jnp.broadcast_to(idx[pl.ds(b, 1), :], (LANES, tb)).T == lane.astype(F32)
    onehot = jnp.where(mine, 1.0, 0.0)
    gate = jnp.sum(jnp.where(mine, prob, 0.0), axis=1, keepdims=True)
    g = stage3[:, 6 * 8:7 * 8, :].reshape(tb, LANES)
    v = v_row[0:1, :]
    spread = jnp.sum(prob * v, axis=1, keepdims=True)
    dlog = gate * g * (onehot - prob) + prob * (v - spread) + (z_coef * z) * prob
    hi = dlog.astype(BF16).astype(F32)
    mid = (dlog - hi).astype(BF16).astype(F32)
    low = dlog - hi - mid
    def at(piece, k):
        return piece if k == 0 else pltpu.roll(piece, k * num_experts, 1)
    pieces = at(hi, 0) + at(mid, 1) + at(low, 2) + at(hi, 3) + at(mid, 4) + at(hi, 5)
    dx = nn(pieces.astype(BF16), wr_back[...])
    pieces_t[...] = pieces.T.astype(BF16)
    for j in range(ROW_TILES):
        cols = slice(j * LANES, (j + 1) * LANES)
        grad_x[:, cols] = (stage3[:, j * 8:(j + 1) * 8, :].reshape(tb, LANES) + dx[:, cols]).astype(BF16)
    acc[...] += nn(pieces_t[...], xv)
    p_acc[...] += jnp.sum(prob.reshape(tb // 8, 8, LANES), axis=0)
    z_acc[...] += jnp.sum(jnp.broadcast_to(z * z, (tb, LANES)).reshape(tb // 8, 8, LANES), axis=0)

    @pl.when(b == pl.num_programs(0) - 1)
    def _():
        n = num_experts
        partial[...] = jnp.zeros_like(partial)
        partial[0:n, :] = acc[0:n, :] + acc[n:2 * n, :] + acc[2 * n:3 * n, :]
        partial[n:n + 1, 0:LANES] = jnp.sum(p_acc[...], axis=0, keepdims=True)
        partial[n:n + 1, LANES:2 * LANES] = jnp.sum(z_acc[...], axis=0, keepdims=True)


def token_side(num_experts, z_coef, addr, x, idx, wr, wr_back, v_row, dback, gback):
    tokens, d_model = x.shape
    n_dev, n_local, cap, _ = dback.shape
    tb = 512
    hbm = pl.BlockSpec(memory_space=pl.ANY)
    idx = idx.astype(F32).reshape(tokens // tb, tb)
    gback = gback.reshape(n_dev * n_local, cap)

    def whole(a):
        return pl.BlockSpec(a.shape, lambda b, addr: (0,) * a.ndim)

    n_groups = n_dev * n_local * cap // 8 + 1
    rows = num_experts + 8
    return pl.pallas_call(
        lambda *refs: token_kernel(num_experts, z_coef, *refs),
        out_shape=(jax.ShapeDtypeStruct(x.shape, BF16), jax.ShapeDtypeStruct((rows, d_model), F32), jax.ShapeDtypeStruct((LANES, d_model), F32)),
        grid_spec=pltpu.PrefetchScalarGridSpec(
            num_scalar_prefetch=1, grid=(tokens // tb,),
            in_specs=[pl.BlockSpec((tb, d_model), lambda b, addr: (b, 0)), whole(idx),
                      whole(wr), whole(wr_back), whole(v_row), hbm, whole(gback)],
            out_specs=[pl.BlockSpec((tb, d_model), lambda b, addr: (b, 0)), pl.BlockSpec((rows, d_model), lambda b, addr: (0, 0)),
                       pl.BlockSpec((LANES, d_model), lambda b, addr: (0, 0))],
            scratch_shapes=[
                pltpu.VMEM((tb // 8 * PITCH, LANES), F32), pltpu.VMEM((n_groups * PITCH, LANES), F32),
                pltpu.VMEM((2, cap, d_model), BF16),
                pltpu.VMEM((LANES, tb), BF16), pltpu.VMEM((8, LANES), F32), pltpu.VMEM((8, LANES), F32),
                pltpu.SemaphoreType.DMA((2,))]),
        compiler_params=pltpu.CompilerParams(vmem_limit_bytes=60 * 2 ** 20),
        name='token_side',
    )(addr, x, idx, wr, wr_back, v_row, dback, gback)


def total_kernel(n_dev, part, out, stats, parts, send_sem, recv_sem):
    me = lax.axis_index('ep')
    barrier = pltpu.get_barrier_semaphore()
    peers = [(me + k) % n_dev for k in range(1, n_dev)]
    for p in peers:
        pl.semaphore_signal(barrier, inc=1, device_id=(p,), device_id_type=MESH)
    pl.semaphore_wait(barrier, n_dev - 1)
    copies = [pltpu.make_async_remote_copy(part, parts.at[me], send_sem.at[k], recv_sem.at[k], device_id=(p,), device_id_type=MESH)
              for k, p in enumerate(peers)]
    for copy in copies:
        copy.start()
    parts[me] = part[...]
    for copy in copies:
        copy.wait()
    total = parts[0]
    for d in range(1, n_dev):
        total = total + parts[d]
    n = out.shape[0]
    out[...] = total[0:n]
    stats[...] = total[n:]


def total_over_devices(n_dev, n_grad, part):
    vmem = pl.BlockSpec(memory_space=pltpu.VMEM)
    return pl.pallas_call(
        lambda *refs: total_kernel(n_dev, *refs),
        out_shape=(jax.ShapeDtypeStruct((n_grad, part.shape[1]), F32), jax.ShapeDtypeStruct((part.shape[0] - n_grad, part.shape[1]), F32)),
        in_specs=[vmem], out_specs=[vmem, vmem],
        scratch_shapes=[pltpu.VMEM((n_dev,) + part.shape, F32), pltpu.SemaphoreType.DMA((n_dev - 1,)), pltpu.SemaphoreType.DMA((n_dev - 1,))],
        compiler_params=pltpu.CompilerParams(collective_id=1, has_side_effects=True),
        name='device_total',
    )(part)


def solution(mesh):
    n_dev = mesh.shape['ep']

    def expert_layer(x_tokens, w_router, expert_idx, w_in, w_out, grad_y):
        tokens, d_model = x_tokens.shape
        n_local = w_in.shape[0]
        num_experts = n_local * n_dev
        capacity = (5 * tokens + 4 * num_experts - 1) // (4 * num_experts)
        total_tok = tokens * n_dev
        tok_slot, counts = route_slots(expert_idx, num_experts, capacity)
        addr = row_address(tok_slot)
        xs, dys = permute(n_dev, n_local, capacity, addr, x_tokens, grad_y)
        w_hi, w_mid, w_low = split3(w_router)
        lanes = ((0, 0), (0, LANES - num_experts))
        wr = jnp.stack([jnp.pad(w, lanes) for w in (w_hi, w_mid, w_low)])
        wr_back = jnp.pad(jnp.concatenate([w.T for w in (w_hi, w_hi, w_hi, w_mid, w_mid, w_low)]), ((0, LANES - 6 * num_experts), (0, 0)))
        cnt = jnp.broadcast_to(jnp.pad(counts.astype(F32), (0, LANES - num_experts))[None], (8, LANES))

        _, _, _, d_back, g_back, gwin, gwout_t, cnt_all = expert_exchange(n_dev, xs, dys, wr, cnt, w_in, w_out)
        load_row = jnp.sum(cnt_all, axis=0) / total_tok
        v_row = AUX_WEIGHT * num_experts * load_row / total_tok
        grad_x, partial, _ = token_side(num_experts, 2.0 * Z_WEIGHT / total_tok, addr, x_tokens, expert_idx, wr, wr_back, v_row, d_back, g_back)
        grad_wr_t, stats = total_over_devices(n_dev, num_experts, partial)
        grad_w_router = grad_wr_t.T
        mean_prob = stats[0, :num_experts] / total_tok
        aux_loss = AUX_WEIGHT * num_experts * jnp.sum(load_row[0, :num_experts] * mean_prob)
        z_loss = Z_WEIGHT * stats[0, LANES] / total_tok
        grad_w_out = jnp.swapaxes(gwout_t, 1, 2)
        return grad_x, gwin, grad_w_out, grad_w_router, aux_loss, z_loss

    return jax.shard_map(expert_layer, mesh=mesh,
                         in_specs=(P('ep', None), P(None, None), P('ep'), P('ep', None, None), P('ep', None, None), P('ep', None)),
                         out_specs=(P('ep', None), P('ep', None, None), P('ep', None, None), P(None, None), P(), P()),
                         check_vma=False)
```

```python
import jax
import jax.numpy as jnp
from jax import lax
from jax.experimental import pallas as pl
from jax.experimental.pallas import tpu as pltpu
from jax.sharding import PartitionSpec as P

AUX_WEIGHT = 0.01
Z_WEIGHT = 0.001
MESH = pl.DeviceIdType.MESH
F32 = jnp.float32
BF16 = jnp.bfloat16
LANES = 128


def route_slots(idx_group, num_experts, capacity):
    onehot = (idx_group[:, None] == jnp.arange(num_experts, dtype=jnp.int32)[None, :]).astype(jnp.int32)
    position = jnp.sum(jnp.cumsum(onehot, axis=0) * onehot, axis=1) - 1
    tok_slot = jnp.where(position < capacity, idx_group * capacity + position, num_experts * capacity)
    return tok_slot, jnp.sum(onehot, axis=0)


def split3(w):
    hi = lax.reduce_precision(w, 8, 7)
    mid = lax.reduce_precision(w - hi, 8, 7)
    return hi.astype(BF16), mid.astype(BF16), (w - hi - mid).astype(BF16)


def nt(a, b):
    return lax.dot_general(a, b, (((1,), (1,)), ((), ())), preferred_element_type=F32)


def nn(a, b):
    return jnp.dot(a, b, preferred_element_type=F32)


def expert_kernel(n_dev, n_local, num_experts, blk, xs, dys, wr, cnt, w_in, w_out,
                  xr, dyr, dsend, dback, dlast, gback, gwin, gwout_t, cnt_all,
                  xv, dyv, gv, x_t, g_t, win_v, wout_v, acc_in, acc_out, o_acc, r_acc, r_out, g_all,
                  x_send, x_recv, dy_send, dy_recv, r_send, r_recv, s_send, s_recv, c_send, c_recv, ld_sem, st_sem, w_sem, flush_sem, own_sem):
    me = lax.axis_index('ep')
    n_blk = w_in.shape[2] // blk
    n_chunk = n_local * n_dev

    def peer_of(k):
        out = 0
        bit = 1
        while bit < n_dev:
            out = out + bit * (((me // bit) + (k // bit)) % 2)
            bit *= 2
        return out

    barrier = pltpu.get_barrier_semaphore()
    for k in range(1, n_dev):
        pl.semaphore_signal(barrier, inc=1, device_id=(peer_of(k),), device_id_type=MESH)
    pl.semaphore_wait(barrier, n_dev - 1)

    def x_copy(k, e):
        p = peer_of(k)
        return pltpu.make_async_remote_copy(xs.at[p, e], xr.at[me, e], x_send.at[e, k], x_recv.at[e, k], device_id=(p,), device_id_type=MESH)

    def dy_copy(k, e):
        p = peer_of(k)
        return pltpu.make_async_remote_copy(dys.at[p, e], dyr.at[me, e], dy_send.at[e, k], dy_recv.at[e, k], device_id=(p,), device_id_type=MESH)

    def r_copy(k, e):
        p = peer_of(k)
        return pltpu.make_async_remote_copy(dsend.at[p, e], dback.at[me, e], r_send.at[e, k], r_recv.at[e, k], device_id=(p,), device_id_type=MESH)

    def s_copy(k, e):
        p = peer_of(k)
        return pltpu.make_async_remote_copy(g_all.at[e, k], gback.at[me, e], s_send.at[e, k], s_recv.at[e, k], device_id=(p,), device_id_type=MESH)

    def c_copy(k):
        p = peer_of(k)
        return pltpu.make_async_remote_copy(cnt, cnt_all.at[me], c_send.at[k], c_recv.at[k], device_id=(p,), device_id_type=MESH)

    own_cnt = pltpu.make_async_copy(cnt, cnt_all.at[me], own_sem.at[n_local])
    own_cnt.start()
    for k in range(1, n_dev):
        c_copy(k).start()
    for e in range(n_local):
        for k in (1, 2, 4, 6, 3, 5, 7):
            x_copy(k, e).start()
            dy_copy(k, e).start()

    order = (0, 1, 2, 4, 6, 3, 5, 7)

    def offset_of(i):
        k = i * 0
        for at, val in enumerate(order):
            k = k + jnp.where(i == at, val, 0)
        return k

    def load(e, i, slot, do):
        k = offset_of(i)
        p = peer_of(k)

        @pl.when(i == 0)
        def _():
            do(pltpu.make_async_copy(xs.at[me, e], xv.at[slot], ld_sem.at[slot, 0]))
            do(pltpu.make_async_copy(dys.at[me, e], dyv.at[slot], ld_sem.at[slot, 1]))

        @pl.when(i > 0)
        def _():
            do(pltpu.make_async_copy(xr.at[p, e], xv.at[slot], ld_sem.at[slot, 0]))
            do(pltpu.make_async_copy(dyr.at[p, e], dyv.at[slot], ld_sem.at[slot, 1]))

    def arrive(e, i):
        @pl.when(i > 0)
        def _():
            k = offset_of(i)
            x_copy(k, e).wait_recv()
            dy_copy(k, e).wait_recv()

    def store(c, do):
        e, i = c // n_dev, c % n_dev
        k = offset_of(i)
        p = peer_of(k)

        @pl.when(e == n_local - 1)
        def _():
            do(pltpu.make_async_copy(r_out.at[c % 2], dlast.at[p], st_sem.at[c % 2]))

        @pl.when(e < n_local - 1)
        def _():
            @pl.when(i == 0)
            def _():
                do(pltpu.make_async_copy(r_out.at[c % 2], dback.at[me, e], st_sem.at[c % 2]))

            @pl.when(i > 0)
            def _():
                do(pltpu.make_async_copy(r_out.at[c % 2], dsend.at[p, e], st_sem.at[c % 2]))

    def own_g(e):
        return pltpu.make_async_copy(g_all.at[e, 0], gback.at[me, e], own_sem.at[e])

    def send_back(c):
        e, i = c // n_dev, c % n_dev
        k = offset_of(i)
        store(c, lambda cp: cp.wait())

        @pl.when(i == 0)
        def _():
            own_g(e).start()

        @pl.when(i > 0)
        def _():
            s_copy(k, e).start()

            @pl.when(e < n_local - 1)
            def _():
                r_copy(k, e).start()

    def weights(e):
        return (pltpu.make_async_copy(w_in.at[e], win_v, w_sem.at[0]), pltpu.make_async_copy(w_out.at[e], wout_v, w_sem.at[1]))

    def flush(e):
        return (pltpu.make_async_copy(acc_in, gwin.at[e], flush_sem.at[0]), pltpu.make_async_copy(acc_out, gwout_t.at[e], flush_sem.at[1]))

    for cp in weights(0):
        cp.start()
    load(0, 0, 0, lambda cp: cp.start())

    def chunk(c, _):
        e, i = c // n_dev, c % n_dev
        k = offset_of(i)
        slot = c % 2

        @pl.when(i == 0)
        def _():
            @pl.when(c > 0)
            def _():
                for cp in weights(e):
                    cp.start()
                for cp in flush(e - 1):
                    cp.wait()
            acc_in[...] = jnp.zeros_like(acc_in)
            acc_out[...] = jnp.zeros_like(acc_out)
            for cp in weights(e):
                cp.wait()

        load(e, i, slot, lambda cp: cp.wait())
        x = xv[slot]
        logits = nn(x, wr[0]) + nn(x, wr[1]) + nn(x, wr[2])
        lane = lax.broadcasted_iota(jnp.int32, logits.shape, 1)
        logits = jnp.where(lane < num_experts, logits, -1e30)
        prob = jnp.exp(logits - jnp.max(logits, axis=1, keepdims=True))
        mine = jnp.sum(jnp.where(lane == me * n_local + e, prob, 0.0), axis=1, keepdims=True)
        gate = mine / jnp.sum(prob, axis=1, keepdims=True)
        grad = (gate * dyv[slot].astype(F32)).astype(BF16)
        gv[...] = grad
        x_t[...] = x.T
        g_t[...] = grad.T
        o_acc[...] = jnp.zeros_like(o_acc)
        r_acc[...] = jnp.zeros_like(r_acc)

        def block(f, _):
            @pl.when(f == n_blk - 1)
            def _():
                @pl.when(c + 1 < n_chunk)
                def _():
                    ne, ni = (c + 1) // n_dev, (c + 1) % n_dev
                    arrive(ne, ni)
                    load(ne, ni, 1 - slot, lambda cp: cp.start())

            @pl.when(f == 1)
            def _():
                @pl.when(c > 0)
                def _():
                    send_back(c - 1)

            cols = pl.ds(pl.multiple_of(f * blk, LANES), blk)
            win = win_v[:, cols]
            wout = wout_v[cols, :]
            hidden = jnp.maximum(nn(xv[slot], win), 0.0).astype(BF16)
            d_hidden = nt(gv[...], wout)
            d_pre = jnp.where(hidden > 0, d_hidden, 0.0).astype(BF16)
            o_acc[...] += nn(hidden, wout)
            r_acc[...] += nt(d_pre, win)
            acc_out[:, cols] += nn(g_t[...], hidden)
            acc_in[:, cols] += nn(x_t[...], d_pre)
            return 0

        lax.fori_loop(0, n_blk, block, 0)
        r_out[slot] = r_acc[...].astype(BF16)
        store(c, lambda cp: cp.start())
        g_val = jnp.sum(o_acc[...].astype(BF16).astype(F32) * dyv[slot].astype(F32), axis=1, keepdims=True)
        g_row = jnp.broadcast_to(g_val, (g_val.shape[0], LANES)).T
        g_all[e, k] = g_row[0:1, :]

        @pl.when(i == n_dev - 1)
        def _():
            for cp in flush(e):
                cp.start()
        return 0

    lax.fori_loop(0, n_chunk, chunk, 0)
    send_back(n_chunk - 1)
    for cp in flush(n_local - 1):
        cp.wait()
    own_cnt.wait()
    for k in range(1, n_dev):
        c_copy(k).wait()
    for e in range(n_local):
        own_g(e).wait()
        for k in range(1, n_dev):
            x_copy(k, e).wait_send()
            dy_copy(k, e).wait_send()
            if e < n_local - 1:
                r_copy(k, e).wait()
            s_copy(k, e).wait()


def expert_exchange(n_dev, xs, dys, wr, cnt, w_in, w_out):
    n_local, d_model, d_ff = w_in.shape
    cap = xs.shape[2]
    num_experts = n_dev * n_local
    blk = d_ff // 4
    hbm = pl.BlockSpec(memory_space=pl.ANY)
    vmem = pl.BlockSpec(memory_space=pltpu.VMEM)
    rows = jax.ShapeDtypeStruct(xs.shape, BF16)
    early = jax.ShapeDtypeStruct((n_dev, n_local - 1, cap, d_model), BF16)
    late = jax.ShapeDtypeStruct((n_dev, cap, d_model), BF16)
    g_shape = jax.ShapeDtypeStruct((n_dev, n_local, 1, cap), F32)
    w_shape = jax.ShapeDtypeStruct((n_local, d_model, d_ff), F32)
    dma = pltpu.SemaphoreType.DMA
    pair = (n_local, n_dev)
    return pl.pallas_call(
        lambda *refs: expert_kernel(n_dev, n_local, num_experts, blk, *refs),
        out_shape=(rows, rows, early, early, late, g_shape, w_shape, w_shape, jax.ShapeDtypeStruct((n_dev,) + cnt.shape, F32)),
        in_specs=[hbm, hbm, vmem, vmem, hbm, hbm],
        out_specs=[hbm] * 9,
        scratch_shapes=[
            pltpu.VMEM((2, cap, d_model), BF16), pltpu.VMEM((2, cap, d_model), BF16), pltpu.VMEM((cap, d_model), BF16),
            pltpu.VMEM((d_model, cap), BF16), pltpu.VMEM((d_model, cap), BF16),
            pltpu.VMEM((d_model, d_ff), BF16), pltpu.VMEM((d_ff, d_model), BF16),
            pltpu.VMEM((d_model, d_ff), F32), pltpu.VMEM((d_model, d_ff), F32),
            pltpu.VMEM((cap, d_model), F32), pltpu.VMEM((cap, d_model), F32),
            pltpu.VMEM((2, cap, d_model), BF16), pltpu.VMEM((n_local, n_dev, 1, cap), F32),
            dma(pair), dma(pair), dma(pair), dma(pair), dma(pair), dma(pair), dma(pair), dma(pair), dma((n_dev,)), dma((n_dev,)),
            dma((2, 2)), dma((2,)), dma((2,)), dma((2,)), dma((n_local + 1,)),
        ],
        compiler_params=pltpu.CompilerParams(collective_id=0, has_side_effects=True, vmem_limit_bytes=63 * 2 ** 20),
        name='expert_exchange',
    )(xs, dys, wr, cnt, w_in, w_out)


PITCH = 6 * 8
ROW_TILES = 6


def row_address(slot):
    return (slot // 8) * PITCH + slot % 8


def row(addr, tiles):
    return pl.ds(addr, tiles, stride=8)


def permute_kernel(tb, addr, x_hbm, dy_hbm, xs, dys, inb, stage, table, outb, in_sem, out_sem):
    tokens = x_hbm.shape[0]
    n_out, n_local, cap, d_model = xs.shape
    groups = cap // 8
    tiled = table.reshape(table.shape[0] // PITCH, PITCH, LANES)
    stage3 = stage.reshape(tb // 8, PITCH, LANES)
    n_in = tokens // tb

    def fetch(source, b):
        return pltpu.make_async_copy(source.at[pl.ds(pl.multiple_of(b * tb, tb), tb), :], inb.at[b % 2], in_sem.at[b % 2])

    def emit(sink, c):
        return pltpu.make_async_copy(outb.at[c % 2], sink.at[c // n_local, c % n_local], out_sem.at[c % 2])

    fetch(x_hbm, 0).start()
    table[...] = jnp.zeros_like(table)
    for source, sink, follow in ((x_hbm, xs, dy_hbm), (dy_hbm, dys, None)):
        def scatter(b, _):
            @pl.when(b + 1 < n_in)
            def _():
                fetch(source, b + 1).start()
            if follow is not None:
                @pl.when(b + 1 == n_in)
                def _():
                    fetch(follow, 0).start()
            fetch(source, b).wait()
            for j in range(ROW_TILES):
                part = inb[b % 2, :, j * LANES:(j + 1) * LANES].astype(F32)
                stage3[:, j * 8:(j + 1) * 8, :] = part.reshape(tb // 8, 8, LANES)

            def move(i, _):
                for r in range(32):
                    at = addr[b * tb + i * 32 + r]
                    table[row(at, ROW_TILES), :] = stage[row(i * (4 * PITCH) + (r // 8) * PITCH + r % 8, ROW_TILES), :]
                return 0

            lax.fori_loop(0, tb // 32, move, 0)
            return 0

        lax.fori_loop(0, n_in, scatter, 0)

        def drain(c, _):
            @pl.when(c >= 2)
            def _():
                emit(sink, c - 2).wait()
            for j in range(ROW_TILES):
                part = tiled[pl.ds(c * groups, groups), j * 8:(j + 1) * 8, :].reshape(cap, LANES)
                outb[c % 2, :, j * LANES:(j + 1) * LANES] = part.astype(BF16)
            emit(sink, c).start()
            return 0

        n_chunk = n_out * n_local
        lax.fori_loop(0, n_chunk, drain, 0)
        for c in (n_chunk - 2, n_chunk - 1):
            emit(sink, c).wait()


def permute(n_dev, n_local, capacity, addr, x, dy):
    tokens, d_model = x.shape
    tb = 512
    hbm = pl.BlockSpec(memory_space=pl.ANY)
    out = jax.ShapeDtypeStruct((n_dev, n_local, capacity, d_model), BF16)
    n_groups = n_dev * n_local * capacity // 8 + 1
    return pl.pallas_call(
        lambda *refs: permute_kernel(tb, *refs),
        out_shape=(out, out),
        grid_spec=pltpu.PrefetchScalarGridSpec(
            num_scalar_prefetch=1, grid=(), in_specs=[hbm, hbm], out_specs=[hbm, hbm],
            scratch_shapes=[
                pltpu.VMEM((2, tb, d_model), BF16), pltpu.VMEM((tb // 8 * PITCH, LANES), F32), pltpu.VMEM((n_groups * PITCH, LANES), F32),
                pltpu.VMEM((2, capacity, d_model), BF16), pltpu.SemaphoreType.DMA((2,)), pltpu.SemaphoreType.DMA((2,))]),
        compiler_params=pltpu.CompilerParams(vmem_limit_bytes=60 * 2 ** 20),
        name='permute_rows',
    )(addr, x, dy)


def router_kernel(num_experts, z_coef, slot, x, idx, wr, v_row, gback, pieces_out, partial, acc, gtab, g_rows, pieces_t, p_acc, z_acc):
    b = pl.program_id(0)
    tb = x.shape[0]
    n_chunk, cap = gback.shape

    @pl.when(b == 0)
    def _():
        acc[...] = jnp.zeros_like(acc)
        p_acc[...] = jnp.zeros_like(p_acc)
        z_acc[...] = jnp.zeros_like(z_acc)
        gtab[n_chunk * cap:, :] = jnp.zeros((8, LANES), F32)

        def fill(c, _):
            gtab[pl.ds(pl.multiple_of(c * cap, 8), cap), :] = jnp.broadcast_to(gback[pl.ds(c, 1), :], (LANES, cap)).T
            return 0

        lax.fori_loop(0, n_chunk, fill, 0)

    def move(i, _):
        for r in range(32):
            g_rows[pl.ds(i * 32 + r, 1), :] = gtab[pl.ds(slot[b * tb + i * 32 + r], 1), :]
        return 0

    lax.fori_loop(0, tb // 32, move, 0)

    xv = x[...]
    logits = nn(xv, wr[0]) + nn(xv, wr[1]) + nn(xv, wr[2])
    lane = lax.broadcasted_iota(jnp.int32, logits.shape, 1)
    real = lane < num_experts
    top = jnp.max(jnp.where(real, logits, -1e30), axis=1, keepdims=True)
    expd = jnp.where(real, jnp.exp(jnp.minimum(logits - top, 0.0)), 0.0)
    total = jnp.sum(expd, axis=1, keepdims=True)
    prob = expd / total
    z = top + jnp.log(total)
    mine = jnp.broadcast_to(idx[pl.ds(b, 1), :], (LANES, tb)).T == lane.astype(F32)
    onehot = jnp.where(mine, 1.0, 0.0)
    gate = jnp.sum(jnp.where(mine, prob, 0.0), axis=1, keepdims=True)
    v = v_row[0:1, :]
    spread = jnp.sum(prob * v, axis=1, keepdims=True)
    dlog = gate * g_rows[...] * (onehot - prob) + prob * (v - spread) + (z_coef * z) * prob
    hi = dlog.astype(BF16).astype(F32)
    mid = (dlog - hi).astype(BF16).astype(F32)
    low = dlog - hi - mid

    def at(piece, k):
        return piece if k == 0 else pltpu.roll(piece, k * num_experts, 1)

    pieces = at(hi, 0) + at(mid, 1) + at(low, 2) + at(hi, 3) + at(mid, 4) + at(hi, 5)
    pieces_out[...] = pieces.astype(BF16)
    pieces_t[...] = pieces.T.astype(BF16)
    acc[...] += nn(pieces_t[...], xv)
    p_acc[...] += jnp.sum(prob.reshape(tb // 8, 8, LANES), axis=0)
    z_acc[...] += jnp.sum(jnp.broadcast_to(z * z, (tb, LANES)).reshape(tb // 8, 8, LANES), axis=0)

    @pl.when(b == pl.num_programs(0) - 1)
    def _():
        n = num_experts
        partial[...] = jnp.zeros_like(partial)
        partial[0:n, :] = acc[0:n, :] + acc[n:2 * n, :] + acc[2 * n:3 * n, :]
        partial[n:n + 1, 0:LANES] = jnp.sum(p_acc[...], axis=0, keepdims=True)
        partial[n:n + 1, LANES:2 * LANES] = jnp.sum(z_acc[...], axis=0, keepdims=True)


def whole(a):
    return pl.BlockSpec(a.shape, lambda b, addr: (0,) * a.ndim)


def router_side(num_experts, z_coef, slot, x, idx, wr, v_row, gback):
    tokens, d_model = x.shape
    n_dev, n_local, _, cap = gback.shape
    tb = 512
    idx = idx.astype(F32).reshape(tokens // tb, tb)
    gback = gback.reshape(n_dev * n_local, cap)
    rows = num_experts + 8
    return pl.pallas_call(
        lambda *refs: router_kernel(num_experts, z_coef, *refs),
        out_shape=(jax.ShapeDtypeStruct((tokens, LANES), BF16), jax.ShapeDtypeStruct((rows, d_model), F32), jax.ShapeDtypeStruct((LANES, d_model), F32)),
        grid_spec=pltpu.PrefetchScalarGridSpec(
            num_scalar_prefetch=1, grid=(tokens // tb,),
            in_specs=[pl.BlockSpec((tb, d_model), lambda b, addr: (b, 0)), whole(idx), whole(wr), whole(v_row), whole(gback)],
            out_specs=[pl.BlockSpec((tb, LANES), lambda b, addr: (b, 0)), pl.BlockSpec((rows, d_model), lambda b, addr: (0, 0)),
                       pl.BlockSpec((LANES, d_model), lambda b, addr: (0, 0))],
            scratch_shapes=[
                pltpu.VMEM((n_dev * n_local * cap + 8, LANES), F32), pltpu.VMEM((tb, LANES), F32),
                pltpu.VMEM((LANES, tb), BF16), pltpu.VMEM((8, LANES), F32), pltpu.VMEM((8, LANES), F32)]),
        cost_estimate=pl.CostEstimate(flops=40 * 10 ** 9, bytes_accessed=16 * 2 ** 20, transcendentals=0),
        compiler_params=pltpu.CompilerParams(vmem_limit_bytes=40 * 2 ** 20),
        name='router_side',
    )(slot, x, idx, wr, v_row, gback)


def combine_kernel(addr, pieces, wr_back, dback, dlast, grad_x, stage, table, inb, in_sem):
    b = pl.program_id(0)
    tb = pieces.shape[0]
    n_out, cap, d_model = dlast.shape
    n_local = dback.shape[1] + 1
    groups = cap // 8
    tiled = table.reshape(table.shape[0] // PITCH, PITCH, LANES)
    stage3 = stage.reshape(tb // 8, PITCH, LANES)

    @pl.when(b == 0)
    def _():
        def fetch(d, e):
            source = dback.at[d, e] if e < n_local - 1 else dlast.at[d]
            return pltpu.make_async_copy(source, inb.at[e], in_sem.at[e])

        for e in range(n_local):
            fetch(0, e).start()
        tiled[n_out * n_local * groups] = jnp.zeros((PITCH, LANES), F32)

        def fill(d, _):
            for e in range(n_local):
                fetch(d, e).wait()
                for j in range(ROW_TILES):
                    part = inb[e, :, j * LANES:(j + 1) * LANES].astype(F32)
                    tiled[pl.ds((d * n_local + e) * groups, groups), j * 8:(j + 1) * 8, :] = part.reshape(groups, 8, LANES)

                @pl.when(d + 1 < n_out)
                def _():
                    fetch(d + 1, e).start()
            return 0

        lax.fori_loop(0, n_out, fill, 0)

    def move(i, _):
        for r in range(32):
            at = addr[b * tb + i * 32 + r]
            stage[row(i * (4 * PITCH) + (r // 8) * PITCH + r % 8, ROW_TILES), :] = table[row(at, ROW_TILES), :]
        return 0

    lax.fori_loop(0, tb // 32, move, 0)
    for j in range(ROW_TILES):
        cols = slice(j * LANES, (j + 1) * LANES)
        grad_x[:, cols] = (stage3[:, j * 8:(j + 1) * 8, :].reshape(tb, LANES) + nn(pieces[...], wr_back[:, cols])).astype(BF16)


def combine(addr, pieces, wr_back, dback, dlast):
    tokens = pieces.shape[0]
    n_dev, cap, d_model = dlast.shape
    n_local = dback.shape[1] + 1
    tb = 512
    hbm = pl.BlockSpec(memory_space=pl.ANY)
    n_groups = n_dev * n_local * cap // 8 + 1
    return pl.pallas_call(
        combine_kernel,
        out_shape=jax.ShapeDtypeStruct((tokens, d_model), BF16),
        grid_spec=pltpu.PrefetchScalarGridSpec(
            num_scalar_prefetch=1, grid=(tokens // tb,),
            in_specs=[pl.BlockSpec((tb, LANES), lambda b, addr: (b, 0)), whole(wr_back), hbm, hbm],
            out_specs=pl.BlockSpec((tb, d_model), lambda b, addr: (b, 0)),
            scratch_shapes=[
                pltpu.VMEM((tb // 8 * PITCH, LANES), F32), pltpu.VMEM((n_groups * PITCH, LANES), F32),
                pltpu.VMEM((n_local, cap, d_model), BF16), pltpu.SemaphoreType.DMA((n_local,))]),
        compiler_params=pltpu.CompilerParams(vmem_limit_bytes=56 * 2 ** 20),
        name='combine_rows',
    )(addr, pieces, wr_back, dback, dlast)


def total_kernel(n_dev, part, out, stats, parts, send_sem, recv_sem):
    me = lax.axis_index('ep')
    barrier = pltpu.get_barrier_semaphore()
    peers = [(me + k) % n_dev for k in range(1, n_dev)]
    for p in peers:
        pl.semaphore_signal(barrier, inc=1, device_id=(p,), device_id_type=MESH)
    pl.semaphore_wait(barrier, n_dev - 1)
    copies = [pltpu.make_async_remote_copy(part, parts.at[me], send_sem.at[k], recv_sem.at[k], device_id=(p,), device_id_type=MESH)
              for k, p in enumerate(peers)]
    for copy in copies:
        copy.start()
    parts[me] = part[...]
    for copy in copies:
        copy.wait()
    total = parts[0]
    for d in range(1, n_dev):
        total = total + parts[d]
    n = out.shape[0]
    out[...] = total[0:n]
    stats[...] = total[n:]


def total_over_devices(n_dev, n_grad, part):
    vmem = pl.BlockSpec(memory_space=pltpu.VMEM)
    return pl.pallas_call(
        lambda *refs: total_kernel(n_dev, *refs),
        out_shape=(jax.ShapeDtypeStruct((n_grad, part.shape[1]), F32), jax.ShapeDtypeStruct((part.shape[0] - n_grad, part.shape[1]), F32)),
        in_specs=[vmem], out_specs=[vmem, vmem],
        scratch_shapes=[pltpu.VMEM((n_dev,) + part.shape, F32), pltpu.SemaphoreType.DMA((n_dev - 1,)), pltpu.SemaphoreType.DMA((n_dev - 1,))],
        compiler_params=pltpu.CompilerParams(collective_id=1, has_side_effects=True),
        name='device_total',
    )(part)


def copy_kernel(source, sink):
    sink[...] = source[...]


def own_copy(a):
    n, rows, cols = a.shape
    spec = pl.BlockSpec((1, rows // 6, cols), lambda e, r: (e, r, 0))
    return pl.pallas_call(
        copy_kernel, out_shape=jax.ShapeDtypeStruct(a.shape, a.dtype), grid=(n, 6), in_specs=[spec], out_specs=spec,
        cost_estimate=pl.CostEstimate(flops=15 * 10 ** 9, bytes_accessed=2 * a.size * 4, transcendentals=0),
        name='own_copy')(a)


def solution(mesh):
    n_dev = mesh.shape['ep']

    def expert_layer(x_tokens, w_router, expert_idx, w_in, w_out, grad_y):
        tokens, d_model = x_tokens.shape
        n_local = w_in.shape[0]
        num_experts = n_local * n_dev
        capacity = (5 * tokens + 4 * num_experts - 1) // (4 * num_experts)
        total_tok = tokens * n_dev
        tok_slot, counts = route_slots(expert_idx, num_experts, capacity)
        addr = row_address(tok_slot)
        xs, dys = permute(n_dev, n_local, capacity, addr, x_tokens, grad_y)
        w_hi, w_mid, w_low = split3(w_router)
        lanes = ((0, 0), (0, LANES - num_experts))
        wr = jnp.stack([jnp.pad(w, lanes) for w in (w_hi, w_mid, w_low)])
        wr_back = jnp.pad(jnp.concatenate([w.T for w in (w_hi, w_hi, w_hi, w_mid, w_mid, w_low)]), ((0, LANES - 6 * num_experts), (0, 0)))
        cnt = jnp.broadcast_to(jnp.pad(counts.astype(F32), (0, LANES - num_experts))[None], (8, LANES))

        _, _, _, d_back, d_last, g_back, gwin, gwout_t, cnt_all = expert_exchange(n_dev, xs, dys, wr, cnt, w_in, w_out)
        d_last = lax.all_to_all(d_last, 'ep', 0, 0, tiled=True)
        load_row = jnp.sum(cnt_all, axis=0) / total_tok
        v_row = AUX_WEIGHT * num_experts * load_row / total_tok
        pieces, partial, _ = router_side(num_experts, 2.0 * Z_WEIGHT / total_tok, tok_slot, x_tokens, expert_idx, wr, v_row, g_back)
        grad_w_out = jnp.swapaxes(gwout_t, 1, 2)
        grad_w_in = own_copy(gwin)
        pieces, partial, grad_w_in, grad_w_out = lax.optimization_barrier((pieces, partial, grad_w_in, grad_w_out))
        grad_x = combine(addr, pieces, wr_back, d_back, d_last)
        grad_wr_t, stats = total_over_devices(n_dev, num_experts, partial)
        grad_w_router = grad_wr_t.T
        mean_prob = stats[0, :num_experts] / total_tok
        aux_loss = AUX_WEIGHT * num_experts * jnp.sum(load_row[0, :num_experts] * mean_prob)
        z_loss = Z_WEIGHT * stats[0, LANES] / total_tok
        return grad_x, grad_w_in, grad_w_out, grad_w_router, aux_loss, z_loss

    return jax.shard_map(expert_layer, mesh=mesh,
                         in_specs=(P('ep', None), P(None, None), P('ep'), P('ep', None, None), P('ep', None, None), P('ep', None)),
                         out_specs=(P('ep', None), P('ep', None, None), P('ep', None, None), P(None, None), P(), P()),
                         check_vma=False)
```

```python
import jax
import jax.numpy as jnp
from jax import lax
from jax.experimental import pallas as pl
from jax.experimental.pallas import tpu as pltpu
from jax.sharding import PartitionSpec as P

AUX_WEIGHT = 0.01
Z_WEIGHT = 0.001
MESH = pl.DeviceIdType.MESH
F32 = jnp.float32
BF16 = jnp.bfloat16
LANES = 128


def route_slots(idx_group, num_experts, capacity):
    onehot = (idx_group[:, None] == jnp.arange(num_experts, dtype=jnp.int32)[None, :]).astype(jnp.int32)
    position = jnp.sum(jnp.cumsum(onehot, axis=0) * onehot, axis=1) - 1
    tok_slot = jnp.where(position < capacity, idx_group * capacity + position, num_experts * capacity)
    return tok_slot, jnp.sum(onehot, axis=0)


def split3(w):
    hi = w.astype(BF16).astype(F32)
    mid = (w - hi).astype(BF16).astype(F32)
    return hi, mid, w - hi - mid


def six_terms(w):
    hi, mid, low = split3(w)
    pad = jnp.zeros((LANES - 6 * w.shape[0], w.shape[1]), F32)
    return jnp.concatenate([hi, hi, hi, mid, mid, low, pad], axis=0).astype(BF16)


def nt(a, b):
    return lax.dot_general(a, b, (((1,), (1,)), ((), ())), preferred_element_type=F32)


def nn(a, b):
    return jnp.dot(a, b, preferred_element_type=F32)


def expert_kernel(n_dev, n_local, num_experts, blk, xs, dys, w_t, cnt, w_in, w_out,
                  xr, dyr, dsend, dback, dlast, gback, gwin, gwout_t, cnt_all,
                  xv, dyv, gv, x_t, g_t, wr, win_v, wout_v, acc_in, acc_out, o_acc, r_acc, r_out, g_all,
                  x_send, x_recv, dy_send, dy_recv, r_send, r_recv, s_send, s_recv, c_send, c_recv, ld_sem, st_sem, w_sem, flush_sem, own_sem):
    me = lax.axis_index('ep')
    n_blk = w_in.shape[2] // blk
    n_chunk = n_local * n_dev

    def peer_of(k):
        out = 0
        bit = 1
        while bit < n_dev:
            out = out + bit * (((me // bit) + (k // bit)) % 2)
            bit *= 2
        return out

    barrier = pltpu.get_barrier_semaphore()
    for k in range(1, n_dev):
        pl.semaphore_signal(barrier, inc=1, device_id=(peer_of(k),), device_id_type=MESH)
    pl.semaphore_wait(barrier, n_dev - 1)

    def x_copy(k, e):
        p = peer_of(k)
        return pltpu.make_async_remote_copy(xs.at[p, e], xr.at[me, e], x_send.at[e, k], x_recv.at[e, k], device_id=(p,), device_id_type=MESH)

    def dy_copy(k, e):
        p = peer_of(k)
        return pltpu.make_async_remote_copy(dys.at[p, e], dyr.at[me, e], dy_send.at[e, k], dy_recv.at[e, k], device_id=(p,), device_id_type=MESH)

    def r_copy(k, e):
        p = peer_of(k)
        return pltpu.make_async_remote_copy(dsend.at[p, e], dback.at[me, e], r_send.at[e, k], r_recv.at[e, k], device_id=(p,), device_id_type=MESH)

    def s_copy(k, e):
        p = peer_of(k)
        return pltpu.make_async_remote_copy(g_all.at[e, k], gback.at[me, e], s_send.at[e, k], s_recv.at[e, k], device_id=(p,), device_id_type=MESH)

    def c_copy(k):
        p = peer_of(k)
        return pltpu.make_async_remote_copy(cnt, cnt_all.at[me], c_send.at[k], c_recv.at[k], device_id=(p,), device_id_type=MESH)

    own_cnt = pltpu.make_async_copy(cnt, cnt_all.at[me], own_sem.at[n_local])
    own_cnt.start()
    for k in range(1, n_dev):
        c_copy(k).start()
    for e in range(n_local):
        for k in (1, 2, 4, 6, 3, 5, 7):
            x_copy(k, e).start()
            dy_copy(k, e).start()

    order = (0, 1, 2, 4, 6, 3, 5, 7)

    def offset_of(i):
        k = i * 0
        for at, val in enumerate(order):
            k = k + jnp.where(i == at, val, 0)
        return k

    def load(e, i, slot, do):
        k = offset_of(i)
        p = peer_of(k)

        @pl.when(i == 0)
        def _():
            do(pltpu.make_async_copy(xs.at[me, e], xv.at[slot], ld_sem.at[slot, 0]))
            do(pltpu.make_async_copy(dys.at[me, e], dyv.at[slot], ld_sem.at[slot, 1]))

        @pl.when(i > 0)
        def _():
            do(pltpu.make_async_copy(xr.at[p, e], xv.at[slot], ld_sem.at[slot, 0]))
            do(pltpu.make_async_copy(dyr.at[p, e], dyv.at[slot], ld_sem.at[slot, 1]))

    def arrive(e, i):
        @pl.when(i > 0)
        def _():
            k = offset_of(i)
            x_copy(k, e).wait_recv()
            dy_copy(k, e).wait_recv()

    def store(c, do):
        e, i = c // n_dev, c % n_dev
        k = offset_of(i)
        p = peer_of(k)

        @pl.when(e == n_local - 1)
        def _():
            do(pltpu.make_async_copy(r_out.at[c % 2], dlast.at[p], st_sem.at[c % 2]))

        @pl.when(e < n_local - 1)
        def _():
            @pl.when(i == 0)
            def _():
                do(pltpu.make_async_copy(r_out.at[c % 2], dback.at[me, e], st_sem.at[c % 2]))

            @pl.when(i > 0)
            def _():
                do(pltpu.make_async_copy(r_out.at[c % 2], dsend.at[p, e], st_sem.at[c % 2]))

    def own_g(e):
        return pltpu.make_async_copy(g_all.at[e, 0], gback.at[me, e], own_sem.at[e])

    def send_back(c):
        e, i = c // n_dev, c % n_dev
        k = offset_of(i)
        store(c, lambda cp: cp.wait())

        @pl.when(i == 0)
        def _():
            own_g(e).start()

        @pl.when(i > 0)
        def _():
            s_copy(k, e).start()

            @pl.when(e < n_local - 1)
            def _():
                r_copy(k, e).start()

    def weights(e):
        return (pltpu.make_async_copy(w_in.at[e], win_v, w_sem.at[0]), pltpu.make_async_copy(w_out.at[e], wout_v, w_sem.at[1]))

    def flush(e):
        return (pltpu.make_async_copy(acc_in, gwin.at[e], flush_sem.at[0]), pltpu.make_async_copy(acc_out, gwout_t.at[e], flush_sem.at[1]))

    for cp in weights(0):
        cp.start()
    load(0, 0, 0, lambda cp: cp.start())
    for at, piece in enumerate(split3(w_t[...])):
        pad = jnp.zeros((LANES - num_experts, piece.shape[1]), F32)
        wr[at] = jnp.concatenate([piece, pad], axis=0).T.astype(BF16)

    def chunk(c, _):
        e, i = c // n_dev, c % n_dev
        k = offset_of(i)
        slot = c % 2

        @pl.when(i == 0)
        def _():
            @pl.when(c > 0)
            def _():
                for cp in weights(e):
                    cp.start()
                for cp in flush(e - 1):
                    cp.wait()
            acc_in[...] = jnp.zeros_like(acc_in)
            acc_out[...] = jnp.zeros_like(acc_out)
            for cp in weights(e):
                cp.wait()

        load(e, i, slot, lambda cp: cp.wait())
        x = xv[slot]
        logits = nn(x, wr[0]) + nn(x, wr[1]) + nn(x, wr[2])
        lane = lax.broadcasted_iota(jnp.int32, logits.shape, 1)
        logits = jnp.where(lane < num_experts, logits, -1e30)
        prob = jnp.exp(logits - jnp.max(logits, axis=1, keepdims=True))
        mine = jnp.sum(jnp.where(lane == me * n_local + e, prob, 0.0), axis=1, keepdims=True)
        gate = mine / jnp.sum(prob, axis=1, keepdims=True)
        grad = (gate * dyv[slot].astype(F32)).astype(BF16)
        gv[...] = grad
        x_t[...] = x.T
        g_t[...] = grad.T
        o_acc[...] = jnp.zeros_like(o_acc)
        r_acc[...] = jnp.zeros_like(r_acc)

        def block(f, _):
            @pl.when(f == n_blk - 1)
            def _():
                @pl.when(c + 1 < n_chunk)
                def _():
                    ne, ni = (c + 1) // n_dev, (c + 1) % n_dev
                    arrive(ne, ni)
                    load(ne, ni, 1 - slot, lambda cp: cp.start())

            @pl.when(f == 1)
            def _():
                @pl.when(c > 0)
                def _():
                    send_back(c - 1)

            cols = pl.ds(pl.multiple_of(f * blk, LANES), blk)
            win = win_v[:, cols]
            wout = wout_v[cols, :]
            hidden = jnp.maximum(nn(xv[slot], win), 0.0).astype(BF16)
            d_hidden = nt(gv[...], wout)
            d_pre = jnp.where(hidden > 0, d_hidden, 0.0).astype(BF16)
            o_acc[...] += nn(hidden, wout)
            r_acc[...] += nt(d_pre, win)
            acc_out[:, cols] += nn(g_t[...], hidden)
            acc_in[:, cols] += nn(x_t[...], d_pre)
            return 0

        lax.fori_loop(0, n_blk, block, 0)
        r_out[slot] = r_acc[...].astype(BF16)
        store(c, lambda cp: cp.start())
        g_val = jnp.sum(o_acc[...].astype(BF16).astype(F32) * dyv[slot].astype(F32), axis=1, keepdims=True)
        g_row = jnp.broadcast_to(g_val, (g_val.shape[0], LANES)).T
        g_all[e, k] = g_row[0:1, :]

        @pl.when(i == n_dev - 1)
        def _():
            for cp in flush(e):
                cp.start()
        return 0

    lax.fori_loop(0, n_chunk, chunk, 0)
    send_back(n_chunk - 1)
    for cp in flush(n_local - 1):
        cp.wait()
    own_cnt.wait()
    for k in range(1, n_dev):
        c_copy(k).wait()
    for e in range(n_local):
        own_g(e).wait()
        for k in range(1, n_dev):
            x_copy(k, e).wait_send()
            dy_copy(k, e).wait_send()
            if e < n_local - 1:
                r_copy(k, e).wait()
            s_copy(k, e).wait()


def expert_exchange(n_dev, xs, dys, w_t, cnt, w_in, w_out):
    n_local, d_model, d_ff = w_in.shape
    cap = xs.shape[2]
    num_experts = n_dev * n_local
    blk = d_ff // 4
    hbm = pl.BlockSpec(memory_space=pl.ANY)
    vmem = pl.BlockSpec(memory_space=pltpu.VMEM)
    rows = jax.ShapeDtypeStruct(xs.shape, BF16)
    early = jax.ShapeDtypeStruct((n_dev, n_local - 1, cap, d_model), BF16)
    late = jax.ShapeDtypeStruct((n_dev, cap, d_model), BF16)
    g_shape = jax.ShapeDtypeStruct((n_dev, n_local, 1, cap), F32)
    w_shape = jax.ShapeDtypeStruct((n_local, d_model, d_ff), F32)
    dma = pltpu.SemaphoreType.DMA
    pair = (n_local, n_dev)
    return pl.pallas_call(
        lambda *refs: expert_kernel(n_dev, n_local, num_experts, blk, *refs),
        out_shape=(rows, rows, early, early, late, g_shape, w_shape, w_shape, jax.ShapeDtypeStruct((n_dev,) + cnt.shape, F32)),
        in_specs=[hbm, hbm, vmem, vmem, hbm, hbm],
        out_specs=[hbm] * 9,
        scratch_shapes=[
            pltpu.VMEM((2, cap, d_model), BF16), pltpu.VMEM((2, cap, d_model), BF16), pltpu.VMEM((cap, d_model), BF16),
            pltpu.VMEM((d_model, cap), BF16), pltpu.VMEM((d_model, cap), BF16), pltpu.VMEM((3, d_model, LANES), BF16),
            pltpu.VMEM((d_model, d_ff), BF16), pltpu.VMEM((d_ff, d_model), BF16),
            pltpu.VMEM((d_model, d_ff), F32), pltpu.VMEM((d_model, d_ff), F32),
            pltpu.VMEM((cap, d_model), F32), pltpu.VMEM((cap, d_model), F32),
            pltpu.VMEM((2, cap, d_model), BF16), pltpu.VMEM((n_local, n_dev, 1, cap), F32),
            dma(pair), dma(pair), dma(pair), dma(pair), dma(pair), dma(pair), dma(pair), dma(pair), dma((n_dev,)), dma((n_dev,)),
            dma((2, 2)), dma((2,)), dma((2,)), dma((2,)), dma((n_local + 1,)),
        ],
        compiler_params=pltpu.CompilerParams(collective_id=0, has_side_effects=True, vmem_limit_bytes=63 * 2 ** 20),
        name='expert_exchange',
    )(xs, dys, w_t, cnt, w_in, w_out)


PITCH = 6 * 8
ROW_TILES = 6


def row_address(slot):
    return (slot // 8) * PITCH + slot % 8


def row(addr, tiles):
    return pl.ds(addr, tiles, stride=8)


def permute_kernel(tb, addr, x_hbm, dy_hbm, xs, dys, inb, stage, table, outb, in_sem, out_sem):
    tokens = x_hbm.shape[0]
    n_out, n_local, cap, d_model = xs.shape
    groups = cap // 8
    tiled = table.reshape(table.shape[0] // PITCH, PITCH, LANES)
    stage3 = stage.reshape(tb // 8, PITCH, LANES)
    n_in = tokens // tb

    n_buf = inb.shape[0]
    n_chunk = n_out * n_local

    def fetch(source, b):
        return pltpu.make_async_copy(source.at[pl.ds(pl.multiple_of(b * tb, tb), tb), :], inb.at[b % n_buf], in_sem.at[b % n_buf])

    def emit(sink, c):
        return pltpu.make_async_copy(outb.at[c], sink.at[c // n_local, c % n_local], out_sem.at[c])

    for b in range(n_buf - 1):
        fetch(x_hbm, b).start()
    table[...] = jnp.zeros_like(table)
    for source, sink, follow, before in ((x_hbm, xs, dy_hbm, None), (dy_hbm, dys, None, xs)):
        def scatter(b, _):
            ahead = b + n_buf - 1

            @pl.when(ahead < n_in)
            def _():
                fetch(source, ahead).start()
            if follow is not None:
                @pl.when(ahead >= n_in)
                def _():
                    fetch(follow, ahead - n_in).start()
            fetch(source, b).wait()
            for j in range(ROW_TILES):
                part = inb[b % n_buf, :, j * LANES:(j + 1) * LANES].astype(F32)
                stage3[:, j * 8:(j + 1) * 8, :] = part.reshape(tb // 8, 8, LANES)

            def move(i, _):
                for r in range(32):
                    at = addr[b * tb + i * 32 + r]
                    table[row(at, ROW_TILES), :] = stage[row(i * (4 * PITCH) + (r // 8) * PITCH + r % 8, ROW_TILES), :]
                return 0

            lax.fori_loop(0, tb // 32, move, 0)
            return 0

        lax.fori_loop(0, n_in, scatter, 0)

        def drain(c, _):
            if before is not None:
                emit(before, c).wait()
            for j in range(ROW_TILES):
                part = tiled[pl.ds(c * groups, groups), j * 8:(j + 1) * 8, :].reshape(cap, LANES)
                outb[c, :, j * LANES:(j + 1) * LANES] = part.astype(BF16)
            emit(sink, c).start()
            return 0

        lax.fori_loop(0, n_chunk, drain, 0)

    def finish(c, _):
        emit(dys, c).wait()
        return 0

    lax.fori_loop(0, n_chunk, finish, 0)


def permute(n_dev, n_local, capacity, addr, x, dy):
    tokens, d_model = x.shape
    tb = 512
    hbm = pl.BlockSpec(memory_space=pl.ANY)
    out = jax.ShapeDtypeStruct((n_dev, n_local, capacity, d_model), BF16)
    n_groups = n_dev * n_local * capacity // 8 + 1
    return pl.pallas_call(
        lambda *refs: permute_kernel(tb, *refs),
        out_shape=(out, out),
        grid_spec=pltpu.PrefetchScalarGridSpec(
            num_scalar_prefetch=1, grid=(), in_specs=[hbm, hbm], out_specs=[hbm, hbm],
            scratch_shapes=[
                pltpu.VMEM((4, tb, d_model), BF16), pltpu.VMEM((tb // 8 * PITCH, LANES), F32), pltpu.VMEM((n_groups * PITCH, LANES), F32),
                pltpu.VMEM((n_dev * n_local, capacity, d_model), BF16), pltpu.SemaphoreType.DMA((4,)), pltpu.SemaphoreType.DMA((n_dev * n_local,))]),
        compiler_params=pltpu.CompilerParams(vmem_limit_bytes=60 * 2 ** 20),
        name='permute_rows',
    )(addr, x, dy)


def router_kernel(z_coef, slot, x, idx, w_t, v_col, gback, pieces_out, partial, acc, gtab, g_rows, w_six, pieces_t, p_acc, z_acc):
    b = pl.program_id(0)
    tb = x.shape[0]
    n_chunk, cap = gback.shape
    n = w_t.shape[0]

    @pl.when(b == 0)
    def _():
        acc[...] = jnp.zeros_like(acc)
        p_acc[...] = jnp.zeros_like(p_acc)
        z_acc[...] = jnp.zeros_like(z_acc)
        w_six[...] = six_terms(w_t[...])
        gtab[n_chunk * cap:, :] = jnp.zeros((8, LANES), F32)

        def fill(c, _):
            gtab[pl.ds(pl.multiple_of(c * cap, 8), cap), :] = jnp.broadcast_to(gback[pl.ds(c, 1), :], (LANES, cap)).T
            return 0

        lax.fori_loop(0, n_chunk, fill, 0)

    def move(i, _):
        for r in range(32):
            g_rows[pl.ds(i * 32 + r, 1), :] = gtab[pl.ds(slot[b * tb + i * 32 + r], 1), :]
        return 0

    lax.fori_loop(0, tb // 32, move, 0)

    xv = x[...]
    terms = nt(w_six[...], xv)
    logits = terms[0:n] + terms[3 * n:4 * n] + terms[5 * n:6 * n]
    top = jnp.max(logits, axis=0, keepdims=True)
    expd = jnp.exp(logits - top)
    total = jnp.sum(expd, axis=0, keepdims=True)
    prob = expd / total
    z = top + jnp.log(total)
    mine = lax.broadcasted_iota(jnp.int32, logits.shape, 0).astype(F32) == idx[pl.ds(b, 1), :]
    onehot = jnp.where(mine, 1.0, 0.0)
    gate = jnp.sum(jnp.where(mine, prob, 0.0), axis=0, keepdims=True)
    g = g_rows[...].T[0:1, :]
    v = v_col[:, 0:1]
    spread = jnp.sum(prob * v, axis=0, keepdims=True)
    dlog = gate * g * (onehot - prob) + prob * (v - spread) + (z_coef * z) * prob
    hi, mid, low = split3(dlog)
    pieces = jnp.concatenate([hi, mid, low, hi, mid, hi, jnp.zeros((LANES - 6 * n, tb), F32)], axis=0)
    pieces_out[...] = pieces.T.astype(BF16)
    pieces_t[...] = pieces.astype(BF16)
    acc[...] += nn(pieces_t[...], xv)
    zz = z * z
    for j in range(tb // LANES):
        p_acc[...] += prob[:, j * LANES:(j + 1) * LANES]
        z_acc[0:1, :] += zz[:, j * LANES:(j + 1) * LANES]

    @pl.when(b == pl.num_programs(0) - 1)
    def _():
        partial[...] = jnp.zeros_like(partial)
        partial[0:n, :] = acc[0:n, :] + acc[n:2 * n, :] + acc[2 * n:3 * n, :]
        p_sum = jnp.broadcast_to(jnp.sum(p_acc[...], axis=1, keepdims=True), p_acc.shape)
        p_full = jnp.concatenate([p_sum, jnp.zeros((LANES - n, LANES), F32)], axis=0).T
        partial[n:n + 1, 0:LANES] = p_full[0:1, :]
        partial[n:n + 1, LANES:2 * LANES] = jnp.broadcast_to(jnp.sum(z_acc[0:1, :], axis=1, keepdims=True), (1, LANES))


def whole(a):
    return pl.BlockSpec(a.shape, lambda b, addr: (0,) * a.ndim)


def router_side(z_coef, slot, x, idx, w_t, v_col, gback):
    tokens, d_model = x.shape
    n_dev, n_local, _, cap = gback.shape
    tb = 512
    n = w_t.shape[0]
    idx = idx.astype(F32).reshape(tokens // tb, tb)
    gback = gback.reshape(n_dev * n_local, cap)
    rows = n + 8
    return pl.pallas_call(
        lambda *refs: router_kernel(z_coef, *refs),
        out_shape=(jax.ShapeDtypeStruct((tokens, LANES), BF16), jax.ShapeDtypeStruct((rows, d_model), F32), jax.ShapeDtypeStruct((LANES, d_model), F32)),
        grid_spec=pltpu.PrefetchScalarGridSpec(
            num_scalar_prefetch=1, grid=(tokens // tb,),
            in_specs=[pl.BlockSpec((tb, d_model), lambda b, addr: (b, 0)), whole(idx), whole(w_t), whole(v_col), whole(gback)],
            out_specs=[pl.BlockSpec((tb, LANES), lambda b, addr: (b, 0)), pl.BlockSpec((rows, d_model), lambda b, addr: (0, 0)),
                       pl.BlockSpec((LANES, d_model), lambda b, addr: (0, 0))],
            scratch_shapes=[
                pltpu.VMEM((n_dev * n_local * cap + 8, LANES), F32), pltpu.VMEM((tb, LANES), F32), pltpu.VMEM((LANES, d_model), BF16),
                pltpu.VMEM((LANES, tb), BF16), pltpu.VMEM((n, LANES), F32), pltpu.VMEM((8, LANES), F32)]),
        cost_estimate=pl.CostEstimate(flops=30 * 10 ** 9, bytes_accessed=16 * 2 ** 20, transcendentals=0),
        compiler_params=pltpu.CompilerParams(vmem_limit_bytes=40 * 2 ** 20),
        name='router_side',
    )(slot, x, idx, w_t, v_col, gback)


def combine_kernel(addr, pieces, w_t, dback, dlast, grad_x, stage, table, inb, w_six, in_sem):
    b = pl.program_id(0)
    tb = pieces.shape[0]
    n_out, cap, d_model = dlast.shape
    n_local = dback.shape[1] + 1
    groups = cap // 8
    tiled = table.reshape(table.shape[0] // PITCH, PITCH, LANES)
    stage3 = stage.reshape(tb // 8, PITCH, LANES)

    @pl.when(b == 0)
    def _():
        n_buf = inb.shape[1]

        def fetch(d, e):
            source = dback.at[d, e] if e < n_local - 1 else dlast.at[d]
            return pltpu.make_async_copy(source, inb.at[e, d % n_buf], in_sem.at[e, d % n_buf])

        for d in range(n_buf):
            for e in range(n_local):
                fetch(d, e).start()
        w_six[...] = six_terms(w_t[...])
        tiled[n_out * n_local * groups] = jnp.zeros((PITCH, LANES), F32)

        def fill(d, _):
            for e in range(n_local):
                fetch(d, e).wait()
                for j in range(ROW_TILES):
                    part = inb[e, d % n_buf, :, j * LANES:(j + 1) * LANES].astype(F32)
                    tiled[pl.ds((d * n_local + e) * groups, groups), j * 8:(j + 1) * 8, :] = part.reshape(groups, 8, LANES)

                @pl.when(d + n_buf < n_out)
                def _():
                    fetch(d + n_buf, e).start()
            return 0

        lax.fori_loop(0, n_out, fill, 0)

    def move(i, _):
        for r in range(32):
            at = addr[b * tb + i * 32 + r]
            stage[row(i * (4 * PITCH) + (r // 8) * PITCH + r % 8, ROW_TILES), :] = table[row(at, ROW_TILES), :]
        return 0

    lax.fori_loop(0, tb // 32, move, 0)
    for j in range(ROW_TILES):
        cols = slice(j * LANES, (j + 1) * LANES)
        grad_x[:, cols] = (stage3[:, j * 8:(j + 1) * 8, :].reshape(tb, LANES) + nn(pieces[...], w_six[:, cols])).astype(BF16)


def combine(addr, pieces, w_t, dback, dlast):
    tokens = pieces.shape[0]
    n_dev, cap, d_model = dlast.shape
    n_local = dback.shape[1] + 1
    tb = 512
    hbm = pl.BlockSpec(memory_space=pl.ANY)
    n_groups = n_dev * n_local * cap // 8 + 1
    return pl.pallas_call(
        combine_kernel,
        out_shape=jax.ShapeDtypeStruct((tokens, d_model), BF16),
        grid_spec=pltpu.PrefetchScalarGridSpec(
            num_scalar_prefetch=1, grid=(tokens // tb,),
            in_specs=[pl.BlockSpec((tb, LANES), lambda b, addr: (b, 0)), whole(w_t), hbm, hbm],
            out_specs=pl.BlockSpec((tb, d_model), lambda b, addr: (b, 0)),
            scratch_shapes=[
                pltpu.VMEM((tb // 8 * PITCH, LANES), F32), pltpu.VMEM((n_groups * PITCH, LANES), F32),
                pltpu.VMEM((n_local, 4, cap, d_model), BF16), pltpu.VMEM((LANES, d_model), BF16), pltpu.SemaphoreType.DMA((n_local, 4))]),
        compiler_params=pltpu.CompilerParams(vmem_limit_bytes=56 * 2 ** 20),
        name='combine_rows',
    )(addr, pieces, w_t, dback, dlast)


def total_kernel(n_dev, part, _before_a, _before_b, out, stats, parts, send_sem, recv_sem):
    me = lax.axis_index('ep')
    barrier = pltpu.get_barrier_semaphore()
    peers = [(me + k) % n_dev for k in range(1, n_dev)]
    for p in peers:
        pl.semaphore_signal(barrier, inc=1, device_id=(p,), device_id_type=MESH)
    pl.semaphore_wait(barrier, n_dev - 1)
    copies = [pltpu.make_async_remote_copy(part, parts.at[me], send_sem.at[k], recv_sem.at[k], device_id=(p,), device_id_type=MESH)
              for k, p in enumerate(peers)]
    for copy in copies:
        copy.start()
    parts[me] = part[...]
    for copy in copies:
        copy.wait()
    total = parts[0]
    for d in range(1, n_dev):
        total = total + parts[d]
    n = out.shape[0]
    out[...] = total[0:n]
    stats[...] = total[n:]


def total_over_devices(n_dev, n_grad, part, before):
    vmem = pl.BlockSpec(memory_space=pltpu.VMEM)
    return pl.pallas_call(
        lambda *refs: total_kernel(n_dev, *refs),
        out_shape=(jax.ShapeDtypeStruct((n_grad, part.shape[1]), F32), jax.ShapeDtypeStruct((part.shape[0] - n_grad, part.shape[1]), F32)),
        in_specs=[vmem] + [pl.BlockSpec(memory_space=pl.ANY)] * 2, out_specs=[vmem, vmem],
        scratch_shapes=[pltpu.VMEM((n_dev,) + part.shape, F32), pltpu.SemaphoreType.DMA((n_dev - 1,)), pltpu.SemaphoreType.DMA((n_dev - 1,))],
        compiler_params=pltpu.CompilerParams(collective_id=1, has_side_effects=True),
        name='device_total',
    )(part, *before)


def copy_kernel(source, sink):
    sink[...] = source[...]


def own_copy(a):
    n, rows, cols = a.shape
    spec = pl.BlockSpec((1, rows // 6, cols), lambda e, r: (e, r, 0))
    return pl.pallas_call(
        copy_kernel, out_shape=jax.ShapeDtypeStruct(a.shape, a.dtype), grid=(n, 6), in_specs=[spec], out_specs=spec,
        cost_estimate=pl.CostEstimate(flops=15 * 10 ** 9, bytes_accessed=2 * a.size * 4, transcendentals=0),
        name='own_copy')(a)


def solution(mesh):
    n_dev = mesh.shape['ep']

    def expert_layer(x_tokens, w_router, expert_idx, w_in, w_out, grad_y):
        tokens, d_model = x_tokens.shape
        n_local = w_in.shape[0]
        num_experts = n_local * n_dev
        capacity = (5 * tokens + 4 * num_experts - 1) // (4 * num_experts)
        total_tok = tokens * n_dev
        tok_slot, counts = route_slots(expert_idx, num_experts, capacity)
        addr = row_address(tok_slot)
        xs, dys = permute(n_dev, n_local, capacity, addr, x_tokens, grad_y)
        w_t = w_router.T
        cnt = jnp.broadcast_to(jnp.pad(counts.astype(F32), (0, LANES - num_experts))[None], (8, LANES))

        _, _, _, d_back, d_last, g_back, gwin, gwout_t, cnt_all = expert_exchange(n_dev, xs, dys, w_t, cnt, w_in, w_out)
        d_last = lax.all_to_all(d_last, 'ep', 0, 0, tiled=True)
        load_row = jnp.sum(cnt_all, axis=0) / total_tok
        v_col = jnp.broadcast_to((AUX_WEIGHT * num_experts * load_row[0, :num_experts] / total_tok)[:, None], (num_experts, LANES))
        pieces, partial, _ = router_side(2.0 * Z_WEIGHT / total_tok, tok_slot, x_tokens, expert_idx, w_t, v_col, g_back)
        grad_w_out = jnp.swapaxes(gwout_t, 1, 2)
        grad_w_in = own_copy(gwin)
        grad_x = combine(addr, pieces, w_t, d_back, d_last)
        grad_wr_t, stats = total_over_devices(n_dev, num_experts, partial, (grad_w_in, grad_w_out))
        grad_w_router = grad_wr_t.T
        mean_prob = stats[0, :num_experts] / total_tok
        aux_loss = AUX_WEIGHT * num_experts * jnp.sum(load_row[0, :num_experts] * mean_prob)
        z_loss = Z_WEIGHT * stats[0, LANES] / total_tok
        return grad_x, grad_w_in, grad_w_out, grad_w_router, aux_loss, z_loss

    return jax.shard_map(expert_layer, mesh=mesh,
                         in_specs=(P('ep', None), P(None, None), P('ep'), P('ep', None, None), P('ep', None, None), P('ep', None)),
                         out_specs=(P('ep', None), P('ep', None, None), P('ep', None, None), P(None, None), P(), P()),
                         check_vma=False)
```

```python
import jax
import jax.numpy as jnp
from jax import lax
from jax.experimental import pallas as pl
from jax.experimental.pallas import tpu as pltpu
from jax.sharding import PartitionSpec as P

AUX_WEIGHT = 0.01
Z_WEIGHT = 0.001
MESH = pl.DeviceIdType.MESH
F32 = jnp.float32
BF16 = jnp.bfloat16
LANES = 128


def split3(w):
    hi = w.astype(BF16).astype(F32)
    mid = (w - hi).astype(BF16).astype(F32)
    return hi, mid, w - hi - mid


def six_terms(w):
    hi, mid, low = split3(w)
    pad = jnp.zeros((LANES - 6 * w.shape[0], w.shape[1]), F32)
    return jnp.concatenate([hi, hi, hi, mid, mid, low, pad], axis=0).astype(BF16)


def nt(a, b):
    return lax.dot_general(a, b, (((1,), (1,)), ((), ())), preferred_element_type=F32)


def nn(a, b):
    return jnp.dot(a, b, preferred_element_type=F32)


EARLY = ((0, 2), (0, 4))


def expert_kernel(n_dev, n_local, num_experts, blk, xs, dys, near_x, near_y, w_t, cnt, w_in, w_out,
                  xr, dyr, dsend, dback, dlast, gback, gwin, gwout_t, cnt_all,
                  xv, dyv, gv, x_t, g_t, wr, win_v, wout_v, acc_in, acc_out, o_acc, r_acc, r_out, g_all,
                  x_send, x_recv, dy_send, dy_recv, r_send, r_recv, s_send, s_recv, c_send, c_recv, ld_sem, st_sem, w_sem, flush_sem, own_sem):
    me = lax.axis_index('ep')
    n_blk = w_in.shape[2] // blk
    n_chunk = n_local * n_dev

    def peer_of(k):
        out = 0
        bit = 1
        while bit < n_dev:
            out = out + bit * (((me // bit) + (k // bit)) % 2)
            bit *= 2
        return out

    barrier = pltpu.get_barrier_semaphore()
    for k in range(1, n_dev):
        pl.semaphore_signal(barrier, inc=1, device_id=(peer_of(k),), device_id_type=MESH)
    pl.semaphore_wait(barrier, n_dev - 1)

    def x_copy(k, e):
        p = peer_of(k)
        return pltpu.make_async_remote_copy(xs.at[p, e], xr.at[me, e], x_send.at[e, k], x_recv.at[e, k], device_id=(p,), device_id_type=MESH)

    def dy_copy(k, e):
        p = peer_of(k)
        return pltpu.make_async_remote_copy(dys.at[p, e], dyr.at[me, e], dy_send.at[e, k], dy_recv.at[e, k], device_id=(p,), device_id_type=MESH)

    def r_copy(k, e):
        p = peer_of(k)
        return pltpu.make_async_remote_copy(dsend.at[p, e], dback.at[me, e], r_send.at[e, k], r_recv.at[e, k], device_id=(p,), device_id_type=MESH)

    def s_copy(k, e):
        p = peer_of(k)
        return pltpu.make_async_remote_copy(g_all.at[e, k], gback.at[me, e], s_send.at[e, k], s_recv.at[e, k], device_id=(p,), device_id_type=MESH)

    def c_copy(k):
        p = peer_of(k)
        return pltpu.make_async_remote_copy(cnt, cnt_all.at[me], c_send.at[k], c_recv.at[k], device_id=(p,), device_id_type=MESH)

    own_cnt = pltpu.make_async_copy(cnt, cnt_all.at[me], own_sem.at[n_local])
    own_cnt.start()
    for k in range(1, n_dev):
        c_copy(k).start()
    for e in range(n_local):
        for k in (1, 2, 4, 6, 3, 5, 7):
            if (e, k) not in EARLY:
                x_copy(k, e).start()
            dy_copy(k, e).start()

    order = (0, 1, 2, 4, 6, 3, 5, 7)

    def offset_of(i):
        k = i * 0
        for at, val in enumerate(order):
            k = k + jnp.where(i == at, val, 0)
        return k

    def load(e, i, slot, do):
        k = offset_of(i)
        p = peer_of(k)

        early = (e == 0) & ((i == 2) | (i == 3))

        def x_from(source):
            do(pltpu.make_async_copy(source, xv.at[slot], ld_sem.at[slot, 0]))

        @pl.when(i == 0)
        def _():
            x_from(xs.at[me, e])
            do(pltpu.make_async_copy(dys.at[me, e], dyv.at[slot], ld_sem.at[slot, 1]))

        @pl.when((e == 0) & (i == 2))
        def _():
            x_from(near_x)

        @pl.when((e == 0) & (i == 3))
        def _():
            x_from(near_y)

        @pl.when((i > 0) & jnp.logical_not(early))
        def _():
            x_from(xr.at[p, e])

        @pl.when(i > 0)
        def _():
            do(pltpu.make_async_copy(dyr.at[p, e], dyv.at[slot], ld_sem.at[slot, 1]))

    def arrive(e, i):
        k = offset_of(i)

        @pl.when((i > 0) & jnp.logical_not((e == 0) & ((i == 2) | (i == 3))))
        def _():
            x_copy(k, e).wait_recv()

        @pl.when(i > 0)
        def _():
            dy_copy(k, e).wait_recv()

    def store(c, do):
        e, i = c // n_dev, c % n_dev
        k = offset_of(i)
        p = peer_of(k)

        @pl.when(e == n_local - 1)
        def _():
            do(pltpu.make_async_copy(r_out.at[c % 2], dlast.at[p], st_sem.at[c % 2]))

        @pl.when(e < n_local - 1)
        def _():
            @pl.when(i == 0)
            def _():
                do(pltpu.make_async_copy(r_out.at[c % 2], dback.at[me, e], st_sem.at[c % 2]))

            @pl.when(i > 0)
            def _():
                do(pltpu.make_async_copy(r_out.at[c % 2], dsend.at[p, e], st_sem.at[c % 2]))

    def own_g(e):
        return pltpu.make_async_copy(g_all.at[e, 0], gback.at[me, e], own_sem.at[e])

    def send_back(c):
        e, i = c // n_dev, c % n_dev
        k = offset_of(i)
        store(c, lambda cp: cp.wait())

        @pl.when(i == 0)
        def _():
            own_g(e).start()

        @pl.when(i > 0)
        def _():
            s_copy(k, e).start()

            @pl.when(e < n_local - 1)
            def _():
                r_copy(k, e).start()

    def weights(e):
        return (pltpu.make_async_copy(w_in.at[e], win_v, w_sem.at[0]), pltpu.make_async_copy(w_out.at[e], wout_v, w_sem.at[1]))

    def flush(e):
        return (pltpu.make_async_copy(acc_in, gwin.at[e], flush_sem.at[0]), pltpu.make_async_copy(acc_out, gwout_t.at[e], flush_sem.at[1]))

    for cp in weights(0):
        cp.start()
    load(0 * me, 0 * me, 0, lambda cp: cp.start())
    for at, piece in enumerate(split3(w_t[...])):
        pad = jnp.zeros((LANES - num_experts, piece.shape[1]), F32)
        wr[at] = jnp.concatenate([piece, pad], axis=0).T.astype(BF16)

    def chunk(c, _):
        e, i = c // n_dev, c % n_dev
        k = offset_of(i)
        slot = c % 2

        @pl.when(i == 0)
        def _():
            @pl.when(c > 0)
            def _():
                for cp in weights(e):
                    cp.start()
                for cp in flush(e - 1):
                    cp.wait()
            acc_in[...] = jnp.zeros_like(acc_in)
            acc_out[...] = jnp.zeros_like(acc_out)
            for cp in weights(e):
                cp.wait()

        load(e, i, slot, lambda cp: cp.wait())
        x = xv[slot]
        logits = nn(x, wr[0]) + nn(x, wr[1]) + nn(x, wr[2])
        lane = lax.broadcasted_iota(jnp.int32, logits.shape, 1)
        logits = jnp.where(lane < num_experts, logits, -1e30)
        prob = jnp.exp(logits - jnp.max(logits, axis=1, keepdims=True))
        mine = jnp.sum(jnp.where(lane == me * n_local + e, prob, 0.0), axis=1, keepdims=True)
        gate = mine / jnp.sum(prob, axis=1, keepdims=True)
        grad = (gate * dyv[slot].astype(F32)).astype(BF16)
        gv[...] = grad
        x_t[...] = x.T
        g_t[...] = grad.T
        o_acc[...] = jnp.zeros_like(o_acc)
        r_acc[...] = jnp.zeros_like(r_acc)

        def block(f, _):
            @pl.when(f == n_blk - 1)
            def _():
                @pl.when(c + 1 < n_chunk)
                def _():
                    ne, ni = (c + 1) // n_dev, (c + 1) % n_dev
                    arrive(ne, ni)
                    load(ne, ni, 1 - slot, lambda cp: cp.start())

            @pl.when(f == 1)
            def _():
                @pl.when(c > 0)
                def _():
                    send_back(c - 1)

            cols = pl.ds(pl.multiple_of(f * blk, LANES), blk)
            win = win_v[:, cols]
            wout = wout_v[cols, :]
            hidden = jnp.maximum(nn(xv[slot], win), 0.0).astype(BF16)
            d_hidden = nt(gv[...], wout)
            d_pre = jnp.where(hidden > 0, d_hidden, 0.0).astype(BF16)
            o_acc[...] += nn(hidden, wout)
            r_acc[...] += nt(d_pre, win)
            acc_out[:, cols] += nn(g_t[...], hidden)
            acc_in[:, cols] += nn(x_t[...], d_pre)
            return 0

        lax.fori_loop(0, n_blk, block, 0)
        r_out[slot] = r_acc[...].astype(BF16)
        store(c, lambda cp: cp.start())
        g_val = jnp.sum(o_acc[...].astype(BF16).astype(F32) * dyv[slot].astype(F32), axis=1, keepdims=True)
        g_row = jnp.broadcast_to(g_val, (g_val.shape[0], LANES)).T
        g_all[e, k] = g_row[0:1, :]

        @pl.when(i == n_dev - 1)
        def _():
            for cp in flush(e):
                cp.start()
        return 0

    lax.fori_loop(0, n_chunk, chunk, 0)
    send_back(n_chunk - 1)
    for cp in flush(n_local - 1):
        cp.wait()
    own_cnt.wait()
    for k in range(1, n_dev):
        c_copy(k).wait()
    for e in range(n_local):
        own_g(e).wait()
        for k in range(1, n_dev):
            if (e, k) not in EARLY:
                x_copy(k, e).wait_send()
            dy_copy(k, e).wait_send()
            if e < n_local - 1:
                r_copy(k, e).wait()
            s_copy(k, e).wait()


def expert_exchange(n_dev, xs, dys, near_x, near_y, w_t, cnt, w_in, w_out):
    n_local, d_model, d_ff = w_in.shape
    cap = xs.shape[2]
    num_experts = n_dev * n_local
    blk = d_ff // 4
    hbm = pl.BlockSpec(memory_space=pl.ANY)
    vmem = pl.BlockSpec(memory_space=pltpu.VMEM)
    rows = jax.ShapeDtypeStruct(xs.shape, BF16)
    early = jax.ShapeDtypeStruct((n_dev, n_local - 1, cap, d_model), BF16)
    late = jax.ShapeDtypeStruct((n_dev, cap, d_model), BF16)
    g_shape = jax.ShapeDtypeStruct((n_dev, n_local, 1, cap), F32)
    w_shape = jax.ShapeDtypeStruct((n_local, d_model, d_ff), F32)
    dma = pltpu.SemaphoreType.DMA
    pair = (n_local, n_dev)
    return pl.pallas_call(
        lambda *refs: expert_kernel(n_dev, n_local, num_experts, blk, *refs),
        out_shape=(rows, rows, early, early, late, g_shape, w_shape, w_shape, jax.ShapeDtypeStruct((n_dev,) + cnt.shape, F32)),
        in_specs=[hbm, hbm, hbm, hbm, vmem, vmem, hbm, hbm],
        out_specs=[hbm] * 9,
        scratch_shapes=[
            pltpu.VMEM((2, cap, d_model), BF16), pltpu.VMEM((2, cap, d_model), BF16), pltpu.VMEM((cap, d_model), BF16),
            pltpu.VMEM((d_model, cap), BF16), pltpu.VMEM((d_model, cap), BF16), pltpu.VMEM((3, d_model, LANES), BF16),
            pltpu.VMEM((d_model, d_ff), BF16), pltpu.VMEM((d_ff, d_model), BF16),
            pltpu.VMEM((d_model, d_ff), F32), pltpu.VMEM((d_model, d_ff), F32),
            pltpu.VMEM((cap, d_model), F32), pltpu.VMEM((cap, d_model), F32),
            pltpu.VMEM((2, cap, d_model), BF16), pltpu.VMEM((n_local, n_dev, 1, cap), F32),
            dma(pair), dma(pair), dma(pair), dma(pair), dma(pair), dma(pair), dma(pair), dma(pair), dma((n_dev,)), dma((n_dev,)),
            dma((2, 2)), dma((2,)), dma((2,)), dma((2,)), dma((n_local + 1,)),
        ],
        compiler_params=pltpu.CompilerParams(collective_id=0, has_side_effects=True, vmem_limit_bytes=63 * 2 ** 20),
        name='expert_exchange',
    )(xs, dys, near_x, near_y, w_t, cnt, w_in, w_out)


PITCH = 6 * 8
ROW_TILES = 6


def row(addr, tiles):
    return pl.ds(addr, tiles, stride=8)


TB = 512
IN_FLIGHT = 4


def permute_rows(addr, source, sink, inb, stage, table, outb, in_sem, out_sem, meanwhile):
    n_out, n_local, cap, d_model = sink.shape
    groups = cap // 8
    tiled = table.reshape(table.shape[0] // PITCH, PITCH, LANES)
    stage3 = stage.reshape(TB // 8, PITCH, LANES)
    n_in = source.shape[0] // TB
    n_chunk = n_out * n_local

    def fetch(b):
        return pltpu.make_async_copy(source.at[pl.ds(pl.multiple_of(b * TB, TB), TB), :], inb.at[b % IN_FLIGHT], in_sem.at[b % IN_FLIGHT])

    def emit(c):
        return pltpu.make_async_copy(outb.at[c], sink.at[c // n_local, c % n_local], out_sem.at[c])

    for b in range(IN_FLIGHT - 1):
        fetch(b).start()
    table[...] = jnp.zeros_like(table)
    meanwhile()

    def scatter(b, _):
        @pl.when(b + IN_FLIGHT - 1 < n_in)
        def _():
            fetch(b + IN_FLIGHT - 1).start()
        fetch(b).wait()
        for j in range(ROW_TILES):
            part = inb[b % IN_FLIGHT, :, j * LANES:(j + 1) * LANES].astype(F32)
            stage3[:, j * 8:(j + 1) * 8, :] = part.reshape(TB // 8, 8, LANES)

        def move(i, _):
            for r in range(32):
                at = addr[b, i * 32 + r]
                table[row(at, ROW_TILES), :] = stage[row(i * (4 * PITCH) + (r // 8) * PITCH + r % 8, ROW_TILES), :]
            return 0

        lax.fori_loop(0, TB // 32, move, 0)
        return 0

    lax.fori_loop(0, n_in, scatter, 0)

    def drain(c, _):
        for j in range(ROW_TILES):
            part = tiled[pl.ds(c * groups, groups), j * 8:(j + 1) * 8, :].reshape(cap, LANES)
            outb[c, :, j * LANES:(j + 1) * LANES] = part.astype(BF16)
        emit(c).start()
        return 0

    def finish(c, _):
        emit(c).wait()
        return 0

    lax.fori_loop(0, n_chunk, drain, 0)
    lax.fori_loop(0, n_chunk, finish, 0)


def route_permute_kernel(idx, x, xs, slot_out, addr_out, count_out, addr, addr_sem, *scratch):
    n_out, n_local, cap, _ = xs.shape
    n = n_out * n_local

    def route():
        below = lax.broadcasted_iota(jnp.int32, (TB, TB), 0) <= lax.broadcasted_iota(jnp.int32, (TB, TB), 1)
        upper = jnp.where(below, 1.0, 0.0).astype(BF16)
        expert = lax.broadcasted_iota(jnp.int32, (n, TB), 0)
        seen = jnp.zeros((n, 1), F32)
        for b in range(idx.shape[0]):
            mine = expert == idx[b:b + 1, :]
            onehot = jnp.where(mine, 1.0, 0.0)
            rank = nn(onehot.astype(BF16), upper)
            pos = jnp.sum(jnp.where(mine, rank + (seen - 1.0), 0.0), axis=0, keepdims=True).astype(jnp.int32)
            slot = jnp.where(pos < cap, idx[b:b + 1, :] * cap + pos, n * cap)
            slot_out[b:b + 1, :] = slot
            group = lax.shift_right_logical(slot, jnp.full_like(slot, 3))
            addr_out[b:b + 1, :] = group * PITCH + (slot - group * 8)
            seen = seen + rank[:, TB - 1:TB]
        count_out[...] = jnp.broadcast_to(seen, count_out.shape)
        copy = pltpu.make_async_copy(addr_out, addr, addr_sem)
        copy.start()
        copy.wait()

    permute_rows(addr, x, xs, *scratch, route)


def permute_scratch(n_slots, cap, d_model):
    return [pltpu.VMEM((IN_FLIGHT, TB, d_model), BF16), pltpu.VMEM((TB // 8 * PITCH, LANES), F32), pltpu.VMEM(((n_slots // 8 + 1) * PITCH, LANES), F32),
            pltpu.VMEM((n_slots // cap, cap, d_model), BF16), pltpu.SemaphoreType.DMA((IN_FLIGHT,)), pltpu.SemaphoreType.DMA((n_slots // cap,))]


def route_permute(n_dev, n_local, cap, idx, x):
    hbm = pl.BlockSpec(memory_space=pl.ANY)
    vmem = pl.BlockSpec(memory_space=pltpu.VMEM)
    table = jax.ShapeDtypeStruct(idx.shape, jnp.int32)
    n = n_dev * n_local
    return pl.pallas_call(
        route_permute_kernel,
        out_shape=(jax.ShapeDtypeStruct((n_dev, n_local, cap, x.shape[1]), BF16), table, table, jax.ShapeDtypeStruct((n, LANES), F32)),
        in_specs=[vmem, hbm], out_specs=[hbm, vmem, vmem, vmem],
        scratch_shapes=[pltpu.SMEM(idx.shape, jnp.int32), pltpu.SemaphoreType.DMA] + permute_scratch(n * cap, cap, x.shape[1]),
        compiler_params=pltpu.CompilerParams(vmem_limit_bytes=60 * 2 ** 20),
        name='route_permute',
    )(idx, x)


def permute(n_dev, n_local, cap, addr, x):
    hbm = pl.BlockSpec(memory_space=pl.ANY)
    return pl.pallas_call(
        lambda *refs: permute_rows(*refs, lambda: None),
        out_shape=jax.ShapeDtypeStruct((n_dev, n_local, cap, x.shape[1]), BF16),
        grid_spec=pltpu.PrefetchScalarGridSpec(
            num_scalar_prefetch=1, grid=(), in_specs=[hbm], out_specs=hbm,
            scratch_shapes=permute_scratch(n_dev * n_local * cap, cap, x.shape[1])),
        cost_estimate=pl.CostEstimate(flops=20 * 10 ** 9, bytes_accessed=28 * 2 ** 20, transcendentals=0),
        compiler_params=pltpu.CompilerParams(vmem_limit_bytes=60 * 2 ** 20),
        name='permute_rows',
    )(addr, x)


def router_kernel(z_coef, slot, x, idx, w_t, v_col, gback, pieces_out, partial, acc, gtab, g_rows, w_six, pieces_t, p_acc, z_acc):
    b = pl.program_id(0)
    tb = x.shape[0]
    n_chunk, cap = gback.shape
    n = w_t.shape[0]

    @pl.when(b == 0)
    def _():
        acc[...] = jnp.zeros_like(acc)
        p_acc[...] = jnp.zeros_like(p_acc)
        z_acc[...] = jnp.zeros_like(z_acc)
        w_six[...] = six_terms(w_t[...])
        gtab[n_chunk * cap:, :] = jnp.zeros((8, LANES), F32)

        def fill(c, _):
            gtab[pl.ds(pl.multiple_of(c * cap, 8), cap), :] = jnp.broadcast_to(gback[pl.ds(c, 1), :], (LANES, cap)).T
            return 0

        lax.fori_loop(0, n_chunk, fill, 0)

    def move(i, _):
        for r in range(32):
            g_rows[pl.ds(i * 32 + r, 1), :] = gtab[pl.ds(slot[b, i * 32 + r], 1), :]
        return 0

    lax.fori_loop(0, tb // 32, move, 0)

    xv = x[...]
    terms = nt(w_six[...], xv)
    logits = terms[0:n] + terms[3 * n:4 * n] + terms[5 * n:6 * n]
    top = jnp.max(logits, axis=0, keepdims=True)
    expd = jnp.exp(logits - top)
    total = jnp.sum(expd, axis=0, keepdims=True)
    prob = expd / total
    z = top + jnp.log(total)
    mine = lax.broadcasted_iota(jnp.int32, logits.shape, 0) == idx[pl.ds(b, 1), :]
    onehot = jnp.where(mine, 1.0, 0.0)
    gate = jnp.sum(jnp.where(mine, prob, 0.0), axis=0, keepdims=True)
    g = g_rows[...].T[0:1, :]
    v = v_col[:, 0:1]
    spread = jnp.sum(prob * v, axis=0, keepdims=True)
    dlog = gate * g * (onehot - prob) + prob * (v - spread) + (z_coef * z) * prob
    hi, mid, low = split3(dlog)
    pieces = jnp.concatenate([hi, mid, low, hi, mid, hi, jnp.zeros((LANES - 6 * n, tb), F32)], axis=0)
    pieces_out[...] = pieces.T.astype(BF16)
    pieces_t[...] = pieces.astype(BF16)
    acc[...] += nn(pieces_t[...], xv)
    zz = z * z
    for j in range(tb // LANES):
        p_acc[...] += prob[:, j * LANES:(j + 1) * LANES]
        z_acc[0:1, :] += zz[:, j * LANES:(j + 1) * LANES]

    @pl.when(b == pl.num_programs(0) - 1)
    def _():
        partial[...] = jnp.zeros_like(partial)
        partial[0:n, :] = acc[0:n, :] + acc[n:2 * n, :] + acc[2 * n:3 * n, :]
        p_sum = jnp.broadcast_to(jnp.sum(p_acc[...], axis=1, keepdims=True), p_acc.shape)
        p_full = jnp.concatenate([p_sum, jnp.zeros((LANES - n, LANES), F32)], axis=0).T
        partial[n:n + 1, 0:LANES] = p_full[0:1, :]
        partial[n:n + 1, LANES:2 * LANES] = jnp.broadcast_to(jnp.sum(z_acc[0:1, :], axis=1, keepdims=True), (1, LANES))


def whole(a):
    return pl.BlockSpec(a.shape, lambda b, addr: (0,) * a.ndim)


def router_side(z_coef, slot, x, idx, w_t, v_col, gback):
    tokens, d_model = x.shape
    n_dev, n_local, _, cap = gback.shape
    tb = TB
    n = w_t.shape[0]
    gback = gback.reshape(n_dev * n_local, cap)
    rows = n + 8
    return pl.pallas_call(
        lambda *refs: router_kernel(z_coef, *refs),
        out_shape=(jax.ShapeDtypeStruct((tokens, LANES), BF16), jax.ShapeDtypeStruct((rows, d_model), F32), jax.ShapeDtypeStruct((LANES, d_model), F32)),
        grid_spec=pltpu.PrefetchScalarGridSpec(
            num_scalar_prefetch=1, grid=(tokens // tb,),
            in_specs=[pl.BlockSpec((tb, d_model), lambda b, addr: (b, 0)), whole(idx), whole(w_t), whole(v_col), whole(gback)],
            out_specs=[pl.BlockSpec((tb, LANES), lambda b, addr: (b, 0)), pl.BlockSpec((rows, d_model), lambda b, addr: (0, 0)),
                       pl.BlockSpec((LANES, d_model), lambda b, addr: (0, 0))],
            scratch_shapes=[
                pltpu.VMEM((n_dev * n_local * cap + 8, LANES), F32), pltpu.VMEM((tb, LANES), F32), pltpu.VMEM((LANES, d_model), BF16),
                pltpu.VMEM((LANES, tb), BF16), pltpu.VMEM((n, LANES), F32), pltpu.VMEM((8, LANES), F32)]),
        cost_estimate=pl.CostEstimate(flops=30 * 10 ** 9, bytes_accessed=16 * 2 ** 20, transcendentals=0),
        compiler_params=pltpu.CompilerParams(vmem_limit_bytes=40 * 2 ** 20),
        name='router_side',
    )(slot, x, idx, w_t, v_col, gback)


def combine_kernel(addr, pieces, w_t, dback, dlast, grad_x, stage, table, inb, w_six, in_sem):
    b = pl.program_id(0)
    tb = pieces.shape[0]
    n_out, cap, d_model = dlast.shape
    n_local = dback.shape[1] + 1
    groups = cap // 8
    tiled = table.reshape(table.shape[0] // PITCH, PITCH, LANES)
    stage3 = stage.reshape(tb // 8, PITCH, LANES)

    @pl.when(b == 0)
    def _():
        n_buf = inb.shape[1]

        def fetch(d, e):
            source = dback.at[d, e] if e < n_local - 1 else dlast.at[d]
            return pltpu.make_async_copy(source, inb.at[e, d % n_buf], in_sem.at[e, d % n_buf])

        for d in range(n_buf):
            for e in range(n_local):
                fetch(d, e).start()
        w_six[...] = six_terms(w_t[...])
        tiled[n_out * n_local * groups] = jnp.zeros((PITCH, LANES), F32)

        def fill(d, _):
            for e in range(n_local):
                fetch(d, e).wait()
                for j in range(ROW_TILES):
                    part = inb[e, d % n_buf, :, j * LANES:(j + 1) * LANES].astype(F32)
                    tiled[pl.ds((d * n_local + e) * groups, groups), j * 8:(j + 1) * 8, :] = part.reshape(groups, 8, LANES)

                @pl.when(d + n_buf < n_out)
                def _():
                    fetch(d + n_buf, e).start()
            return 0

        lax.fori_loop(0, n_out, fill, 0)

    def move(i, _):
        for r in range(32):
            at = addr[b, i * 32 + r]
            stage[row(i * (4 * PITCH) + (r // 8) * PITCH + r % 8, ROW_TILES), :] = table[row(at, ROW_TILES), :]
        return 0

    lax.fori_loop(0, tb // 32, move, 0)
    for j in range(ROW_TILES):
        cols = slice(j * LANES, (j + 1) * LANES)
        grad_x[:, cols] = (stage3[:, j * 8:(j + 1) * 8, :].reshape(tb, LANES) + nn(pieces[...], w_six[:, cols])).astype(BF16)


def combine(addr, pieces, w_t, dback, dlast):
    tokens = pieces.shape[0]
    n_dev, cap, d_model = dlast.shape
    n_local = dback.shape[1] + 1
    tb = TB
    hbm = pl.BlockSpec(memory_space=pl.ANY)
    n_groups = n_dev * n_local * cap // 8 + 1
    return pl.pallas_call(
        combine_kernel,
        out_shape=jax.ShapeDtypeStruct((tokens, d_model), BF16),
        grid_spec=pltpu.PrefetchScalarGridSpec(
            num_scalar_prefetch=1, grid=(tokens // tb,),
            in_specs=[pl.BlockSpec((tb, LANES), lambda b, addr: (b, 0)), whole(w_t), hbm, hbm],
            out_specs=pl.BlockSpec((tb, d_model), lambda b, addr: (b, 0)),
            scratch_shapes=[
                pltpu.VMEM((tb // 8 * PITCH, LANES), F32), pltpu.VMEM((n_groups * PITCH, LANES), F32),
                pltpu.VMEM((n_local, 4, cap, d_model), BF16), pltpu.VMEM((LANES, d_model), BF16), pltpu.SemaphoreType.DMA((n_local, 4))]),
        compiler_params=pltpu.CompilerParams(vmem_limit_bytes=56 * 2 ** 20),
        name='combine_rows',
    )(addr, pieces, w_t, dback, dlast)


def total_kernel(n_dev, part, _before_a, _before_b, out, stats, parts, send_sem, recv_sem):
    me = lax.axis_index('ep')
    barrier = pltpu.get_barrier_semaphore()
    peers = [(me + k) % n_dev for k in range(1, n_dev)]
    for p in peers:
        pl.semaphore_signal(barrier, inc=1, device_id=(p,), device_id_type=MESH)
    pl.semaphore_wait(barrier, n_dev - 1)
    copies = [pltpu.make_async_remote_copy(part, parts.at[me], send_sem.at[k], recv_sem.at[k], device_id=(p,), device_id_type=MESH)
              for k, p in enumerate(peers)]
    for copy in copies:
        copy.start()
    parts[me] = part[...]
    for copy in copies:
        copy.wait()
    total = parts[0]
    for d in range(1, n_dev):
        total = total + parts[d]
    n = out.shape[0]
    out[...] = total[0:n]
    stats[...] = total[n:]


def total_over_devices(n_dev, n_grad, part, before):
    vmem = pl.BlockSpec(memory_space=pltpu.VMEM)
    return pl.pallas_call(
        lambda *refs: total_kernel(n_dev, *refs),
        out_shape=(jax.ShapeDtypeStruct((n_grad, part.shape[1]), F32), jax.ShapeDtypeStruct((part.shape[0] - n_grad, part.shape[1]), F32)),
        in_specs=[vmem] + [pl.BlockSpec(memory_space=pl.ANY)] * 2, out_specs=[vmem, vmem],
        scratch_shapes=[pltpu.VMEM((n_dev,) + part.shape, F32), pltpu.SemaphoreType.DMA((n_dev - 1,)), pltpu.SemaphoreType.DMA((n_dev - 1,))],
        compiler_params=pltpu.CompilerParams(collective_id=1, has_side_effects=True),
        name='device_total',
    )(part, *before)


def copy_kernel(source, sink):
    sink[...] = source[...]


def own_copy(a):
    n, rows, cols = a.shape
    spec = pl.BlockSpec((1, rows // 6, cols), lambda e, r: (e, r, 0))
    return pl.pallas_call(
        copy_kernel, out_shape=jax.ShapeDtypeStruct(a.shape, a.dtype), grid=(n, 6), in_specs=[spec], out_specs=spec,
        cost_estimate=pl.CostEstimate(flops=15 * 10 ** 9, bytes_accessed=2 * a.size * 4, transcendentals=0),
        name='own_copy')(a)


def solution(mesh):
    n_dev = mesh.shape['ep']

    def expert_layer(x_tokens, w_router, expert_idx, w_in, w_out, grad_y):
        tokens, d_model = x_tokens.shape
        n_local = w_in.shape[0]
        num_experts = n_local * n_dev
        capacity = (5 * tokens + 4 * num_experts - 1) // (4 * num_experts)
        total_tok = tokens * n_dev
        w_t = w_router.T
        idx = expert_idx.reshape(tokens // TB, TB)
        xs, slot, addr, cnt = route_permute(n_dev, n_local, capacity, idx, x_tokens)
        me = lax.axis_index('ep')
        near_x, near_y = [lax.ppermute(lax.dynamic_slice(xs, (me ^ k, e, 0, 0), (1, 1, capacity, d_model)).reshape(capacity, d_model), 'ep',
                                       [(d, d ^ k) for d in range(n_dev)]) for e, k in EARLY]
        dys = permute(n_dev, n_local, capacity, addr, grad_y)

        _, _, _, d_back, d_last, g_back, gwin, gwout_t, cnt_all = expert_exchange(n_dev, xs, dys, near_x, near_y, w_t, cnt, w_in, w_out)
        d_last = lax.all_to_all(d_last, 'ep', 0, 0, tiled=True)
        load_frac = jnp.sum(cnt_all, axis=0) / total_tok
        v_col = AUX_WEIGHT * num_experts * load_frac / total_tok
        pieces, partial, _ = router_side(2.0 * Z_WEIGHT / total_tok, slot, x_tokens, idx, w_t, v_col, g_back)
        grad_w_out = jnp.swapaxes(gwout_t, 1, 2)
        grad_w_in = own_copy(gwin)
        grad_x = combine(addr, pieces, w_t, d_back, d_last)
        grad_wr_t, stats = total_over_devices(n_dev, num_experts, partial, (grad_w_in, grad_w_out))
        grad_w_router = grad_wr_t.T
        mean_prob = stats[0, :num_experts] / total_tok
        aux_loss = AUX_WEIGHT * num_experts * jnp.sum(load_frac[:, 0] * mean_prob)
        z_loss = Z_WEIGHT * stats[0, LANES] / total_tok
        return grad_x, grad_w_in, grad_w_out, grad_w_router, aux_loss, z_loss

    return jax.shard_map(expert_layer, mesh=mesh,
                         in_specs=(P('ep', None), P(None, None), P('ep'), P('ep', None, None), P('ep', None, None), P('ep', None)),
                         out_specs=(P('ep', None), P('ep', None, None), P('ep', None, None), P(None, None), P(), P()),
                         check_vma=False)
```

```python
import jax
import jax.numpy as jnp
from jax import lax
from jax.experimental import pallas as pl
from jax.experimental.pallas import tpu as pltpu
from jax.sharding import PartitionSpec as P

AUX_WEIGHT = 0.01
Z_WEIGHT = 0.001
MESH = pl.DeviceIdType.MESH
F32 = jnp.float32
BF16 = jnp.bfloat16
LANES = 128


def split3(w):
    hi = w.astype(BF16).astype(F32)
    mid = (w - hi).astype(BF16).astype(F32)
    return hi, mid, w - hi - mid


def six_terms(w):
    hi, mid, low = split3(w)
    pad = jnp.zeros((LANES - 6 * w.shape[0], w.shape[1]), F32)
    return jnp.concatenate([hi, hi, hi, mid, mid, low, pad], axis=0).astype(BF16)


def nt(a, b):
    return lax.dot_general(a, b, (((1,), (1,)), ((), ())), preferred_element_type=F32)


def nn(a, b):
    return jnp.dot(a, b, preferred_element_type=F32)


EARLY = ((0, 2), (0, 4))


def expert_kernel(n_dev, n_local, num_experts, blk, xs, dys, near_x, near_y, w_t, cnt, w_in, w_out,
                  xr, dyr, dsend, dback, dlast, gback, gwin, gwout_t, cnt_all,
                  xv, dyv, gv, x_t, g_t, wr, win_v, wout_v, acc_in, acc_out, o_acc, r_acc, r_out, g_all,
                  x_send, x_recv, dy_send, dy_recv, r_send, r_recv, s_send, s_recv, c_send, c_recv, ld_sem, st_sem, w_sem, flush_sem, own_sem):
    me = lax.axis_index('ep')
    n_blk = w_in.shape[2] // blk
    n_chunk = n_local * n_dev

    def peer_of(k):
        out = 0
        bit = 1
        while bit < n_dev:
            out = out + bit * (((me // bit) + (k // bit)) % 2)
            bit *= 2
        return out

    barrier = pltpu.get_barrier_semaphore()
    for k in range(1, n_dev):
        pl.semaphore_signal(barrier, inc=1, device_id=(peer_of(k),), device_id_type=MESH)
    pl.semaphore_wait(barrier, n_dev - 1)

    def x_copy(k, e):
        p = peer_of(k)
        return pltpu.make_async_remote_copy(xs.at[p, e], xr.at[me, e], x_send.at[e, k], x_recv.at[e, k], device_id=(p,), device_id_type=MESH)

    def dy_copy(k, e):
        p = peer_of(k)
        return pltpu.make_async_remote_copy(dys.at[p, e], dyr.at[me, e], dy_send.at[e, k], dy_recv.at[e, k], device_id=(p,), device_id_type=MESH)

    def r_copy(k, e):
        p = peer_of(k)
        return pltpu.make_async_remote_copy(dsend.at[p, e], dback.at[me, e], r_send.at[e, k], r_recv.at[e, k], device_id=(p,), device_id_type=MESH)

    def s_copy(k, e):
        p = peer_of(k)
        return pltpu.make_async_remote_copy(g_all.at[e, k], gback.at[me, e], s_send.at[e, k], s_recv.at[e, k], device_id=(p,), device_id_type=MESH)

    def c_copy(k):
        p = peer_of(k)
        return pltpu.make_async_remote_copy(cnt, cnt_all.at[me], c_send.at[k], c_recv.at[k], device_id=(p,), device_id_type=MESH)

    own_cnt = pltpu.make_async_copy(cnt, cnt_all.at[me], own_sem.at[n_local])
    own_cnt.start()
    for k in range(1, n_dev):
        c_copy(k).start()
    for e in range(n_local):
        for k in (1, 2, 4, 6, 3, 5, 7):
            if (e, k) not in EARLY:
                x_copy(k, e).start()
            dy_copy(k, e).start()

    order = (0, 1, 2, 4, 6, 3, 5, 7)

    def offset_of(i):
        k = i * 0
        for at, val in enumerate(order):
            k = k + jnp.where(i == at, val, 0)
        return k

    def load(e, i, slot, do):
        k = offset_of(i)
        p = peer_of(k)

        early = (e == 0) & ((i == 2) | (i == 3))

        def x_from(source):
            do(pltpu.make_async_copy(source, xv.at[slot], ld_sem.at[slot, 0]))

        @pl.when(i == 0)
        def _():
            x_from(xs.at[me, e])
            do(pltpu.make_async_copy(dys.at[me, e], dyv.at[slot], ld_sem.at[slot, 1]))

        @pl.when((e == 0) & (i == 2))
        def _():
            x_from(near_x)

        @pl.when((e == 0) & (i == 3))
        def _():
            x_from(near_y)

        @pl.when((i > 0) & jnp.logical_not(early))
        def _():
            x_from(xr.at[p, e])

        @pl.when(i > 0)
        def _():
            do(pltpu.make_async_copy(dyr.at[p, e], dyv.at[slot], ld_sem.at[slot, 1]))

    def arrive(e, i):
        k = offset_of(i)

        @pl.when((i > 0) & jnp.logical_not((e == 0) & ((i == 2) | (i == 3))))
        def _():
            x_copy(k, e).wait_recv()

        @pl.when(i > 0)
        def _():
            dy_copy(k, e).wait_recv()

    def store(c, do):
        e, i = c // n_dev, c % n_dev
        k = offset_of(i)
        p = peer_of(k)

        @pl.when(e == n_local - 1)
        def _():
            do(pltpu.make_async_copy(r_out.at[c % 2], dlast.at[p], st_sem.at[c % 2]))

        @pl.when(e < n_local - 1)
        def _():
            @pl.when(i == 0)
            def _():
                do(pltpu.make_async_copy(r_out.at[c % 2], dback.at[me, e], st_sem.at[c % 2]))

            @pl.when(i > 0)
            def _():
                do(pltpu.make_async_copy(r_out.at[c % 2], dsend.at[p, e], st_sem.at[c % 2]))

    def own_g(e):
        return pltpu.make_async_copy(g_all.at[e, 0], gback.at[me, e], own_sem.at[e])

    def send_back(c):
        e, i = c // n_dev, c % n_dev
        k = offset_of(i)
        store(c, lambda cp: cp.wait())

        @pl.when(i == 0)
        def _():
            own_g(e).start()

        @pl.when(i > 0)
        def _():
            s_copy(k, e).start()

            @pl.when(e < n_local - 1)
            def _():
                r_copy(k, e).start()

    def weights(e):
        return (pltpu.make_async_copy(w_in.at[e], win_v, w_sem.at[0]), pltpu.make_async_copy(w_out.at[e], wout_v, w_sem.at[1]))

    def flush(e):
        return (pltpu.make_async_copy(acc_in, gwin.at[e], flush_sem.at[0]), pltpu.make_async_copy(acc_out, gwout_t.at[e], flush_sem.at[1]))

    for cp in weights(0):
        cp.start()
    load(0 * me, 0 * me, 0, lambda cp: cp.start())
    for at, piece in enumerate(split3(w_t[...])):
        pad = jnp.zeros((LANES - num_experts, piece.shape[1]), F32)
        wr[at] = jnp.concatenate([piece, pad], axis=0).T.astype(BF16)

    def chunk(c, _):
        e, i = c // n_dev, c % n_dev
        k = offset_of(i)
        slot = c % 2

        @pl.when(i == 0)
        def _():
            @pl.when(c > 0)
            def _():
                for cp in weights(e):
                    cp.start()
                for cp in flush(e - 1):
                    cp.wait()
            acc_in[...] = jnp.zeros_like(acc_in)
            acc_out[...] = jnp.zeros_like(acc_out)
            for cp in weights(e):
                cp.wait()

        load(e, i, slot, lambda cp: cp.wait())
        x = xv[slot]
        logits = nn(x, wr[0]) + nn(x, wr[1]) + nn(x, wr[2])
        lane = lax.broadcasted_iota(jnp.int32, logits.shape, 1)
        logits = jnp.where(lane < num_experts, logits, -1e30)
        prob = jnp.exp(logits - jnp.max(logits, axis=1, keepdims=True))
        mine = jnp.sum(jnp.where(lane == me * n_local + e, prob, 0.0), axis=1, keepdims=True)
        gate = mine / jnp.sum(prob, axis=1, keepdims=True)
        grad = (gate * dyv[slot].astype(F32)).astype(BF16)
        gv[...] = grad
        x_t[...] = x.T
        g_t[...] = grad.T
        o_acc[...] = jnp.zeros_like(o_acc)
        r_acc[...] = jnp.zeros_like(r_acc)

        def block(f, _):
            @pl.when(f == n_blk - 1)
            def _():
                @pl.when(c + 1 < n_chunk)
                def _():
                    ne, ni = (c + 1) // n_dev, (c + 1) % n_dev
                    arrive(ne, ni)
                    load(ne, ni, 1 - slot, lambda cp: cp.start())

            @pl.when(f == 1)
            def _():
                @pl.when(c > 0)
                def _():
                    send_back(c - 1)

            cols = pl.ds(pl.multiple_of(f * blk, LANES), blk)
            win = win_v[:, cols]
            wout = wout_v[cols, :]
            hidden = jnp.maximum(nn(xv[slot], win), 0.0).astype(BF16)
            d_hidden = nt(gv[...], wout)
            d_pre = jnp.where(hidden > 0, d_hidden, 0.0).astype(BF16)
            o_acc[...] += nn(hidden, wout)
            r_acc[...] += nt(d_pre, win)
            acc_out[:, cols] += nn(g_t[...], hidden)
            acc_in[:, cols] += nn(x_t[...], d_pre)
            return 0

        lax.fori_loop(0, n_blk, block, 0)
        r_out[slot] = r_acc[...].astype(BF16)
        store(c, lambda cp: cp.start())
        g_val = jnp.sum(o_acc[...].astype(BF16).astype(F32) * dyv[slot].astype(F32), axis=1, keepdims=True)
        g_row = jnp.broadcast_to(g_val, (g_val.shape[0], LANES)).T
        g_all[e, k] = g_row[0:1, :]

        @pl.when(i == n_dev - 1)
        def _():
            for cp in flush(e):
                cp.start()
        return 0

    lax.fori_loop(0, n_chunk, chunk, 0)
    send_back(n_chunk - 1)
    for cp in flush(n_local - 1):
        cp.wait()
    own_cnt.wait()
    for k in range(1, n_dev):
        c_copy(k).wait()
    for e in range(n_local):
        own_g(e).wait()
        for k in range(1, n_dev):
            if (e, k) not in EARLY:
                x_copy(k, e).wait_send()
            dy_copy(k, e).wait_send()
            if e < n_local - 1:
                r_copy(k, e).wait()
            s_copy(k, e).wait()


def expert_exchange(n_dev, xs, dys, near_x, near_y, w_t, cnt, w_in, w_out):
    n_local, d_model, d_ff = w_in.shape
    cap = xs.shape[2]
    num_experts = n_dev * n_local
    blk = d_ff // 4
    hbm = pl.BlockSpec(memory_space=pl.ANY)
    vmem = pl.BlockSpec(memory_space=pltpu.VMEM)
    rows = jax.ShapeDtypeStruct(xs.shape, BF16)
    early = jax.ShapeDtypeStruct((n_dev, n_local - 1, cap, d_model), BF16)
    late = jax.ShapeDtypeStruct((n_dev, cap, d_model), BF16)
    g_shape = jax.ShapeDtypeStruct((n_dev, n_local, 1, cap), F32)
    w_shape = jax.ShapeDtypeStruct((n_local, d_model, d_ff), F32)
    dma = pltpu.SemaphoreType.DMA
    pair = (n_local, n_dev)
    return pl.pallas_call(
        lambda *refs: expert_kernel(n_dev, n_local, num_experts, blk, *refs),
        out_shape=(rows, rows, early, early, late, g_shape, w_shape, w_shape, jax.ShapeDtypeStruct((n_dev,) + cnt.shape, F32)),
        in_specs=[hbm, hbm, hbm, hbm, vmem, vmem, hbm, hbm],
        out_specs=[hbm] * 9,
        scratch_shapes=[
            pltpu.VMEM((2, cap, d_model), BF16), pltpu.VMEM((2, cap, d_model), BF16), pltpu.VMEM((cap, d_model), BF16),
            pltpu.VMEM((d_model, cap), BF16), pltpu.VMEM((d_model, cap), BF16), pltpu.VMEM((3, d_model, LANES), BF16),
            pltpu.VMEM((d_model, d_ff), BF16), pltpu.VMEM((d_ff, d_model), BF16),
            pltpu.VMEM((d_model, d_ff), F32), pltpu.VMEM((d_model, d_ff), F32),
            pltpu.VMEM((cap, d_model), F32), pltpu.VMEM((cap, d_model), F32),
            pltpu.VMEM((2, cap, d_model), BF16), pltpu.VMEM((n_local, n_dev, 1, cap), F32),
            dma(pair), dma(pair), dma(pair), dma(pair), dma(pair), dma(pair), dma(pair), dma(pair), dma((n_dev,)), dma((n_dev,)),
            dma((2, 2)), dma((2,)), dma((2,)), dma((2,)), dma((n_local + 1,)),
        ],
        compiler_params=pltpu.CompilerParams(collective_id=0, has_side_effects=True, vmem_limit_bytes=63 * 2 ** 20),
        name='expert_exchange',
    )(xs, dys, near_x, near_y, w_t, cnt, w_in, w_out)


PITCH = 6 * 8
ROW_TILES = 6


def row(addr, tiles):
    return pl.ds(addr, tiles, stride=8)


TB = 512
IN_FLIGHT = 4


def permute_rows(addr, source, sink, inb, stage, table, outb, in_sem, out_sem, meanwhile):
    n_out, n_local, cap, d_model = sink.shape
    groups = cap // 8
    tiled = table.reshape(table.shape[0] // PITCH, PITCH, LANES)
    stage3 = stage.reshape(TB // 8, PITCH, LANES)
    n_in = source.shape[0] // TB
    n_chunk = n_out * n_local

    def fetch(b):
        return pltpu.make_async_copy(source.at[pl.ds(pl.multiple_of(b * TB, TB), TB), :], inb.at[b % IN_FLIGHT], in_sem.at[b % IN_FLIGHT])

    def emit(c):
        return pltpu.make_async_copy(outb.at[c], sink.at[c // n_local, c % n_local], out_sem.at[c])

    for b in range(IN_FLIGHT - 1):
        fetch(b).start()
    table[...] = jnp.zeros_like(table)
    meanwhile()

    def scatter(b, _):
        @pl.when(b + IN_FLIGHT - 1 < n_in)
        def _():
            fetch(b + IN_FLIGHT - 1).start()
        fetch(b).wait()
        for j in range(ROW_TILES):
            part = inb[b % IN_FLIGHT, :, j * LANES:(j + 1) * LANES].astype(F32)
            stage3[:, j * 8:(j + 1) * 8, :] = part.reshape(TB // 8, 8, LANES)

        def move(i, _):
            for r in range(32):
                at = addr[b * TB + i * 32 + r]
                table[row(at, ROW_TILES), :] = stage[row(i * (4 * PITCH) + (r // 8) * PITCH + r % 8, ROW_TILES), :]
            return 0

        lax.fori_loop(0, TB // 32, move, 0)
        return 0

    lax.fori_loop(0, n_in, scatter, 0)

    def drain(c, _):
        for j in range(ROW_TILES):
            part = tiled[pl.ds(c * groups, groups), j * 8:(j + 1) * 8, :].reshape(cap, LANES)
            outb[c, :, j * LANES:(j + 1) * LANES] = part.astype(BF16)
        emit(c).start()
        return 0

    def finish(c, _):
        emit(c).wait()
        return 0

    lax.fori_loop(0, n_chunk, drain, 0)
    lax.fori_loop(0, n_chunk, finish, 0)


def route_permute_kernel(idx, x, xs, slot_out, addr_out, count_out, addr, addr_sem, *scratch):
    n_out, n_local, cap, _ = xs.shape
    n = n_out * n_local

    def route():
        below = lax.broadcasted_iota(jnp.int32, (TB, TB), 0) <= lax.broadcasted_iota(jnp.int32, (TB, TB), 1)
        upper = jnp.where(below, 1.0, 0.0).astype(BF16)
        expert = lax.broadcasted_iota(jnp.int32, (n, TB), 0)
        seen = jnp.zeros((n, 1), F32)
        for b in range(idx.shape[0]):
            mine = expert == idx[b:b + 1, :]
            onehot = jnp.where(mine, 1.0, 0.0)
            rank = nn(onehot.astype(BF16), upper)
            pos = jnp.sum(jnp.where(mine, rank + (seen - 1.0), 0.0), axis=0, keepdims=True).astype(jnp.int32)
            slot = jnp.where(pos < cap, idx[b:b + 1, :] * cap + pos, n * cap)
            slot_out[b:b + 1, :] = slot
            group = lax.shift_right_logical(slot, jnp.full_like(slot, 3))
            addr_out[b:b + 1, :] = group * PITCH + (slot - group * 8)
            seen = seen + rank[:, TB - 1:TB]
        count_out[...] = jnp.broadcast_to(seen, count_out.shape)
        copies = [pltpu.make_async_copy(addr_out.at[b], addr.at[pl.ds(b * TB, TB)], addr_sem.at[b]) for b in range(idx.shape[0])]
        for copy in copies:
            copy.start()
        for copy in copies:
            copy.wait()

    permute_rows(addr, x, xs, *scratch, route)


def permute_scratch(n_slots, cap, d_model):
    return [pltpu.VMEM((IN_FLIGHT, TB, d_model), BF16), pltpu.VMEM((TB // 8 * PITCH, LANES), F32), pltpu.VMEM(((n_slots // 8 + 1) * PITCH, LANES), F32),
            pltpu.VMEM((n_slots // cap, cap, d_model), BF16), pltpu.SemaphoreType.DMA((IN_FLIGHT,)), pltpu.SemaphoreType.DMA((n_slots // cap,))]


def route_permute(n_dev, n_local, cap, idx, x):
    hbm = pl.BlockSpec(memory_space=pl.ANY)
    vmem = pl.BlockSpec(memory_space=pltpu.VMEM)
    table = jax.ShapeDtypeStruct(idx.shape, jnp.int32)
    n = n_dev * n_local
    return pl.pallas_call(
        route_permute_kernel,
        out_shape=(jax.ShapeDtypeStruct((n_dev, n_local, cap, x.shape[1]), BF16), table, table, jax.ShapeDtypeStruct((n, LANES), F32)),
        in_specs=[vmem, hbm], out_specs=[hbm, vmem, vmem, vmem],
        scratch_shapes=[pltpu.SMEM((idx.size,), jnp.int32), pltpu.SemaphoreType.DMA((idx.shape[0],))] + permute_scratch(n * cap, cap, x.shape[1]),
        compiler_params=pltpu.CompilerParams(vmem_limit_bytes=60 * 2 ** 20),
        name='route_permute',
    )(idx, x)


def permute(n_dev, n_local, cap, addr, x):
    hbm = pl.BlockSpec(memory_space=pl.ANY)
    return pl.pallas_call(
        lambda *refs: permute_rows(*refs, lambda: None),
        out_shape=jax.ShapeDtypeStruct((n_dev, n_local, cap, x.shape[1]), BF16),
        grid_spec=pltpu.PrefetchScalarGridSpec(
            num_scalar_prefetch=1, grid=(), in_specs=[hbm], out_specs=hbm,
            scratch_shapes=permute_scratch(n_dev * n_local * cap, cap, x.shape[1])),
        cost_estimate=pl.CostEstimate(flops=20 * 10 ** 9, bytes_accessed=28 * 2 ** 20, transcendentals=0),
        compiler_params=pltpu.CompilerParams(vmem_limit_bytes=60 * 2 ** 20),
        name='permute_rows',
    )(addr, x)


def router_kernel(z_coef, slot, x, idx, w_t, v_col, gback, pieces_out, partial, acc, gtab, g_rows, w_six, pieces_t, p_acc, z_acc):
    b = pl.program_id(0)
    tb = x.shape[0]
    n_chunk, cap = gback.shape
    n = w_t.shape[0]

    @pl.when(b == 0)
    def _():
        acc[...] = jnp.zeros_like(acc)
        p_acc[...] = jnp.zeros_like(p_acc)
        z_acc[...] = jnp.zeros_like(z_acc)
        w_six[...] = six_terms(w_t[...])
        gtab[n_chunk * cap:, :] = jnp.zeros((8, LANES), F32)

        def fill(c, _):
            gtab[pl.ds(pl.multiple_of(c * cap, 8), cap), :] = jnp.broadcast_to(gback[pl.ds(c, 1), :], (LANES, cap)).T
            return 0

        lax.fori_loop(0, n_chunk, fill, 0)

    def move(i, _):
        for r in range(32):
            g_rows[pl.ds(i * 32 + r, 1), :] = gtab[pl.ds(slot[b * tb + i * 32 + r], 1), :]
        return 0

    lax.fori_loop(0, tb // 32, move, 0)

    xv = x[...]
    terms = nt(w_six[...], xv)
    logits = terms[0:n] + terms[3 * n:4 * n] + terms[5 * n:6 * n]
    top = jnp.max(logits, axis=0, keepdims=True)
    expd = jnp.exp(logits - top)
    total = jnp.sum(expd, axis=0, keepdims=True)
    prob = expd / total
    z = top + jnp.log(total)
    mine = lax.broadcasted_iota(jnp.int32, logits.shape, 0) == idx[pl.ds(b, 1), :]
    onehot = jnp.where(mine, 1.0, 0.0)
    gate = jnp.sum(jnp.where(mine, prob, 0.0), axis=0, keepdims=True)
    g = g_rows[...].T[0:1, :]
    v = v_col[:, 0:1]
    spread = jnp.sum(prob * v, axis=0, keepdims=True)
    dlog = gate * g * (onehot - prob) + prob * (v - spread) + (z_coef * z) * prob
    hi, mid, low = split3(dlog)
    pieces = jnp.concatenate([hi, mid, low, hi, mid, hi, jnp.zeros((LANES - 6 * n, tb), F32)], axis=0)
    pieces_out[...] = pieces.T.astype(BF16)
    pieces_t[...] = pieces.astype(BF16)
    acc[...] += nn(pieces_t[...], xv)
    zz = z * z
    for j in range(tb // LANES):
        p_acc[...] += prob[:, j * LANES:(j + 1) * LANES]
        z_acc[0:1, :] += zz[:, j * LANES:(j + 1) * LANES]

    @pl.when(b == pl.num_programs(0) - 1)
    def _():
        partial[...] = jnp.zeros_like(partial)
        partial[0:n, :] = acc[0:n, :] + acc[n:2 * n, :] + acc[2 * n:3 * n, :]
        p_sum = jnp.broadcast_to(jnp.sum(p_acc[...], axis=1, keepdims=True), p_acc.shape)
        p_full = jnp.concatenate([p_sum, jnp.zeros((LANES - n, LANES), F32)], axis=0).T
        partial[n:n + 1, 0:LANES] = p_full[0:1, :]
        partial[n:n + 1, LANES:2 * LANES] = jnp.broadcast_to(jnp.sum(z_acc[0:1, :], axis=1, keepdims=True), (1, LANES))


def whole(a):
    return pl.BlockSpec(a.shape, lambda b, addr: (0,) * a.ndim)


def router_side(z_coef, slot, x, idx, w_t, v_col, gback):
    tokens, d_model = x.shape
    n_dev, n_local, _, cap = gback.shape
    tb = TB
    n = w_t.shape[0]
    gback = gback.reshape(n_dev * n_local, cap)
    rows = n + 8
    return pl.pallas_call(
        lambda *refs: router_kernel(z_coef, *refs),
        out_shape=(jax.ShapeDtypeStruct((tokens, LANES), BF16), jax.ShapeDtypeStruct((rows, d_model), F32), jax.ShapeDtypeStruct((LANES, d_model), F32)),
        grid_spec=pltpu.PrefetchScalarGridSpec(
            num_scalar_prefetch=1, grid=(tokens // tb,),
            in_specs=[pl.BlockSpec((tb, d_model), lambda b, addr: (b, 0)), whole(idx), whole(w_t), whole(v_col), whole(gback)],
            out_specs=[pl.BlockSpec((tb, LANES), lambda b, addr: (b, 0)), pl.BlockSpec((rows, d_model), lambda b, addr: (0, 0)),
                       pl.BlockSpec((LANES, d_model), lambda b, addr: (0, 0))],
            scratch_shapes=[
                pltpu.VMEM((n_dev * n_local * cap + 8, LANES), F32), pltpu.VMEM((tb, LANES), F32), pltpu.VMEM((LANES, d_model), BF16),
                pltpu.VMEM((LANES, tb), BF16), pltpu.VMEM((n, LANES), F32), pltpu.VMEM((8, LANES), F32)]),
        cost_estimate=pl.CostEstimate(flops=30 * 10 ** 9, bytes_accessed=16 * 2 ** 20, transcendentals=0),
        compiler_params=pltpu.CompilerParams(vmem_limit_bytes=40 * 2 ** 20),
        name='router_side',
    )(slot, x, idx, w_t, v_col, gback)


def combine_kernel(addr, pieces, w_t, dback, dlast, grad_x, stage, table, inb, w_six, in_sem):
    b = pl.program_id(0)
    tb = pieces.shape[0]
    n_out, cap, d_model = dlast.shape
    n_local = dback.shape[1] + 1
    groups = cap // 8
    tiled = table.reshape(table.shape[0] // PITCH, PITCH, LANES)
    stage3 = stage.reshape(tb // 8, PITCH, LANES)

    @pl.when(b == 0)
    def _():
        n_buf = inb.shape[1]

        def fetch(d, e):
            source = dback.at[d, e] if e < n_local - 1 else dlast.at[d]
            return pltpu.make_async_copy(source, inb.at[e, d % n_buf], in_sem.at[e, d % n_buf])

        for d in range(n_buf):
            for e in range(n_local):
                fetch(d, e).start()
        w_six[...] = six_terms(w_t[...])
        tiled[n_out * n_local * groups] = jnp.zeros((PITCH, LANES), F32)

        def fill(d, _):
            for e in range(n_local):
                fetch(d, e).wait()
                for j in range(ROW_TILES):
                    part = inb[e, d % n_buf, :, j * LANES:(j + 1) * LANES].astype(F32)
                    tiled[pl.ds((d * n_local + e) * groups, groups), j * 8:(j + 1) * 8, :] = part.reshape(groups, 8, LANES)

                @pl.when(d + n_buf < n_out)
                def _():
                    fetch(d + n_buf, e).start()
            return 0

        lax.fori_loop(0, n_out, fill, 0)

    def move(i, _):
        for r in range(32):
            at = addr[b * tb + i * 32 + r]
            stage[row(i * (4 * PITCH) + (r // 8) * PITCH + r % 8, ROW_TILES), :] = table[row(at, ROW_TILES), :]
        return 0

    lax.fori_loop(0, tb // 32, move, 0)
    for j in range(ROW_TILES):
        cols = slice(j * LANES, (j + 1) * LANES)
        grad_x[:, cols] = (stage3[:, j * 8:(j + 1) * 8, :].reshape(tb, LANES) + nn(pieces[...], w_six[:, cols])).astype(BF16)


def combine(addr, pieces, w_t, dback, dlast):
    tokens = pieces.shape[0]
    n_dev, cap, d_model = dlast.shape
    n_local = dback.shape[1] + 1
    tb = TB
    hbm = pl.BlockSpec(memory_space=pl.ANY)
    n_groups = n_dev * n_local * cap // 8 + 1
    return pl.pallas_call(
        combine_kernel,
        out_shape=jax.ShapeDtypeStruct((tokens, d_model), BF16),
        grid_spec=pltpu.PrefetchScalarGridSpec(
            num_scalar_prefetch=1, grid=(tokens // tb,),
            in_specs=[pl.BlockSpec((tb, LANES), lambda b, addr: (b, 0)), whole(w_t), hbm, hbm],
            out_specs=pl.BlockSpec((tb, d_model), lambda b, addr: (b, 0)),
            scratch_shapes=[
                pltpu.VMEM((tb // 8 * PITCH, LANES), F32), pltpu.VMEM((n_groups * PITCH, LANES), F32),
                pltpu.VMEM((n_local, 4, cap, d_model), BF16), pltpu.VMEM((LANES, d_model), BF16), pltpu.SemaphoreType.DMA((n_local, 4))]),
        compiler_params=pltpu.CompilerParams(vmem_limit_bytes=56 * 2 ** 20),
        name='combine_rows',
    )(addr, pieces, w_t, dback, dlast)


def total_kernel(n_dev, part, _before_a, _before_b, out, stats, parts, send_sem, recv_sem):
    me = lax.axis_index('ep')
    barrier = pltpu.get_barrier_semaphore()
    peers = [(me + k) % n_dev for k in range(1, n_dev)]
    for p in peers:
        pl.semaphore_signal(barrier, inc=1, device_id=(p,), device_id_type=MESH)
    pl.semaphore_wait(barrier, n_dev - 1)
    copies = [pltpu.make_async_remote_copy(part, parts.at[me], send_sem.at[k], recv_sem.at[k], device_id=(p,), device_id_type=MESH)
              for k, p in enumerate(peers)]
    for copy in copies:
        copy.start()
    parts[me] = part[...]
    for copy in copies:
        copy.wait()
    total = parts[0]
    for d in range(1, n_dev):
        total = total + parts[d]
    n = out.shape[0]
    out[...] = total[0:n]
    stats[...] = total[n:]


def total_over_devices(n_dev, n_grad, part, before):
    vmem = pl.BlockSpec(memory_space=pltpu.VMEM)
    return pl.pallas_call(
        lambda *refs: total_kernel(n_dev, *refs),
        out_shape=(jax.ShapeDtypeStruct((n_grad, part.shape[1]), F32), jax.ShapeDtypeStruct((part.shape[0] - n_grad, part.shape[1]), F32)),
        in_specs=[vmem] + [pl.BlockSpec(memory_space=pl.ANY)] * 2, out_specs=[vmem, vmem],
        scratch_shapes=[pltpu.VMEM((n_dev,) + part.shape, F32), pltpu.SemaphoreType.DMA((n_dev - 1,)), pltpu.SemaphoreType.DMA((n_dev - 1,))],
        compiler_params=pltpu.CompilerParams(collective_id=1, has_side_effects=True),
        name='device_total',
    )(part, *before)


def copy_kernel(source, sink):
    sink[...] = source[...]


def own_copy(a):
    n, rows, cols = a.shape
    spec = pl.BlockSpec((1, rows // 6, cols), lambda e, r: (e, r, 0))
    return pl.pallas_call(
        copy_kernel, out_shape=jax.ShapeDtypeStruct(a.shape, a.dtype), grid=(n, 6), in_specs=[spec], out_specs=spec,
        cost_estimate=pl.CostEstimate(flops=15 * 10 ** 9, bytes_accessed=2 * a.size * 4, transcendentals=0),
        name='own_copy')(a)


def solution(mesh):
    n_dev = mesh.shape['ep']

    def expert_layer(x_tokens, w_router, expert_idx, w_in, w_out, grad_y):
        tokens, d_model = x_tokens.shape
        n_local = w_in.shape[0]
        num_experts = n_local * n_dev
        capacity = (5 * tokens + 4 * num_experts - 1) // (4 * num_experts)
        total_tok = tokens * n_dev
        w_t = w_router.T
        idx = expert_idx.reshape(tokens // TB, TB)
        xs, slot, addr, cnt = route_permute(n_dev, n_local, capacity, idx, x_tokens)
        slot, addr = slot.reshape(tokens), addr.reshape(tokens)
        me = lax.axis_index('ep')
        near_x, near_y = [lax.ppermute(lax.dynamic_slice(xs, (me ^ k, e, 0, 0), (1, 1, capacity, d_model)).reshape(capacity, d_model), 'ep',
                                       [(d, d ^ k) for d in range(n_dev)]) for e, k in EARLY]
        dys = permute(n_dev, n_local, capacity, addr, grad_y)

        _, _, _, d_back, d_last, g_back, gwin, gwout_t, cnt_all = expert_exchange(n_dev, xs, dys, near_x, near_y, w_t, cnt, w_in, w_out)
        d_last = lax.all_to_all(d_last, 'ep', 0, 0, tiled=True)
        load_frac = jnp.sum(cnt_all, axis=0) / total_tok
        v_col = AUX_WEIGHT * num_experts * load_frac / total_tok
        pieces, partial, _ = router_side(2.0 * Z_WEIGHT / total_tok, slot, x_tokens, idx, w_t, v_col, g_back)
        grad_w_out = jnp.swapaxes(gwout_t, 1, 2)
        grad_w_in = own_copy(gwin)
        grad_x = combine(addr, pieces, w_t, d_back, d_last)
        grad_wr_t, stats = total_over_devices(n_dev, num_experts, partial, (grad_w_in, grad_w_out))
        grad_w_router = grad_wr_t.T
        mean_prob = stats[0, :num_experts] / total_tok
        aux_loss = AUX_WEIGHT * num_experts * jnp.sum(load_frac[:, 0] * mean_prob)
        z_loss = Z_WEIGHT * stats[0, LANES] / total_tok
        return grad_x, grad_w_in, grad_w_out, grad_w_router, aux_loss, z_loss

    return jax.shard_map(expert_layer, mesh=mesh,
                         in_specs=(P('ep', None), P(None, None), P('ep'), P('ep', None, None), P('ep', None, None), P('ep', None)),
                         out_specs=(P('ep', None), P('ep', None, None), P('ep', None, None), P(None, None), P(), P()),
                         check_vma=False)
```

```python
import jax
import jax.numpy as jnp
from jax import lax
from jax.experimental import pallas as pl
from jax.experimental.pallas import tpu as pltpu
from jax.sharding import PartitionSpec as P

AUX_WEIGHT = 0.01
Z_WEIGHT = 0.001
MESH = pl.DeviceIdType.MESH
F32 = jnp.float32
BF16 = jnp.bfloat16
LANES = 128


def split3(w):
    hi = w.astype(BF16).astype(F32)
    mid = (w - hi).astype(BF16).astype(F32)
    return hi, mid, w - hi - mid


def six_terms(w):
    hi, mid, low = split3(w)
    pad = jnp.zeros((LANES - 6 * w.shape[0], w.shape[1]), F32)
    return jnp.concatenate([hi, hi, hi, mid, mid, low, pad], axis=0).astype(BF16)


def nt(a, b):
    return lax.dot_general(a, b, (((1,), (1,)), ((), ())), preferred_element_type=F32)


def nn(a, b):
    return jnp.dot(a, b, preferred_element_type=F32)


EARLY = ((0, 2), (0, 4))


def expert_kernel(n_dev, n_local, num_experts, blk, xs, dys, near_x, near_y, w_t, cnt, w_in, w_out,
                  xr, dyr, dsend, dback, dlast, gback, gwin, gwout_t, cnt_all,
                  xv, dyv, gv, x_t, g_t, wr, win_v, wout_v, acc_in, acc_out, o_acc, r_acc, r_out, g_all,
                  x_send, x_recv, dy_send, dy_recv, r_send, r_recv, s_send, s_recv, c_send, c_recv, ld_sem, st_sem, w_sem, flush_sem, own_sem):
    me = lax.axis_index('ep')
    n_blk = w_in.shape[2] // blk
    n_chunk = n_local * n_dev

    def peer_of(k):
        out = 0
        bit = 1
        while bit < n_dev:
            out = out + bit * (((me // bit) + (k // bit)) % 2)
            bit *= 2
        return out

    barrier = pltpu.get_barrier_semaphore()
    for k in range(1, n_dev):
        pl.semaphore_signal(barrier, inc=1, device_id=(peer_of(k),), device_id_type=MESH)
    pl.semaphore_wait(barrier, n_dev - 1)

    def x_copy(k, e):
        p = peer_of(k)
        return pltpu.make_async_remote_copy(xs.at[p, e], xr.at[me, e], x_send.at[e, k], x_recv.at[e, k], device_id=(p,), device_id_type=MESH)

    def dy_copy(k, e):
        p = peer_of(k)
        return pltpu.make_async_remote_copy(dys.at[p, e], dyr.at[me, e], dy_send.at[e, k], dy_recv.at[e, k], device_id=(p,), device_id_type=MESH)

    def r_copy(k, e):
        p = peer_of(k)
        return pltpu.make_async_remote_copy(dsend.at[p, e], dback.at[me, e], r_send.at[e, k], r_recv.at[e, k], device_id=(p,), device_id_type=MESH)

    def s_copy(k, e):
        p = peer_of(k)
        return pltpu.make_async_remote_copy(g_all.at[e, k], gback.at[me, e], s_send.at[e, k], s_recv.at[e, k], device_id=(p,), device_id_type=MESH)

    def c_copy(k):
        p = peer_of(k)
        return pltpu.make_async_remote_copy(cnt, cnt_all.at[me], c_send.at[k], c_recv.at[k], device_id=(p,), device_id_type=MESH)

    own_cnt = pltpu.make_async_copy(cnt, cnt_all.at[me], own_sem.at[n_local])
    own_cnt.start()
    for k in range(1, n_dev):
        c_copy(k).start()
    for e in range(n_local):
        for k in (1, 2, 4, 6, 3, 5, 7):
            if (e, k) not in EARLY:
                x_copy(k, e).start()
            dy_copy(k, e).start()

    order = (0, 1, 2, 4, 6, 3, 5, 7)

    def offset_of(i):
        k = i * 0
        for at, val in enumerate(order):
            k = k + jnp.where(i == at, val, 0)
        return k

    def load(e, i, slot, do):
        k = offset_of(i)
        p = peer_of(k)

        early = (e == 0) & ((i == 2) | (i == 3))

        def x_from(source):
            do(pltpu.make_async_copy(source, xv.at[slot], ld_sem.at[slot, 0]))

        @pl.when(i == 0)
        def _():
            x_from(xs.at[me, e])
            do(pltpu.make_async_copy(dys.at[me, e], dyv.at[slot], ld_sem.at[slot, 1]))

        @pl.when((e == 0) & (i == 2))
        def _():
            x_from(near_x)

        @pl.when((e == 0) & (i == 3))
        def _():
            x_from(near_y)

        @pl.when((i > 0) & jnp.logical_not(early))
        def _():
            x_from(xr.at[p, e])

        @pl.when(i > 0)
        def _():
            do(pltpu.make_async_copy(dyr.at[p, e], dyv.at[slot], ld_sem.at[slot, 1]))

    def arrive(e, i):
        k = offset_of(i)

        @pl.when((i > 0) & jnp.logical_not((e == 0) & ((i == 2) | (i == 3))))
        def _():
            x_copy(k, e).wait_recv()

        @pl.when(i > 0)
        def _():
            dy_copy(k, e).wait_recv()

    def store(c, do):
        e, i = c // n_dev, c % n_dev
        k = offset_of(i)
        p = peer_of(k)

        @pl.when(e == n_local - 1)
        def _():
            do(pltpu.make_async_copy(r_out.at[c % 2], dlast.at[p], st_sem.at[c % 2]))

        @pl.when(e < n_local - 1)
        def _():
            @pl.when(i == 0)
            def _():
                do(pltpu.make_async_copy(r_out.at[c % 2], dback.at[me, e], st_sem.at[c % 2]))

            @pl.when(i > 0)
            def _():
                do(pltpu.make_async_copy(r_out.at[c % 2], dsend.at[p, e], st_sem.at[c % 2]))

    def own_g(e):
        return pltpu.make_async_copy(g_all.at[e, 0], gback.at[me, e], own_sem.at[e])

    def send_back(c):
        e, i = c // n_dev, c % n_dev
        k = offset_of(i)
        store(c, lambda cp: cp.wait())

        @pl.when(i == 0)
        def _():
            own_g(e).start()

        @pl.when(i > 0)
        def _():
            s_copy(k, e).start()

            @pl.when(e < n_local - 1)
            def _():
                r_copy(k, e).start()

    def weights(e):
        return (pltpu.make_async_copy(w_in.at[e], win_v, w_sem.at[0]), pltpu.make_async_copy(w_out.at[e], wout_v, w_sem.at[1]))

    def flush(e):
        return (pltpu.make_async_copy(acc_in, gwin.at[e], flush_sem.at[0]), pltpu.make_async_copy(acc_out, gwout_t.at[e], flush_sem.at[1]))

    for cp in weights(0):
        cp.start()
    load(0 * me, 0 * me, 0, lambda cp: cp.start())
    for at, piece in enumerate(split3(w_t[...])):
        pad = jnp.zeros((LANES - num_experts, piece.shape[1]), F32)
        wr[at] = jnp.concatenate([piece, pad], axis=0).T.astype(BF16)

    def chunk(c, _):
        e, i = c // n_dev, c % n_dev
        k = offset_of(i)
        slot = c % 2

        @pl.when(i == 0)
        def _():
            @pl.when(c > 0)
            def _():
                for cp in weights(e):
                    cp.start()
                for cp in flush(e - 1):
                    cp.wait()
            acc_in[...] = jnp.zeros_like(acc_in)
            acc_out[...] = jnp.zeros_like(acc_out)
            for cp in weights(e):
                cp.wait()

        load(e, i, slot, lambda cp: cp.wait())
        x = xv[slot]
        logits = nn(x, wr[0]) + nn(x, wr[1]) + nn(x, wr[2])
        lane = lax.broadcasted_iota(jnp.int32, logits.shape, 1)
        logits = jnp.where(lane < num_experts, logits, -1e30)
        prob = jnp.exp(logits - jnp.max(logits, axis=1, keepdims=True))
        mine = jnp.sum(jnp.where(lane == me * n_local + e, prob, 0.0), axis=1, keepdims=True)
        gate = mine / jnp.sum(prob, axis=1, keepdims=True)
        grad = (gate * dyv[slot].astype(F32)).astype(BF16)
        gv[...] = grad
        x_t[...] = x.T
        g_t[...] = grad.T
        o_acc[...] = jnp.zeros_like(o_acc)
        r_acc[...] = jnp.zeros_like(r_acc)

        def block(f, _):
            @pl.when(f == n_blk - 1)
            def _():
                @pl.when(c + 1 < n_chunk)
                def _():
                    ne, ni = (c + 1) // n_dev, (c + 1) % n_dev
                    arrive(ne, ni)
                    load(ne, ni, 1 - slot, lambda cp: cp.start())

            @pl.when(f == 1)
            def _():
                @pl.when(c > 0)
                def _():
                    send_back(c - 1)

            cols = pl.ds(pl.multiple_of(f * blk, LANES), blk)
            win = win_v[:, cols]
            wout = wout_v[cols, :]
            hidden = jnp.maximum(nn(xv[slot], win), 0.0).astype(BF16)
            d_hidden = nt(gv[...], wout)
            d_pre = jnp.where(hidden > 0, d_hidden, 0.0).astype(BF16)
            o_acc[...] += nn(hidden, wout)
            r_acc[...] += nt(d_pre, win)
            acc_out[:, cols] += nn(g_t[...], hidden)
            acc_in[:, cols] += nn(x_t[...], d_pre)
            return 0

        lax.fori_loop(0, n_blk, block, 0)
        r_out[slot] = r_acc[...].astype(BF16)
        store(c, lambda cp: cp.start())
        g_val = jnp.sum(o_acc[...].astype(BF16).astype(F32) * dyv[slot].astype(F32), axis=1, keepdims=True)
        g_row = jnp.broadcast_to(g_val, (g_val.shape[0], LANES)).T
        g_all[e, k] = g_row[0:1, :]

        @pl.when(i == n_dev - 1)
        def _():
            for cp in flush(e):
                cp.start()
        return 0

    lax.fori_loop(0, n_chunk, chunk, 0)
    send_back(n_chunk - 1)
    for cp in flush(n_local - 1):
        cp.wait()
    own_cnt.wait()
    for k in range(1, n_dev):
        c_copy(k).wait()
    for e in range(n_local):
        own_g(e).wait()
        for k in range(1, n_dev):
            if (e, k) not in EARLY:
                x_copy(k, e).wait_send()
            dy_copy(k, e).wait_send()
            if e < n_local - 1:
                r_copy(k, e).wait()
            s_copy(k, e).wait()


def expert_exchange(n_dev, xs, dys, near_x, near_y, w_t, cnt, w_in, w_out):
    n_local, d_model, d_ff = w_in.shape
    cap = xs.shape[2]
    num_experts = n_dev * n_local
    blk = d_ff // 4
    hbm = pl.BlockSpec(memory_space=pl.ANY)
    vmem = pl.BlockSpec(memory_space=pltpu.VMEM)
    rows = jax.ShapeDtypeStruct(xs.shape, BF16)
    early = jax.ShapeDtypeStruct((n_dev, n_local - 1, cap, d_model), BF16)
    late = jax.ShapeDtypeStruct((n_dev, cap, d_model), BF16)
    g_shape = jax.ShapeDtypeStruct((n_dev, n_local, 1, cap), F32)
    w_shape = jax.ShapeDtypeStruct((n_local, d_model, d_ff), F32)
    dma = pltpu.SemaphoreType.DMA
    pair = (n_local, n_dev)
    return pl.pallas_call(
        lambda *refs: expert_kernel(n_dev, n_local, num_experts, blk, *refs),
        out_shape=(rows, rows, early, early, late, g_shape, w_shape, w_shape, jax.ShapeDtypeStruct((n_dev,) + cnt.shape, F32)),
        in_specs=[hbm, hbm, hbm, hbm, vmem, vmem, hbm, hbm],
        out_specs=[hbm] * 9,
        scratch_shapes=[
            pltpu.VMEM((2, cap, d_model), BF16), pltpu.VMEM((2, cap, d_model), BF16), pltpu.VMEM((cap, d_model), BF16),
            pltpu.VMEM((d_model, cap), BF16), pltpu.VMEM((d_model, cap), BF16), pltpu.VMEM((3, d_model, LANES), BF16),
            pltpu.VMEM((d_model, d_ff), BF16), pltpu.VMEM((d_ff, d_model), BF16),
            pltpu.VMEM((d_model, d_ff), F32), pltpu.VMEM((d_model, d_ff), F32),
            pltpu.VMEM((cap, d_model), F32), pltpu.VMEM((cap, d_model), F32),
            pltpu.VMEM((2, cap, d_model), BF16), pltpu.VMEM((n_local, n_dev, 1, cap), F32),
            dma(pair), dma(pair), dma(pair), dma(pair), dma(pair), dma(pair), dma(pair), dma(pair), dma((n_dev,)), dma((n_dev,)),
            dma((2, 2)), dma((2,)), dma((2,)), dma((2,)), dma((n_local + 1,)),
        ],
        compiler_params=pltpu.CompilerParams(collective_id=0, has_side_effects=True, vmem_limit_bytes=63 * 2 ** 20),
        name='expert_exchange',
    )(xs, dys, near_x, near_y, w_t, cnt, w_in, w_out)


PITCH = 6 * 8
ROW_TILES = 6


def row(addr, tiles):
    return pl.ds(addr, tiles, stride=8)


TB = 512
IN_FLIGHT = 4


def permute_rows(addr, source, sink, inb, stage, table, outb, in_sem, out_sem, meanwhile, extra):
    n_out, n_local, cap, d_model = sink.shape
    groups = cap // 8
    tiled = table.reshape(table.shape[0] // PITCH, PITCH, LANES)
    stage3 = stage.reshape(TB // 8, PITCH, LANES)
    n_in = source.shape[0] // TB
    n_chunk = n_out * n_local

    def fetch(b):
        return pltpu.make_async_copy(source.at[pl.ds(pl.multiple_of(b * TB, TB), TB), :], inb.at[b % IN_FLIGHT], in_sem.at[b % IN_FLIGHT])

    def emit(c):
        return pltpu.make_async_copy(outb.at[c], sink.at[c // n_local, c % n_local], out_sem.at[c])

    for b in range(IN_FLIGHT - 1):
        fetch(b).start()
    table[...] = jnp.zeros_like(table)
    meanwhile()

    def scatter(b, _):
        @pl.when(b + IN_FLIGHT - 1 < n_in)
        def _():
            fetch(b + IN_FLIGHT - 1).start()
        fetch(b).wait()
        for j in range(ROW_TILES):
            part = inb[b % IN_FLIGHT, :, j * LANES:(j + 1) * LANES].astype(F32)
            stage3[:, j * 8:(j + 1) * 8, :] = part.reshape(TB // 8, 8, LANES)

        def move(i, _):
            for r in range(32):
                at = addr[b * TB + i * 32 + r]
                table[row(at, ROW_TILES), :] = stage[row(i * (4 * PITCH) + (r // 8) * PITCH + r % 8, ROW_TILES), :]
            return 0

        lax.fori_loop(0, TB // 32, move, 0)
        return 0

    lax.fori_loop(0, n_in, scatter, 0)

    def drain(c, _):
        for j in range(ROW_TILES):
            part = tiled[pl.ds(c * groups, groups), j * 8:(j + 1) * 8, :].reshape(cap, LANES)
            outb[c, :, j * LANES:(j + 1) * LANES] = part.astype(BF16)
        emit(c).start()
        return 0

    def finish(c, _):
        emit(c).wait()
        return 0

    lax.fori_loop(0, n_chunk, drain, 0)
    extra(outb)
    lax.fori_loop(0, n_chunk, finish, 0)


def route_permute_kernel(idx, x, xs, near_x, near_y, slot_out, addr_out, count_out, addr, addr_sem, near_sem, *scratch):
    n_out, n_local, cap, _ = xs.shape
    n = n_out * n_local

    def route():
        below = lax.broadcasted_iota(jnp.int32, (TB, TB), 0) <= lax.broadcasted_iota(jnp.int32, (TB, TB), 1)
        upper = jnp.where(below, 1.0, 0.0).astype(BF16)
        expert = lax.broadcasted_iota(jnp.int32, (n, TB), 0)
        seen = jnp.zeros((n, 1), F32)
        for b in range(idx.shape[0]):
            mine = expert == idx[b:b + 1, :]
            onehot = jnp.where(mine, 1.0, 0.0)
            rank = nn(onehot.astype(BF16), upper)
            pos = jnp.sum(jnp.where(mine, rank + (seen - 1.0), 0.0), axis=0, keepdims=True).astype(jnp.int32)
            slot = jnp.where(pos < cap, idx[b:b + 1, :] * cap + pos, n * cap)
            slot_out[b:b + 1, :] = slot
            group = lax.shift_right_logical(slot, jnp.full_like(slot, 3))
            addr_out[b:b + 1, :] = group * PITCH + (slot - group * 8)
            seen = seen + rank[:, TB - 1:TB]
        count_out[...] = jnp.broadcast_to(seen, count_out.shape)
        load_table(addr_out, addr, addr_sem)

    def near(outb):
        me = lax.axis_index('ep')
        copies = []
        for at, ((e, k), sink) in enumerate(zip(EARLY, (near_x, near_y))):
            p = me + k - 2 * k * ((me // k) % 2)
            copies.append(pltpu.make_async_copy(outb.at[p * n_local + e], sink, near_sem.at[at]))
        for copy in copies:
            copy.start()
        for copy in copies:
            copy.wait()

    permute_rows(addr, x, xs, *scratch, route, near)


def permute_scratch(n_slots, cap, d_model):
    return [pltpu.VMEM((IN_FLIGHT, TB, d_model), BF16), pltpu.VMEM((TB // 8 * PITCH, LANES), F32), pltpu.VMEM(((n_slots // 8 + 1) * PITCH, LANES), F32),
            pltpu.VMEM((n_slots // cap, cap, d_model), BF16), pltpu.SemaphoreType.DMA((IN_FLIGHT,)), pltpu.SemaphoreType.DMA((n_slots // cap,))]


def route_permute(n_dev, n_local, cap, idx, x):
    hbm = pl.BlockSpec(memory_space=pl.ANY)
    vmem = pl.BlockSpec(memory_space=pltpu.VMEM)
    table = jax.ShapeDtypeStruct(idx.shape, jnp.int32)
    n = n_dev * n_local
    block = jax.ShapeDtypeStruct((cap, x.shape[1]), BF16)
    return pl.pallas_call(
        route_permute_kernel,
        out_shape=(jax.ShapeDtypeStruct((n_dev, n_local, cap, x.shape[1]), BF16), block, block, table, table, jax.ShapeDtypeStruct((n, LANES), F32)),
        in_specs=[vmem, hbm], out_specs=[hbm, hbm, hbm, vmem, vmem, vmem],
        scratch_shapes=[pltpu.SMEM((idx.size,), jnp.int32), pltpu.SemaphoreType.DMA((idx.shape[0],)), pltpu.SemaphoreType.DMA((2,))] + permute_scratch(n * cap, cap, x.shape[1]),
        compiler_params=pltpu.CompilerParams(vmem_limit_bytes=60 * 2 ** 20),
        name='route_permute',
    )(idx, x)


def load_table(table, addr, sem):
    copies = [pltpu.make_async_copy(table.at[b], addr.at[pl.ds(b * TB, TB)], sem.at[b]) for b in range(table.shape[0])]
    for copy in copies:
        copy.start()
    for copy in copies:
        copy.wait()


def permute_kernel(table, x, xs, addr, addr_sem, *scratch):
    permute_rows(addr, x, xs, *scratch, lambda: load_table(table, addr, addr_sem), lambda outb: None)


def permute(n_dev, n_local, cap, addr, x):
    hbm = pl.BlockSpec(memory_space=pl.ANY)
    return pl.pallas_call(
        permute_kernel,
        out_shape=jax.ShapeDtypeStruct((n_dev, n_local, cap, x.shape[1]), BF16),
        in_specs=[pl.BlockSpec(memory_space=pltpu.VMEM), hbm], out_specs=hbm,
        scratch_shapes=[pltpu.SMEM((addr.size,), jnp.int32), pltpu.SemaphoreType.DMA((addr.shape[0],))]
        + permute_scratch(n_dev * n_local * cap, cap, x.shape[1]),
        cost_estimate=pl.CostEstimate(flops=20 * 10 ** 9, bytes_accessed=28 * 2 ** 20, transcendentals=0),
        compiler_params=pltpu.CompilerParams(vmem_limit_bytes=60 * 2 ** 20),
        name='permute_rows',
    )(addr, x)


def router_kernel(z_coef, slot, x, idx, w_t, v_col, gback, pieces_out, partial, acc, gtab, g_rows, w_six, pieces_t, p_acc, z_acc):
    b = pl.program_id(0)
    tb = x.shape[0]
    n_chunk, cap = gback.shape
    n = w_t.shape[0]

    @pl.when(b == 0)
    def _():
        acc[...] = jnp.zeros_like(acc)
        p_acc[...] = jnp.zeros_like(p_acc)
        z_acc[...] = jnp.zeros_like(z_acc)
        w_six[...] = six_terms(w_t[...])
        gtab[n_chunk * cap:, :] = jnp.zeros((8, LANES), F32)

        def fill(c, _):
            gtab[pl.ds(pl.multiple_of(c * cap, 8), cap), :] = jnp.broadcast_to(gback[pl.ds(c, 1), :], (LANES, cap)).T
            return 0

        lax.fori_loop(0, n_chunk, fill, 0)

    def move(i, _):
        for r in range(32):
            g_rows[pl.ds(i * 32 + r, 1), :] = gtab[pl.ds(slot[b * tb + i * 32 + r], 1), :]
        return 0

    lax.fori_loop(0, tb // 32, move, 0)

    xv = x[...]
    terms = nt(w_six[...], xv)
    logits = terms[0:n] + terms[3 * n:4 * n] + terms[5 * n:6 * n]
    top = jnp.max(logits, axis=0, keepdims=True)
    expd = jnp.exp(logits - top)
    total = jnp.sum(expd, axis=0, keepdims=True)
    prob = expd / total
    z = top + jnp.log(total)
    mine = lax.broadcasted_iota(jnp.int32, logits.shape, 0) == idx[pl.ds(b, 1), :]
    onehot = jnp.where(mine, 1.0, 0.0)
    gate = jnp.sum(jnp.where(mine, prob, 0.0), axis=0, keepdims=True)
    g = g_rows[...].T[0:1, :]
    v = v_col[:, 0:1]
    spread = jnp.sum(prob * v, axis=0, keepdims=True)
    dlog = gate * g * (onehot - prob) + prob * (v - spread) + (z_coef * z) * prob
    hi, mid, low = split3(dlog)
    pieces = jnp.concatenate([hi, mid, low, hi, mid, hi, jnp.zeros((LANES - 6 * n, tb), F32)], axis=0)
    pieces_out[...] = pieces.T.astype(BF16)
    pieces_t[...] = pieces.astype(BF16)
    acc[...] += nn(pieces_t[...], xv)
    zz = z * z
    for j in range(tb // LANES):
        p_acc[...] += prob[:, j * LANES:(j + 1) * LANES]
        z_acc[0:1, :] += zz[:, j * LANES:(j + 1) * LANES]

    @pl.when(b == pl.num_programs(0) - 1)
    def _():
        partial[...] = jnp.zeros_like(partial)
        partial[0:n, :] = acc[0:n, :] + acc[n:2 * n, :] + acc[2 * n:3 * n, :]
        p_sum = jnp.broadcast_to(jnp.sum(p_acc[...], axis=1, keepdims=True), p_acc.shape)
        p_full = jnp.concatenate([p_sum, jnp.zeros((LANES - n, LANES), F32)], axis=0).T
        partial[n:n + 1, 0:LANES] = p_full[0:1, :]
        partial[n:n + 1, LANES:2 * LANES] = jnp.broadcast_to(jnp.sum(z_acc[0:1, :], axis=1, keepdims=True), (1, LANES))


def whole(a):
    return pl.BlockSpec(a.shape, lambda b, addr: (0,) * a.ndim)


def router_side(z_coef, slot, x, idx, w_t, v_col, gback):
    tokens, d_model = x.shape
    n_dev, n_local, _, cap = gback.shape
    tb = TB
    n = w_t.shape[0]
    gback = gback.reshape(n_dev * n_local, cap)
    rows = n + 8
    return pl.pallas_call(
        lambda *refs: router_kernel(z_coef, *refs),
        out_shape=(jax.ShapeDtypeStruct((tokens, LANES), BF16), jax.ShapeDtypeStruct((rows, d_model), F32), jax.ShapeDtypeStruct((LANES, d_model), F32)),
        grid_spec=pltpu.PrefetchScalarGridSpec(
            num_scalar_prefetch=1, grid=(tokens // tb,),
            in_specs=[pl.BlockSpec((tb, d_model), lambda b, addr: (b, 0)), whole(idx), whole(w_t), whole(v_col), whole(gback)],
            out_specs=[pl.BlockSpec((tb, LANES), lambda b, addr: (b, 0)), pl.BlockSpec((rows, d_model), lambda b, addr: (0, 0)),
                       pl.BlockSpec((LANES, d_model), lambda b, addr: (0, 0))],
            scratch_shapes=[
                pltpu.VMEM((n_dev * n_local * cap + 8, LANES), F32), pltpu.VMEM((tb, LANES), F32), pltpu.VMEM((LANES, d_model), BF16),
                pltpu.VMEM((LANES, tb), BF16), pltpu.VMEM((n, LANES), F32), pltpu.VMEM((8, LANES), F32)]),
        cost_estimate=pl.CostEstimate(flops=30 * 10 ** 9, bytes_accessed=16 * 2 ** 20, transcendentals=0),
        compiler_params=pltpu.CompilerParams(vmem_limit_bytes=40 * 2 ** 20),
        name='router_side',
    )(slot, x, idx, w_t, v_col, gback)


def combine_kernel(addr, pieces, w_t, dback, dlast, grad_x, stage, table, inb, w_six, in_sem):
    b = pl.program_id(0)
    tb = pieces.shape[0]
    n_out, cap, d_model = dlast.shape
    n_local = dback.shape[1] + 1
    groups = cap // 8
    tiled = table.reshape(table.shape[0] // PITCH, PITCH, LANES)
    stage3 = stage.reshape(tb // 8, PITCH, LANES)

    @pl.when(b == 0)
    def _():
        n_buf = inb.shape[1]

        def fetch(d, e):
            source = dback.at[d, e] if e < n_local - 1 else dlast.at[d]
            return pltpu.make_async_copy(source, inb.at[e, d % n_buf], in_sem.at[e, d % n_buf])

        for d in range(n_buf):
            for e in range(n_local):
                fetch(d, e).start()
        w_six[...] = six_terms(w_t[...])
        tiled[n_out * n_local * groups] = jnp.zeros((PITCH, LANES), F32)

        def fill(d, _):
            for e in range(n_local):
                fetch(d, e).wait()
                for j in range(ROW_TILES):
                    part = inb[e, d % n_buf, :, j * LANES:(j + 1) * LANES].astype(F32)
                    tiled[pl.ds((d * n_local + e) * groups, groups), j * 8:(j + 1) * 8, :] = part.reshape(groups, 8, LANES)

                @pl.when(d + n_buf < n_out)
                def _():
                    fetch(d + n_buf, e).start()
            return 0

        lax.fori_loop(0, n_out, fill, 0)

    def move(i, _):
        for r in range(32):
            at = addr[b * tb + i * 32 + r]
            stage[row(i * (4 * PITCH) + (r // 8) * PITCH + r % 8, ROW_TILES), :] = table[row(at, ROW_TILES), :]
        return 0

    lax.fori_loop(0, tb // 32, move, 0)
    for j in range(ROW_TILES):
        cols = slice(j * LANES, (j + 1) * LANES)
        grad_x[:, cols] = (stage3[:, j * 8:(j + 1) * 8, :].reshape(tb, LANES) + nn(pieces[...], w_six[:, cols])).astype(BF16)


def combine(addr, pieces, w_t, dback, dlast):
    tokens = pieces.shape[0]
    n_dev, cap, d_model = dlast.shape
    n_local = dback.shape[1] + 1
    tb = 2 * TB
    hbm = pl.BlockSpec(memory_space=pl.ANY)
    n_groups = n_dev * n_local * cap // 8 + 1
    return pl.pallas_call(
        combine_kernel,
        out_shape=jax.ShapeDtypeStruct((tokens, d_model), BF16),
        grid_spec=pltpu.PrefetchScalarGridSpec(
            num_scalar_prefetch=1, grid=(tokens // tb,),
            in_specs=[pl.BlockSpec((tb, LANES), lambda b, addr: (b, 0)), whole(w_t), hbm, hbm],
            out_specs=pl.BlockSpec((tb, d_model), lambda b, addr: (b, 0)),
            scratch_shapes=[
                pltpu.VMEM((tb // 8 * PITCH, LANES), F32), pltpu.VMEM((n_groups * PITCH, LANES), F32),
                pltpu.VMEM((n_local, 4, cap, d_model), BF16), pltpu.VMEM((LANES, d_model), BF16), pltpu.SemaphoreType.DMA((n_local, 4))]),
        compiler_params=pltpu.CompilerParams(vmem_limit_bytes=56 * 2 ** 20),
        name='combine_rows',
    )(addr, pieces, w_t, dback, dlast)


def total_kernel(n_dev, total_tok, part, load, _before_a, _before_b, out, aux, zl, parts, send_sem, recv_sem):
    me = lax.axis_index('ep')
    barrier = pltpu.get_barrier_semaphore()
    peers = [(me + k) % n_dev for k in range(1, n_dev)]
    for p in peers:
        pl.semaphore_signal(barrier, inc=1, device_id=(p,), device_id_type=MESH)
    pl.semaphore_wait(barrier, n_dev - 1)
    copies = [pltpu.make_async_remote_copy(part, parts.at[me], send_sem.at[k], recv_sem.at[k], device_id=(p,), device_id_type=MESH)
              for k, p in enumerate(peers)]
    for copy in copies:
        copy.start()
    parts[me] = part[...]
    for copy in copies:
        copy.wait()
    total = parts[0]
    for d in range(1, n_dev):
        total = total + parts[d]
    n = out.shape[0]
    out[...] = total[0:n]
    load_row = jnp.concatenate([load[...], jnp.zeros((LANES - n, LANES), F32)], axis=0).T[0:1, :]
    aux[0, 0] = AUX_WEIGHT * n * jnp.sum(load_row * (total[n:n + 1, 0:LANES] / total_tok))
    zl[0, 0] = Z_WEIGHT * jnp.max(total[n:n + 1, LANES:2 * LANES]) / total_tok


def total_over_devices(n_dev, total_tok, part, load, before):
    vmem = pl.BlockSpec(memory_space=pltpu.VMEM)
    smem = pl.BlockSpec(memory_space=pltpu.SMEM)
    one = jax.ShapeDtypeStruct((1, 1), F32)
    return pl.pallas_call(
        lambda *refs: total_kernel(n_dev, total_tok, *refs),
        out_shape=(jax.ShapeDtypeStruct((load.shape[0], part.shape[1]), F32), one, one),
        in_specs=[vmem, vmem] + [pl.BlockSpec(memory_space=pl.ANY)] * 2, out_specs=[vmem, smem, smem],
        scratch_shapes=[pltpu.VMEM((n_dev,) + part.shape, F32), pltpu.SemaphoreType.DMA((n_dev - 1,)), pltpu.SemaphoreType.DMA((n_dev - 1,))],
        compiler_params=pltpu.CompilerParams(collective_id=1, has_side_effects=True),
        name='device_total',
    )(part, load, *before)


def copy_kernel(source, sink):
    sink[...] = source[...]


def own_copy(a):
    n, rows, cols = a.shape
    spec = pl.BlockSpec((1, rows // 6, cols), lambda e, r: (e, r, 0))
    return pl.pallas_call(
        copy_kernel, out_shape=jax.ShapeDtypeStruct(a.shape, a.dtype), grid=(n, 6), in_specs=[spec], out_specs=spec,
        cost_estimate=pl.CostEstimate(flops=15 * 10 ** 9, bytes_accessed=2 * a.size * 4, transcendentals=0),
        name='own_copy')(a)


def solution(mesh):
    n_dev = mesh.shape['ep']

    def expert_layer(x_tokens, w_router, expert_idx, w_in, w_out, grad_y):
        tokens, d_model = x_tokens.shape
        n_local = w_in.shape[0]
        num_experts = n_local * n_dev
        capacity = (5 * tokens + 4 * num_experts - 1) // (4 * num_experts)
        total_tok = tokens * n_dev
        w_t = w_router.T
        idx = expert_idx.reshape(tokens // TB, TB)
        xs, near_x, near_y, slot, addr, cnt = route_permute(n_dev, n_local, capacity, idx, x_tokens)
        near_x, near_y = [lax.ppermute(block, 'ep', [(d, d ^ k) for d in range(n_dev)]) for block, (_, k) in zip((near_x, near_y), EARLY)]
        dys = permute(n_dev, n_local, capacity, addr, grad_y)
        slot, addr = slot.reshape(tokens), addr.reshape(tokens)

        _, _, _, d_back, d_last, g_back, gwin, gwout_t, cnt_all = expert_exchange(n_dev, xs, dys, near_x, near_y, w_t, cnt, w_in, w_out)
        d_last = lax.all_to_all(d_last, 'ep', 0, 0, tiled=True)
        load_frac = jnp.sum(cnt_all, axis=0) / total_tok
        v_col = AUX_WEIGHT * num_experts * load_frac / total_tok
        pieces, partial, _ = router_side(2.0 * Z_WEIGHT / total_tok, slot, x_tokens, idx, w_t, v_col, g_back)
        grad_w_out = jnp.swapaxes(gwout_t, 1, 2)
        grad_w_in = own_copy(gwin)
        grad_x = combine(addr, pieces, w_t, d_back, d_last)
        grad_wr_t, aux_loss, z_loss = total_over_devices(n_dev, total_tok, partial, load_frac, (grad_w_in, grad_w_out))
        grad_w_router, aux_loss, z_loss = grad_wr_t.T, aux_loss.reshape(()), z_loss.reshape(())
        return grad_x, grad_w_in, grad_w_out, grad_w_router, aux_loss, z_loss

    return jax.shard_map(expert_layer, mesh=mesh,
                         in_specs=(P('ep', None), P(None, None), P('ep'), P('ep', None, None), P('ep', None, None), P('ep', None)),
                         out_specs=(P('ep', None), P('ep', None, None), P('ep', None, None), P(None, None), P(), P()),
                         check_vma=False)
```

```python
import jax
import jax.numpy as jnp
from jax import lax
from jax.experimental import pallas as pl
from jax.experimental.pallas import tpu as pltpu
from jax.sharding import PartitionSpec as P

AUX_WEIGHT = 0.01
Z_WEIGHT = 0.001
MESH = pl.DeviceIdType.MESH
F32 = jnp.float32
BF16 = jnp.bfloat16
LANES = 128


def split3(w):
    hi = w.astype(BF16).astype(F32)
    mid = (w - hi).astype(BF16).astype(F32)
    return hi, mid, w - hi - mid


def six_terms(w):
    hi, mid, low = split3(w)
    pad = jnp.zeros((LANES - 6 * w.shape[0], w.shape[1]), F32)
    return jnp.concatenate([hi, hi, hi, mid, mid, low, pad], axis=0).astype(BF16)


def nt(a, b):
    return lax.dot_general(a, b, (((1,), (1,)), ((), ())), preferred_element_type=F32)


def nn(a, b):
    return jnp.dot(a, b, preferred_element_type=F32)


EARLY = ((0, 2), (0, 4))


def expert_kernel(n_dev, n_local, num_experts, blk, xs, dys, near_x, near_y, w_t, cnt, w_in, w_out,
                  xr, dyr, dsend, dback, dlast, gback, gwin, gwout_t, cnt_all,
                  xv, dyv, gv, x_t, g_t, wr, win_v, wout_v, acc_in, acc_out, o_acc, r_acc, r_out, g_all,
                  x_send, x_recv, dy_send, dy_recv, r_send, r_recv, s_send, s_recv, c_send, c_recv, ld_sem, st_sem, w_sem, flush_sem, own_sem):
    me = lax.axis_index('ep')
    n_blk = w_in.shape[2] // blk
    n_chunk = n_local * n_dev

    def peer_of(k):
        out = 0
        bit = 1
        while bit < n_dev:
            out = out + bit * (((me // bit) + (k // bit)) % 2)
            bit *= 2
        return out

    barrier = pltpu.get_barrier_semaphore()
    for k in range(1, n_dev):
        pl.semaphore_signal(barrier, inc=1, device_id=(peer_of(k),), device_id_type=MESH)
    pl.semaphore_wait(barrier, n_dev - 1)

    def x_copy(k, e):
        p = peer_of(k)
        return pltpu.make_async_remote_copy(xs.at[p, e], xr.at[me, e], x_send.at[e, k], x_recv.at[e, k], device_id=(p,), device_id_type=MESH)

    def dy_copy(k, e):
        p = peer_of(k)
        return pltpu.make_async_remote_copy(dys.at[p, e], dyr.at[me, e], dy_send.at[e, k], dy_recv.at[e, k], device_id=(p,), device_id_type=MESH)

    def r_copy(k, e):
        p = peer_of(k)
        return pltpu.make_async_remote_copy(dsend.at[p, e], dback.at[me, e], r_send.at[e, k], r_recv.at[e, k], device_id=(p,), device_id_type=MESH)

    def s_copy(k, e):
        p = peer_of(k)
        return pltpu.make_async_remote_copy(g_all.at[e, k], gback.at[me, e], s_send.at[e, k], s_recv.at[e, k], device_id=(p,), device_id_type=MESH)

    def c_copy(k):
        p = peer_of(k)
        return pltpu.make_async_remote_copy(cnt, cnt_all.at[me], c_send.at[k], c_recv.at[k], device_id=(p,), device_id_type=MESH)

    own_cnt = pltpu.make_async_copy(cnt, cnt_all.at[me], own_sem.at[n_local])
    own_cnt.start()
    for k in range(1, n_dev):
        c_copy(k).start()
    for e in range(n_local):
        for k in (1, 2, 4, 6, 3, 5, 7):
            if (e, k) not in EARLY:
                x_copy(k, e).start()
            dy_copy(k, e).start()

    order = (0, 1, 2, 4, 6, 3, 5, 7)

    def offset_of(i):
        k = i * 0
        for at, val in enumerate(order):
            k = k + jnp.where(i == at, val, 0)
        return k

    def load(e, i, slot, do):
        k = offset_of(i)
        p = peer_of(k)

        early = (e == 0) & ((i == 2) | (i == 3))

        def x_from(source):
            do(pltpu.make_async_copy(source, xv.at[slot], ld_sem.at[slot, 0]))

        @pl.when(i == 0)
        def _():
            x_from(xs.at[me, e])
            do(pltpu.make_async_copy(dys.at[me, e], dyv.at[slot], ld_sem.at[slot, 1]))

        @pl.when((e == 0) & (i == 2))
        def _():
            x_from(near_x)

        @pl.when((e == 0) & (i == 3))
        def _():
            x_from(near_y)

        @pl.when((i > 0) & jnp.logical_not(early))
        def _():
            x_from(xr.at[p, e])

        @pl.when(i > 0)
        def _():
            do(pltpu.make_async_copy(dyr.at[p, e], dyv.at[slot], ld_sem.at[slot, 1]))

    def arrive(e, i):
        k = offset_of(i)

        @pl.when((i > 0) & jnp.logical_not((e == 0) & ((i == 2) | (i == 3))))
        def _():
            x_copy(k, e).wait_recv()

        @pl.when(i > 0)
        def _():
            dy_copy(k, e).wait_recv()

    def store(c, do):
        e, i = c // n_dev, c % n_dev
        k = offset_of(i)
        p = peer_of(k)

        @pl.when(e == n_local - 1)
        def _():
            do(pltpu.make_async_copy(r_out.at[c % 2], dlast.at[p], st_sem.at[c % 2]))

        @pl.when(e < n_local - 1)
        def _():
            @pl.when(i == 0)
            def _():
                do(pltpu.make_async_copy(r_out.at[c % 2], dback.at[me, e], st_sem.at[c % 2]))

            @pl.when(i > 0)
            def _():
                do(pltpu.make_async_copy(r_out.at[c % 2], dsend.at[p, e], st_sem.at[c % 2]))

    def own_g(e):
        return pltpu.make_async_copy(g_all.at[e, 0], gback.at[me, e], own_sem.at[e])

    def send_back(c):
        e, i = c // n_dev, c % n_dev
        k = offset_of(i)
        store(c, lambda cp: cp.wait())

        @pl.when(i == 0)
        def _():
            own_g(e).start()

        @pl.when(i > 0)
        def _():
            s_copy(k, e).start()

            @pl.when(e < n_local - 1)
            def _():
                r_copy(k, e).start()

    def weights(e):
        return (pltpu.make_async_copy(w_in.at[e], win_v, w_sem.at[0]), pltpu.make_async_copy(w_out.at[e], wout_v, w_sem.at[1]))

    def flush(e):
        return (pltpu.make_async_copy(acc_in, gwin.at[e], flush_sem.at[0]), pltpu.make_async_copy(acc_out, gwout_t.at[e], flush_sem.at[1]))

    for cp in weights(0):
        cp.start()
    load(0 * me, 0 * me, 0, lambda cp: cp.start())
    for at, piece in enumerate(split3(w_t[...])):
        pad = jnp.zeros((LANES - num_experts, piece.shape[1]), F32)
        wr[at] = jnp.concatenate([piece, pad], axis=0).T.astype(BF16)

    def chunk(c, _):
        e, i = c // n_dev, c % n_dev
        k = offset_of(i)
        slot = c % 2

        @pl.when(i == 0)
        def _():
            @pl.when(c > 0)
            def _():
                for cp in weights(e):
                    cp.start()
                for cp in flush(e - 1):
                    cp.wait()
            acc_in[...] = jnp.zeros_like(acc_in)
            acc_out[...] = jnp.zeros_like(acc_out)
            for cp in weights(e):
                cp.wait()

        load(e, i, slot, lambda cp: cp.wait())
        x = xv[slot]
        logits = nn(x, wr[0]) + nn(x, wr[1]) + nn(x, wr[2])
        lane = lax.broadcasted_iota(jnp.int32, logits.shape, 1)
        logits = jnp.where(lane < num_experts, logits, -1e30)
        prob = jnp.exp(logits - jnp.max(logits, axis=1, keepdims=True))
        mine = jnp.sum(jnp.where(lane == me * n_local + e, prob, 0.0), axis=1, keepdims=True)
        gate = mine / jnp.sum(prob, axis=1, keepdims=True)
        grad = (gate * dyv[slot].astype(F32)).astype(BF16)
        gv[...] = grad
        x_t[...] = x.T
        g_t[...] = grad.T
        o_acc[...] = jnp.zeros_like(o_acc)
        r_acc[...] = jnp.zeros_like(r_acc)

        def block(f, _):
            @pl.when(f == n_blk - 1)
            def _():
                @pl.when(c + 1 < n_chunk)
                def _():
                    ne, ni = (c + 1) // n_dev, (c + 1) % n_dev
                    arrive(ne, ni)
                    load(ne, ni, 1 - slot, lambda cp: cp.start())

            @pl.when(f == 1)
            def _():
                @pl.when(c > 0)
                def _():
                    send_back(c - 1)

            cols = pl.ds(pl.multiple_of(f * blk, LANES), blk)
            win = win_v[:, cols]
            wout = wout_v[cols, :]
            hidden = jnp.maximum(nn(xv[slot], win), 0.0).astype(BF16)
            d_hidden = nt(gv[...], wout)
            d_pre = jnp.where(hidden > 0, d_hidden, 0.0).astype(BF16)
            o_acc[...] += nn(hidden, wout)
            r_acc[...] += nt(d_pre, win)
            acc_out[:, cols] += nn(g_t[...], hidden)
            acc_in[:, cols] += nn(x_t[...], d_pre)
            return 0

        lax.fori_loop(0, n_blk, block, 0)
        r_out[slot] = r_acc[...].astype(BF16)
        store(c, lambda cp: cp.start())
        g_val = jnp.sum(o_acc[...].astype(BF16).astype(F32) * dyv[slot].astype(F32), axis=1, keepdims=True)
        g_row = jnp.broadcast_to(g_val, (g_val.shape[0], LANES)).T
        g_all[e, k] = g_row[0:1, :]

        @pl.when(i == n_dev - 1)
        def _():
            for cp in flush(e):
                cp.start()
        return 0

    lax.fori_loop(0, n_chunk, chunk, 0)
    send_back(n_chunk - 1)
    for cp in flush(n_local - 1):
        cp.wait()
    own_cnt.wait()
    for k in range(1, n_dev):
        c_copy(k).wait()
    for e in range(n_local):
        own_g(e).wait()
        for k in range(1, n_dev):
            if (e, k) not in EARLY:
                x_copy(k, e).wait_send()
            dy_copy(k, e).wait_send()
            if e < n_local - 1:
                r_copy(k, e).wait()
            s_copy(k, e).wait()


def expert_exchange(n_dev, xs, dys, near_x, near_y, w_t, cnt, w_in, w_out):
    n_local, d_model, d_ff = w_in.shape
    cap = xs.shape[2]
    num_experts = n_dev * n_local
    blk = d_ff // 4
    hbm = pl.BlockSpec(memory_space=pl.ANY)
    vmem = pl.BlockSpec(memory_space=pltpu.VMEM)
    rows = jax.ShapeDtypeStruct(xs.shape, BF16)
    early = jax.ShapeDtypeStruct((n_dev, n_local - 1, cap, d_model), BF16)
    late = jax.ShapeDtypeStruct((n_dev, cap, d_model), BF16)
    g_shape = jax.ShapeDtypeStruct((n_dev, n_local, 1, cap), F32)
    w_shape = jax.ShapeDtypeStruct((n_local, d_model, d_ff), F32)
    dma = pltpu.SemaphoreType.DMA
    pair = (n_local, n_dev)
    return pl.pallas_call(
        lambda *refs: expert_kernel(n_dev, n_local, num_experts, blk, *refs),
        out_shape=(rows, rows, early, early, late, g_shape, w_shape, w_shape, jax.ShapeDtypeStruct((n_dev,) + cnt.shape, F32)),
        in_specs=[hbm, hbm, hbm, hbm, vmem, vmem, hbm, hbm],
        out_specs=[hbm] * 9,
        scratch_shapes=[
            pltpu.VMEM((2, cap, d_model), BF16), pltpu.VMEM((2, cap, d_model), BF16), pltpu.VMEM((cap, d_model), BF16),
            pltpu.VMEM((d_model, cap), BF16), pltpu.VMEM((d_model, cap), BF16), pltpu.VMEM((3, d_model, LANES), BF16),
            pltpu.VMEM((d_model, d_ff), BF16), pltpu.VMEM((d_ff, d_model), BF16),
            pltpu.VMEM((d_model, d_ff), F32), pltpu.VMEM((d_model, d_ff), F32),
            pltpu.VMEM((cap, d_model), F32), pltpu.VMEM((cap, d_model), F32),
            pltpu.VMEM((2, cap, d_model), BF16), pltpu.VMEM((n_local, n_dev, 1, cap), F32),
            dma(pair), dma(pair), dma(pair), dma(pair), dma(pair), dma(pair), dma(pair), dma(pair), dma((n_dev,)), dma((n_dev,)),
            dma((2, 2)), dma((2,)), dma((2,)), dma((2,)), dma((n_local + 1,)),
        ],
        compiler_params=pltpu.CompilerParams(collective_id=0, has_side_effects=True, vmem_limit_bytes=63 * 2 ** 20),
        name='expert_exchange',
    )(xs, dys, near_x, near_y, w_t, cnt, w_in, w_out)


PITCH = 7 * 8
STEP = 9
UNROLL = 128
ROW_TILES = 6


def row(addr, tiles):
    return pl.ds(addr, tiles, stride=STEP)


TB = 512
IN_FLIGHT = 4


def permute_rows(addr, source, sink, inb, stage, table, outb, in_sem, out_sem, meanwhile, extra):
    n_out, n_local, cap, d_model = sink.shape
    groups = cap // 8
    tiled = table.reshape(table.shape[0] // PITCH, PITCH, LANES)
    stage3 = stage.reshape(TB // 8, PITCH, LANES)
    n_in = source.shape[0] // TB
    n_chunk = n_out * n_local

    def fetch(b):
        return pltpu.make_async_copy(source.at[pl.ds(pl.multiple_of(b * TB, TB), TB), :], inb.at[b % IN_FLIGHT], in_sem.at[b % IN_FLIGHT])

    def emit(c):
        return pltpu.make_async_copy(outb.at[c], sink.at[c // n_local, c % n_local], out_sem.at[c])

    for b in range(IN_FLIGHT - 1):
        fetch(b).start()
    table[...] = jnp.zeros_like(table)
    meanwhile()

    def scatter(b, _):
        @pl.when(b + IN_FLIGHT - 1 < n_in)
        def _():
            fetch(b + IN_FLIGHT - 1).start()
        fetch(b).wait()
        for j in range(ROW_TILES):
            part = inb[b % IN_FLIGHT, :, j * LANES:(j + 1) * LANES].astype(F32)
            stage3[:, j * STEP:j * STEP + 8, :] = part.reshape(TB // 8, 8, LANES)

        def move(i, _):
            for r in range(UNROLL):
                at = addr[b * TB + i * UNROLL + r]
                table[row(at, ROW_TILES), :] = stage[row(i * (UNROLL // 8 * PITCH) + (r // 8) * PITCH + r % 8, ROW_TILES), :]
            return 0

        lax.fori_loop(0, TB // UNROLL, move, 0)
        return 0

    lax.fori_loop(0, n_in, scatter, 0)

    def drain(c, _):
        for j in range(ROW_TILES):
            part = tiled[pl.ds(c * groups, groups), j * STEP:j * STEP + 8, :].reshape(cap, LANES)
            outb[c, :, j * LANES:(j + 1) * LANES] = part.astype(BF16)
        emit(c).start()
        return 0

    def finish(c, _):
        emit(c).wait()
        return 0

    lax.fori_loop(0, n_chunk, drain, 0)
    extra(outb)
    lax.fori_loop(0, n_chunk, finish, 0)


def route_permute_kernel(idx, x, xs, near_x, near_y, slot_out, addr_out, count_out, addr, addr_sem, near_sem, *scratch):
    n_out, n_local, cap, _ = xs.shape
    n = n_out * n_local

    def route():
        below = lax.broadcasted_iota(jnp.int32, (TB, TB), 0) <= lax.broadcasted_iota(jnp.int32, (TB, TB), 1)
        upper = jnp.where(below, 1.0, 0.0).astype(BF16)
        expert = lax.broadcasted_iota(jnp.int32, (n, TB), 0)
        seen = jnp.zeros((n, 1), F32)
        for b in range(idx.shape[0]):
            mine = expert == idx[b:b + 1, :]
            onehot = jnp.where(mine, 1.0, 0.0)
            rank = nn(onehot.astype(BF16), upper)
            pos = jnp.sum(jnp.where(mine, rank + (seen - 1.0), 0.0), axis=0, keepdims=True).astype(jnp.int32)
            slot = jnp.where(pos < cap, idx[b:b + 1, :] * cap + pos, n * cap)
            slot_out[b:b + 1, :] = slot
            group = lax.shift_right_logical(slot, jnp.full_like(slot, 3))
            addr_out[b:b + 1, :] = group * PITCH + (slot - group * 8)
            seen = seen + rank[:, TB - 1:TB]
        count_out[...] = jnp.broadcast_to(seen, count_out.shape)
        load_table(addr_out, addr, addr_sem)

    def near(outb):
        me = lax.axis_index('ep')
        copies = []
        for at, ((e, k), sink) in enumerate(zip(EARLY, (near_x, near_y))):
            p = me + k - 2 * k * ((me // k) % 2)
            copies.append(pltpu.make_async_copy(outb.at[p * n_local + e], sink, near_sem.at[at]))
        for copy in copies:
            copy.start()
        for copy in copies:
            copy.wait()

    permute_rows(addr, x, xs, *scratch, route, near)


def permute_scratch(n_slots, cap, d_model):
    return [pltpu.VMEM((IN_FLIGHT, TB, d_model), BF16), pltpu.VMEM((TB // 8 * PITCH, LANES), F32), pltpu.VMEM(((n_slots // 8 + 1) * PITCH, LANES), F32),
            pltpu.VMEM((n_slots // cap, cap, d_model), BF16), pltpu.SemaphoreType.DMA((IN_FLIGHT,)), pltpu.SemaphoreType.DMA((n_slots // cap,))]


def route_permute(n_dev, n_local, cap, idx, x):
    hbm = pl.BlockSpec(memory_space=pl.ANY)
    vmem = pl.BlockSpec(memory_space=pltpu.VMEM)
    table = jax.ShapeDtypeStruct(idx.shape, jnp.int32)
    n = n_dev * n_local
    block = jax.ShapeDtypeStruct((cap, x.shape[1]), BF16)
    return pl.pallas_call(
        route_permute_kernel,
        out_shape=(jax.ShapeDtypeStruct((n_dev, n_local, cap, x.shape[1]), BF16), block, block, table, table, jax.ShapeDtypeStruct((n, LANES), F32)),
        in_specs=[vmem, hbm], out_specs=[hbm, hbm, hbm, vmem, vmem, vmem],
        scratch_shapes=[pltpu.SMEM((idx.size,), jnp.int32), pltpu.SemaphoreType.DMA((idx.shape[0],)), pltpu.SemaphoreType.DMA((2,))] + permute_scratch(n * cap, cap, x.shape[1]),
        compiler_params=pltpu.CompilerParams(vmem_limit_bytes=60 * 2 ** 20),
        name='route_permute',
    )(idx, x)


def load_table(table, addr, sem):
    copies = [pltpu.make_async_copy(table.at[b], addr.at[pl.ds(b * TB, TB)], sem.at[b]) for b in range(table.shape[0])]
    for copy in copies:
        copy.start()
    for copy in copies:
        copy.wait()


def permute_kernel(table, x, xs, addr, addr_sem, *scratch):
    permute_rows(addr, x, xs, *scratch, lambda: load_table(table, addr, addr_sem), lambda outb: None)


def permute(n_dev, n_local, cap, addr, x):
    hbm = pl.BlockSpec(memory_space=pl.ANY)
    return pl.pallas_call(
        permute_kernel,
        out_shape=jax.ShapeDtypeStruct((n_dev, n_local, cap, x.shape[1]), BF16),
        in_specs=[pl.BlockSpec(memory_space=pltpu.VMEM), hbm], out_specs=hbm,
        scratch_shapes=[pltpu.SMEM((addr.size,), jnp.int32), pltpu.SemaphoreType.DMA((addr.shape[0],))]
        + permute_scratch(n_dev * n_local * cap, cap, x.shape[1]),
        cost_estimate=pl.CostEstimate(flops=20 * 10 ** 9, bytes_accessed=28 * 2 ** 20, transcendentals=0),
        compiler_params=pltpu.CompilerParams(vmem_limit_bytes=60 * 2 ** 20),
        name='permute_rows',
    )(addr, x)


def router_kernel(z_coef, slot, x, idx, w_t, v_col, gback, pieces_out, partial, acc, gtab, g_rows, w_six, pieces_t, p_acc, z_acc):
    b = pl.program_id(0)
    tb = x.shape[0]
    n_chunk, cap = gback.shape
    n = w_t.shape[0]

    @pl.when(b == 0)
    def _():
        acc[...] = jnp.zeros_like(acc)
        p_acc[...] = jnp.zeros_like(p_acc)
        z_acc[...] = jnp.zeros_like(z_acc)
        w_six[...] = six_terms(w_t[...])
        gtab[n_chunk * cap:, :] = jnp.zeros((8, LANES), F32)

        def fill(c, _):
            gtab[pl.ds(pl.multiple_of(c * cap, 8), cap), :] = jnp.broadcast_to(gback[pl.ds(c, 1), :], (LANES, cap)).T
            return 0

        lax.fori_loop(0, n_chunk, fill, 0)

    def move(i, _):
        for r in range(UNROLL):
            g_rows[pl.ds(i * UNROLL + r, 1), :] = gtab[pl.ds(slot[b * tb + i * UNROLL + r], 1), :]
        return 0

    lax.fori_loop(0, tb // UNROLL, move, 0)

    xv = x[...]
    terms = nt(w_six[...], xv)
    logits = terms[0:n] + terms[3 * n:4 * n] + terms[5 * n:6 * n]
    top = jnp.max(logits, axis=0, keepdims=True)
    expd = jnp.exp(logits - top)
    total = jnp.sum(expd, axis=0, keepdims=True)
    prob = expd / total
    z = top + jnp.log(total)
    mine = lax.broadcasted_iota(jnp.int32, logits.shape, 0) == idx[pl.ds(b, 1), :]
    onehot = jnp.where(mine, 1.0, 0.0)
    gate = jnp.sum(jnp.where(mine, prob, 0.0), axis=0, keepdims=True)
    g = g_rows[...].T[0:1, :]
    v = v_col[:, 0:1]
    spread = jnp.sum(prob * v, axis=0, keepdims=True)
    dlog = gate * g * (onehot - prob) + prob * (v - spread) + (z_coef * z) * prob
    hi, mid, low = split3(dlog)
    pieces = jnp.concatenate([hi, mid, low, hi, mid, hi, jnp.zeros((LANES - 6 * n, tb), F32)], axis=0)
    pieces_out[...] = pieces.T.astype(BF16)
    pieces_t[...] = pieces.astype(BF16)
    acc[...] += nn(pieces_t[...], xv)
    zz = z * z
    for j in range(tb // LANES):
        p_acc[...] += prob[:, j * LANES:(j + 1) * LANES]
        z_acc[0:1, :] += zz[:, j * LANES:(j + 1) * LANES]

    @pl.when(b == pl.num_programs(0) - 1)
    def _():
        partial[...] = jnp.zeros_like(partial)
        partial[0:n, :] = acc[0:n, :] + acc[n:2 * n, :] + acc[2 * n:3 * n, :]
        p_sum = jnp.broadcast_to(jnp.sum(p_acc[...], axis=1, keepdims=True), p_acc.shape)
        p_full = jnp.concatenate([p_sum, jnp.zeros((LANES - n, LANES), F32)], axis=0).T
        partial[n:n + 1, 0:LANES] = p_full[0:1, :]
        partial[n:n + 1, LANES:2 * LANES] = jnp.broadcast_to(jnp.sum(z_acc[0:1, :], axis=1, keepdims=True), (1, LANES))


def whole(a):
    return pl.BlockSpec(a.shape, lambda b, addr: (0,) * a.ndim)


def router_side(z_coef, slot, x, idx, w_t, v_col, gback):
    tokens, d_model = x.shape
    n_dev, n_local, _, cap = gback.shape
    tb = TB
    n = w_t.shape[0]
    gback = gback.reshape(n_dev * n_local, cap)
    rows = n + 8
    return pl.pallas_call(
        lambda *refs: router_kernel(z_coef, *refs),
        out_shape=(jax.ShapeDtypeStruct((tokens, LANES), BF16), jax.ShapeDtypeStruct((rows, d_model), F32), jax.ShapeDtypeStruct((LANES, d_model), F32)),
        grid_spec=pltpu.PrefetchScalarGridSpec(
            num_scalar_prefetch=1, grid=(tokens // tb,),
            in_specs=[pl.BlockSpec((tb, d_model), lambda b, addr: (b, 0)), whole(idx), whole(w_t), whole(v_col), whole(gback)],
            out_specs=[pl.BlockSpec((tb, LANES), lambda b, addr: (b, 0)), pl.BlockSpec((rows, d_model), lambda b, addr: (0, 0)),
                       pl.BlockSpec((LANES, d_model), lambda b, addr: (0, 0))],
            scratch_shapes=[
                pltpu.VMEM((n_dev * n_local * cap + 8, LANES), F32), pltpu.VMEM((tb, LANES), F32), pltpu.VMEM((LANES, d_model), BF16),
                pltpu.VMEM((LANES, tb), BF16), pltpu.VMEM((n, LANES), F32), pltpu.VMEM((8, LANES), F32)]),
        cost_estimate=pl.CostEstimate(flops=30 * 10 ** 9, bytes_accessed=16 * 2 ** 20, transcendentals=0),
        compiler_params=pltpu.CompilerParams(vmem_limit_bytes=40 * 2 ** 20),
        name='router_side',
    )(slot, x, idx, w_t, v_col, gback)


def combine_kernel(addr, pieces, w_t, dback, dlast, grad_x, stage, table, inb, w_six, in_sem):
    b = pl.program_id(0)
    tb = pieces.shape[0]
    n_out, cap, d_model = dlast.shape
    n_local = dback.shape[1] + 1
    groups = cap // 8
    tiled = table.reshape(table.shape[0] // PITCH, PITCH, LANES)
    stage3 = stage.reshape(tb // 8, PITCH, LANES)

    @pl.when(b == 0)
    def _():
        n_buf = inb.shape[1]

        def fetch(d, e):
            source = dback.at[d, e] if e < n_local - 1 else dlast.at[d]
            return pltpu.make_async_copy(source, inb.at[e, d % n_buf], in_sem.at[e, d % n_buf])

        for d in range(n_buf):
            for e in range(n_local):
                fetch(d, e).start()
        w_six[...] = six_terms(w_t[...])
        tiled[n_out * n_local * groups] = jnp.zeros((PITCH, LANES), F32)

        def fill(d, _):
            for e in range(n_local):
                fetch(d, e).wait()
                for j in range(ROW_TILES):
                    part = inb[e, d % n_buf, :, j * LANES:(j + 1) * LANES].astype(F32)
                    tiled[pl.ds((d * n_local + e) * groups, groups), j * STEP:j * STEP + 8, :] = part.reshape(groups, 8, LANES)

                @pl.when(d + n_buf < n_out)
                def _():
                    fetch(d + n_buf, e).start()
            return 0

        lax.fori_loop(0, n_out, fill, 0)

    def move(i, _):
        for r in range(UNROLL):
            at = addr[b * tb + i * UNROLL + r]
            stage[row(i * (UNROLL // 8 * PITCH) + (r // 8) * PITCH + r % 8, ROW_TILES), :] = table[row(at, ROW_TILES), :]
        return 0

    lax.fori_loop(0, tb // UNROLL, move, 0)
    for j in range(ROW_TILES):
        cols = slice(j * LANES, (j + 1) * LANES)
        grad_x[:, cols] = (stage3[:, j * STEP:j * STEP + 8, :].reshape(tb, LANES) + nn(pieces[...], w_six[:, cols])).astype(BF16)


def combine(addr, pieces, w_t, dback, dlast):
    tokens = pieces.shape[0]
    n_dev, cap, d_model = dlast.shape
    n_local = dback.shape[1] + 1
    tb = 2 * TB
    hbm = pl.BlockSpec(memory_space=pl.ANY)
    n_groups = n_dev * n_local * cap // 8 + 1
    return pl.pallas_call(
        combine_kernel,
        out_shape=jax.ShapeDtypeStruct((tokens, d_model), BF16),
        grid_spec=pltpu.PrefetchScalarGridSpec(
            num_scalar_prefetch=1, grid=(tokens // tb,),
            in_specs=[pl.BlockSpec((tb, LANES), lambda b, addr: (b, 0)), whole(w_t), hbm, hbm],
            out_specs=pl.BlockSpec((tb, d_model), lambda b, addr: (b, 0)),
            scratch_shapes=[
                pltpu.VMEM((tb // 8 * PITCH, LANES), F32), pltpu.VMEM((n_groups * PITCH, LANES), F32),
                pltpu.VMEM((n_local, 4, cap, d_model), BF16), pltpu.VMEM((LANES, d_model), BF16), pltpu.SemaphoreType.DMA((n_local, 4))]),
        compiler_params=pltpu.CompilerParams(vmem_limit_bytes=56 * 2 ** 20),
        name='combine_rows',
    )(addr, pieces, w_t, dback, dlast)


def total_kernel(n_dev, total_tok, part, load, _before_a, _before_b, out, aux, zl, parts, send_sem, recv_sem):
    me = lax.axis_index('ep')
    barrier = pltpu.get_barrier_semaphore()
    peers = [(me + k) % n_dev for k in range(1, n_dev)]
    for p in peers:
        pl.semaphore_signal(barrier, inc=1, device_id=(p,), device_id_type=MESH)
    pl.semaphore_wait(barrier, n_dev - 1)
    copies = [pltpu.make_async_remote_copy(part, parts.at[me], send_sem.at[k], recv_sem.at[k], device_id=(p,), device_id_type=MESH)
              for k, p in enumerate(peers)]
    for copy in copies:
        copy.start()
    parts[me] = part[...]
    for copy in copies:
        copy.wait()
    total = parts[0]
    for d in range(1, n_dev):
        total = total + parts[d]
    n = out.shape[0]
    out[...] = total[0:n]
    load_row = jnp.concatenate([load[...], jnp.zeros((LANES - n, LANES), F32)], axis=0).T[0:1, :]
    aux[0, 0] = AUX_WEIGHT * n * jnp.sum(load_row * (total[n:n + 1, 0:LANES] / total_tok))
    zl[0, 0] = Z_WEIGHT * jnp.max(total[n:n + 1, LANES:2 * LANES]) / total_tok


def total_over_devices(n_dev, total_tok, part, load, before):
    vmem = pl.BlockSpec(memory_space=pltpu.VMEM)
    smem = pl.BlockSpec(memory_space=pltpu.SMEM)
    one = jax.ShapeDtypeStruct((1, 1), F32)
    return pl.pallas_call(
        lambda *refs: total_kernel(n_dev, total_tok, *refs),
        out_shape=(jax.ShapeDtypeStruct((load.shape[0], part.shape[1]), F32), one, one),
        in_specs=[vmem, vmem] + [pl.BlockSpec(memory_space=pl.ANY)] * 2, out_specs=[vmem, smem, smem],
        scratch_shapes=[pltpu.VMEM((n_dev,) + part.shape, F32), pltpu.SemaphoreType.DMA((n_dev - 1,)), pltpu.SemaphoreType.DMA((n_dev - 1,))],
        compiler_params=pltpu.CompilerParams(collective_id=1, has_side_effects=True),
        name='device_total',
    )(part, load, *before)


def copy_kernel(source, sink):
    sink[...] = source[...]


def own_copy(a):
    n, rows, cols = a.shape
    spec = pl.BlockSpec((1, rows // 6, cols), lambda e, r: (e, r, 0))
    return pl.pallas_call(
        copy_kernel, out_shape=jax.ShapeDtypeStruct(a.shape, a.dtype), grid=(n, 6), in_specs=[spec], out_specs=spec,
        cost_estimate=pl.CostEstimate(flops=15 * 10 ** 9, bytes_accessed=2 * a.size * 4, transcendentals=0),
        name='own_copy')(a)


def solution(mesh):
    n_dev = mesh.shape['ep']

    def expert_layer(x_tokens, w_router, expert_idx, w_in, w_out, grad_y):
        tokens, d_model = x_tokens.shape
        n_local = w_in.shape[0]
        num_experts = n_local * n_dev
        capacity = (5 * tokens + 4 * num_experts - 1) // (4 * num_experts)
        total_tok = tokens * n_dev
        w_t = w_router.T
        idx = expert_idx.reshape(tokens // TB, TB)
        xs, near_x, near_y, slot, addr, cnt = route_permute(n_dev, n_local, capacity, idx, x_tokens)
        near_x, near_y = [lax.ppermute(block, 'ep', [(d, d ^ k) for d in range(n_dev)]) for block, (_, k) in zip((near_x, near_y), EARLY)]
        dys = permute(n_dev, n_local, capacity, addr, grad_y)
        slot, addr = slot.reshape(tokens), addr.reshape(tokens)

        _, _, _, d_back, d_last, g_back, gwin, gwout_t, cnt_all = expert_exchange(n_dev, xs, dys, near_x, near_y, w_t, cnt, w_in, w_out)
        d_last = lax.all_to_all(d_last, 'ep', 0, 0, tiled=True)
        load_frac = jnp.sum(cnt_all, axis=0) / total_tok
        v_col = AUX_WEIGHT * num_experts * load_frac / total_tok
        pieces, partial, _ = router_side(2.0 * Z_WEIGHT / total_tok, slot, x_tokens, idx, w_t, v_col, g_back)
        grad_w_out = jnp.swapaxes(gwout_t, 1, 2)
        grad_w_in = own_copy(gwin)
        grad_x = combine(addr, pieces, w_t, d_back, d_last)
        grad_wr_t, aux_loss, z_loss = total_over_devices(n_dev, total_tok, partial, load_frac, (grad_w_in, grad_w_out))
        grad_w_router, aux_loss, z_loss = grad_wr_t.T, aux_loss.reshape(()), z_loss.reshape(())
        return grad_x, grad_w_in, grad_w_out, grad_w_router, aux_loss, z_loss

    return jax.shard_map(expert_layer, mesh=mesh,
                         in_specs=(P('ep', None), P(None, None), P('ep'), P('ep', None, None), P('ep', None, None), P('ep', None)),
                         out_specs=(P('ep', None), P('ep', None, None), P('ep', None, None), P(None, None), P(), P()),
                         check_vma=False)
```
